16 devices in a mesh: data: 2 (over y, z), tp: 8 (over x, core).
Axes of the slice: x: 4, y: 2, z: 1, core: 2. Of those that a mesh axis runs over, the one named last changes fastest.
The devices are a block of a 4x4x8 slice.
Arguments:
- attn_out: bfloat16 [1024, 12288], P('data', 'tp'), parts along dimension 0
- w_out: bfloat16 [12288, 12288], P('tp')
- residual: bfloat16 [1024, 12288], P('data', 'tp'), parts along dimension 0
- norm_gain: float32 [12288], P('tp')
Outputs:
- output 1: bfloat16 [1024, 12288], P('data', 'tp'), parts along dimension 0
- output 2: bfloat16 [1024, 12288], P('data', 'tp'), parts along dimension 0
There are 2 independent parts. The reference program is written for one: setup_inputs(seed, part) draws one part's arguments, and reference() takes and returns one part's arrays. A program takes and returns all parts, laid end to end along the dimension named above; an argument that names none is the same for every part.
All inputs are finite; a program needn't handle non-finite values.
Results may differ from the reference program's by a relative error of at most 0.00634263.
Values are sent between devices in bfloat16 or wider.
A program may use at most 768 MiB of HBM per device.

```python
import jax
import jax.numpy as jnp
from jax import lax

D_MODEL = 12288
N_HEADS = 96
HEAD_DIM = 128
TOKENS = 512
EPS = 1e-5


def setup_inputs(seed: int = 0, part: int = 0) -> dict:
    proj_width = N_HEADS * HEAD_DIM
    part_key = jax.random.fold_in(jax.random.key(seed), part)
    key_attn, key_resid = jax.random.split(part_key, 2)
    key_weight, key_gain = jax.random.split(jax.random.key(seed + 1), 2)
    attn_out = jax.random.normal(key_attn, (TOKENS, proj_width), jnp.float32).astype(jnp.bfloat16)
    weight_vals = jax.random.normal(key_weight, (proj_width, D_MODEL), jnp.float32) * proj_width ** -0.5
    w_out = weight_vals.astype(jnp.bfloat16)
    residual = jax.random.normal(key_resid, (TOKENS, D_MODEL), jnp.float32).astype(jnp.bfloat16)
    norm_gain = jax.random.uniform(key_gain, (D_MODEL,), jnp.float32, 0.5, 1.5)
    return {"attn_out": attn_out, "w_out": w_out, "residual": residual, "norm_gain": norm_gain}


def reference(attn_out, w_out, residual, norm_gain):
    projected = jnp.dot(attn_out, w_out, preferred_element_type=jnp.float32)
    hidden = residual.astype(jnp.float32) + projected
    mean_sq = jnp.mean(hidden * hidden, axis=-1, keepdims=True)
    normed = hidden * lax.rsqrt(mean_sq + EPS) * norm_gain
    return (hidden.astype(jnp.bfloat16), normed.astype(jnp.bfloat16))
```

```python
import functools

import jax
import jax.numpy as jnp
from jax import lax
from jax.experimental import pallas as pl
from jax.experimental.pallas import tpu as pltpu
from jax.sharding import PartitionSpec as P

EPS = 1e-5
MESH = pl.DeviceIdType.MESH
CORES = 2
CHIPS = 4
UNIT = 256
W_SLOTS = 4
RB = 64
AHEAD = 3
LAG = 3


def _kernel(
    tp_size, d_model,
    a_hbm, w_hbm, r_hbm, g_hbm, hid_hbm, nrm_hbm,
    a, w, p, rx, relay_out, relay_in, res, gain, hbuf, hout, nout, sq_out, sq_in,
    in_sem, w_sem, send_sem, recv_sem, rsend_sem, rrecv_sem, qsend_sem, qrecv_sem, out_sem,
):
    rows, d_local = r_hbm.shape
    half = d_local // 2
    nu = half // UNIT
    per_group = CORES * 2 * nu
    total = CHIPS * per_group
    chunks = rows // RB

    me = lax.axis_index("tp")
    x, c = lax.div(me, CORES), lax.rem(me, CORES)

    def chip(offset, core):
        return lax.rem(x + offset, CHIPS) * CORES + core

    def decode(s):
        g, j = lax.div(s, per_group), lax.rem(s, per_group)
        i, eb, hh = lax.div(j, 4), lax.rem(lax.div(j, 2), 2), lax.rem(j, 2)
        return g, i, eb, lax.rem(eb + 1 + c, 2), lax.rem(hh + c, 2)

    def w_copy(s):
        g, i, _, e, h = decode(s)
        o = lax.rem(6 - g + 2 * h * lax.rem(g, 2), CHIPS)
        col = pl.multiple_of(chip(o, e) * d_local + h * half + i * UNIT, UNIT)
        k = lax.rem(s, W_SLOTS)
        return pltpu.make_async_copy(w_hbm.at[:, pl.ds(col, UNIT)], w.at[k], w_sem.at[k])

    def block_copy(s, slot, target):
        return pltpu.make_async_remote_copy(
            src_ref=p.at[s], dst_ref=rx.at[slot], send_sem=send_sem.at[s], recv_sem=recv_sem.at[slot],
            device_id={"tp": target}, device_id_type=MESH)

    def local_unit(g, h, i):
        return g * per_group + i * 4 + 2 + lax.rem(h + c, 2)

    def relay_copy(h, r):
        return pltpu.make_async_remote_copy(
            src_ref=relay_out.at[h, r], dst_ref=relay_in.at[h, r],
            send_sem=rsend_sem.at[h, r], recv_sem=rrecv_sem.at[h, r],
            device_id={"tp": chip(3 - 2 * h, c)}, device_id_type=MESH)

    def sq_copy(r, t):
        return pltpu.make_async_remote_copy(
            src_ref=sq_out.at[r], dst_ref=sq_in.at[r, me],
            send_sem=qsend_sem.at[r, t], recv_sem=qrecv_sem.at[r, me],
            device_id={"tp": lax.rem(me + t, tp_size)}, device_id_type=MESH)

    def chunk_rows(r):
        return pl.ds(pl.multiple_of(r * RB, RB), RB)

    barrier = pltpu.get_barrier_semaphore()
    for t in range(1, tp_size):
        pl.semaphore_signal(barrier, inc=1, device_id={"tp": lax.rem(me + t, tp_size)}, device_id_type=MESH)

    w_copy(jnp.int32(0)).start()
    a_copy = pltpu.make_async_copy(a_hbm, a, in_sem.at[0])
    a_copy.start()
    for s in range(1, W_SLOTS):
        w_copy(jnp.int32(s)).start()
    r_copy = pltpu.make_async_copy(r_hbm, res, in_sem.at[1])
    r_copy.start()
    g_copy = pltpu.make_async_copy(g_hbm, gain, in_sem.at[2])
    g_copy.start()
    a_copy.wait()

    @pl.loop(0, total)
    def _(s):
        g, i, eb, e, h = decode(s)
        w_copy(s).wait()
        k = lax.rem(s, W_SLOTS)
        p[s] = jnp.dot(a[...], w[k], preferred_element_type=jnp.float32).astype(p.dtype)

        @pl.when(s + W_SLOTS < total)
        def _():
            w_copy(s + W_SLOTS).start()

        @pl.when(s == 0)
        def _():
            pl.semaphore_wait(barrier, tp_size - 1)

        @pl.when(g == 0)
        def _():
            block_copy(s, (h * 2 + c) * nu + i, chip(3 + 2 * h, e)).start()

        @pl.when(g == 1)
        def _():
            block_copy(s, (4 + h * 2 + c) * nu + i, chip(1 + 2 * h, e)).start()

        @pl.when(jnp.logical_and(g >= 2, eb == 0))
        def _():
            block_copy(s, (4 + g * 2 + h) * nu + i, x * CORES + 1 - c).start()

    def wait_blocks(lo, hi):
        @pl.loop(lo, hi)
        def _(slot):
            block_copy(0, slot, me).wait_recv()

    wait_blocks(0, 4 * nu)
    wait_blocks(10 * nu, 12 * nu)

    @pl.loop(0, chunks)
    def _(r):
        rs = chunk_rows(r)
        for h in range(2):
            for i in range(nu):
                acc = p[local_unit(3, h, i), rs, :].astype(jnp.float32)
                acc += rx[(10 + h) * nu + i, rs, :].astype(jnp.float32)
                acc += rx[(h * 2) * nu + i, rs, :].astype(jnp.float32)
                acc += rx[(h * 2 + 1) * nu + i, rs, :].astype(jnp.float32)
                relay_out[h, r, :, i * UNIT:(i + 1) * UNIT] = acc

        @pl.when(r < AHEAD)
        def _():
            for h in range(2):
                relay_copy(h, r).start()

    r_copy.wait()
    g_copy.wait()
    wait_blocks(8 * nu, 10 * nu)
    wait_blocks(4 * nu, 8 * nu)

    eye = (lax.broadcasted_iota(jnp.int32, (RB, 128), 0)
           == lax.broadcasted_iota(jnp.int32, (RB, 128), 1))

    def hid_copy(r):
        return pltpu.make_async_copy(hout.at[r], hid_hbm.at[chunk_rows(r), :], out_sem.at[0, r])

    def nrm_copy(r):
        return pltpu.make_async_copy(nout.at[r], nrm_hbm.at[chunk_rows(r), :], out_sem.at[1, r])

    def normalise(r):
        for t in range(1, tp_size):
            src = lax.rem(me + t, tp_size)
            pltpu.make_async_remote_copy(
                src_ref=sq_out.at[r], dst_ref=sq_in.at[r, src],
                send_sem=qsend_sem.at[r, t], recv_sem=qrecv_sem.at[r, src],
                device_id={"tp": src}, device_id_type=MESH).wait_recv()
        tot = sq_in[r, 0]
        for t in range(1, tp_size):
            tot += sq_in[r, t]
        col = jnp.sum(jnp.where(eye, jnp.broadcast_to(tot, (RB, 128)), 0.0), axis=1, keepdims=True)
        scale = lax.rsqrt(col / d_model + EPS)
        nout[r] = (hbuf[r] * scale * gain[...]).astype(nout.dtype)
        nrm_copy(r).start()

    @pl.loop(0, chunks)
    def _(r):
        @pl.when(r + AHEAD < chunks)
        def _():
            for h in range(2):
                relay_copy(h, r + AHEAD).start()

        rs = chunk_rows(r)
        sq = jnp.zeros((RB, UNIT), jnp.float32)
        for h in range(2):
            relay_copy(h, r).wait_recv()
            for i in range(nu):
                cols = slice(h * half + i * UNIT, h * half + (i + 1) * UNIT)
                acc = p[local_unit(2, h, i), rs, :].astype(jnp.float32)
                acc += rx[(8 + h) * nu + i, rs, :].astype(jnp.float32)
                acc += rx[(4 + h * 2) * nu + i, rs, :].astype(jnp.float32)
                acc += rx[(5 + h * 2) * nu + i, rs, :].astype(jnp.float32)
                acc += relay_in[h, r, :, i * UNIT:(i + 1) * UNIT]
                acc += res[rs, cols].astype(jnp.float32)
                hbuf[r, :, cols] = acc
                hout[r, :, cols] = acc.astype(hout.dtype)
                sq += acc * acc
        sq = jnp.sum(sq, axis=1, keepdims=True)
        packed = jnp.sum(jnp.where(eye, jnp.broadcast_to(sq, (RB, 128)), 0.0), axis=0, keepdims=True)
        sq_out[r] = packed
        sq_in[r, me] = packed
        hid_copy(r).start()
        for t in range(1, tp_size):
            sq_copy(r, t).start()

        @pl.when(r >= LAG)
        def _():
            normalise(r - LAG)

    @pl.loop(chunks - LAG, chunks)
    def _(r):
        normalise(r)

    @pl.loop(0, total)
    def _(s):
        g, i, eb, e, h = decode(s)

        @pl.when(jnp.logical_or(g < 2, eb == 0))
        def _():
            block_copy(s, 0, me).wait_send()

    @pl.loop(0, chunks)
    def _(r):
        for h in range(2):
            relay_copy(h, r).wait_send()
        for t in range(1, tp_size):
            sq_copy(r, t).wait_send()
        hid_copy(r).wait()
        nrm_copy(r).wait()


def solution(mesh):
    tp_size = mesh.shape["tp"]

    def local_step(attn_blk, w_blk, resid_blk, gain_blk):
        rows, k_dim = attn_blk.shape
        d_local = resid_blk.shape[1]
        d_model = w_blk.shape[1]
        half = d_local // 2
        nu = half // UNIT
        units = tp_size * 2 * nu
        chunks = rows // RB
        assert tp_size == CORES * CHIPS and half % UNIT == 0 and rows % RB == 0
        any_spec = pl.BlockSpec(memory_space=pl.ANY)
        dma = pltpu.SemaphoreType.DMA
        return pl.pallas_call(
            functools.partial(_kernel, tp_size, d_model),
            out_shape=[jax.ShapeDtypeStruct((rows, d_local), jnp.bfloat16)] * 2,
            in_specs=[any_spec] * 4,
            out_specs=[any_spec] * 2,
            scratch_shapes=[
                pltpu.VMEM((rows, k_dim), jnp.bfloat16),
                pltpu.VMEM((W_SLOTS, k_dim, UNIT), jnp.bfloat16),
                pltpu.VMEM((units, rows, UNIT), jnp.bfloat16),
                pltpu.VMEM((12 * nu, rows, UNIT), jnp.bfloat16),
                pltpu.VMEM((2, chunks, RB, half), jnp.float32),
                pltpu.VMEM((2, chunks, RB, half), jnp.float32),
                pltpu.VMEM((rows, d_local), jnp.bfloat16),
                pltpu.VMEM((1, d_local), jnp.float32),
                pltpu.VMEM((chunks, RB, d_local), jnp.float32),
                pltpu.VMEM((chunks, RB, d_local), jnp.bfloat16),
                pltpu.VMEM((chunks, RB, d_local), jnp.bfloat16),
                pltpu.VMEM((chunks, 1, 128), jnp.float32),
                pltpu.VMEM((chunks, tp_size, 1, 128), jnp.float32),
                dma((3,)),
                dma((W_SLOTS,)),
                dma((units,)),
                dma((12 * nu,)),
                dma((2, chunks)),
                dma((2, chunks)),
                dma((chunks, tp_size)),
                dma((chunks, tp_size)),
                dma((2, chunks)),
            ],
            compiler_params=pltpu.CompilerParams(
                collective_id=0, has_side_effects=True, vmem_limit_bytes=56 * 1024 * 1024
            ),
            name="proj_scatter_norm",
        )(attn_blk, w_blk, resid_blk, gain_blk.reshape(1, d_local))

    return jax.shard_map(
        local_step,
        mesh=mesh,
        in_specs=(P("data", "tp"), P("tp", None), P("data", "tp"), P("tp")),
        out_specs=(P("data", "tp"), P("data", "tp")),
        check_vma=False,
    )
```

```python
import functools

import jax
import jax.numpy as jnp
from jax import lax
from jax.experimental import pallas as pl
from jax.experimental.pallas import tpu as pltpu
from jax.sharding import PartitionSpec as P

EPS = 1e-5
MESH = pl.DeviceIdType.MESH
CORES = 2
CHIPS = 4
UNIT = 256
W_SLOTS = 4
RB = 64
AHEAD = 3
LAG = 3
A_BLOCKS = 4


def _kernel(
    tp_size, d_model,
    a_hbm, w_hbm, r_hbm, g_hbm, hid, nrm,
    a, w, p, rx, relay_out, relay_in, res, gain, hbuf, sq_out, sq_in,
    a_sem, in_sem, w_sem, send_sem, recv_sem, rsend_sem, rrecv_sem, qsend_sem, qrecv_sem,
):
    rows, d_local = r_hbm.shape
    half = d_local // 2
    nu = half // UNIT
    per_group = CORES * 2 * nu
    total = CHIPS * per_group
    chunks = rows // RB
    ab = rows // A_BLOCKS

    me = lax.axis_index("tp")
    x, c = lax.div(me, CORES), lax.rem(me, CORES)

    def chip(offset, core):
        return lax.rem(x + offset, CHIPS) * CORES + core

    def decode(s):
        g, j = lax.div(s, per_group), lax.rem(s, per_group)
        i, eb, hh = lax.div(j, 4), lax.rem(lax.div(j, 2), 2), lax.rem(j, 2)
        return g, i, eb, lax.rem(eb + 1 + c, 2), lax.rem(hh + c, 2)

    def w_copy(s):
        g, i, _, e, h = decode(s)
        o = lax.rem(6 - g + 2 * h * lax.rem(g, 2), CHIPS)
        col = pl.multiple_of(chip(o, e) * d_local + h * half + i * UNIT, UNIT)
        k = lax.rem(s, W_SLOTS)
        return pltpu.make_async_copy(w_hbm.at[:, pl.ds(col, UNIT)], w.at[k], w_sem.at[k])

    def a_copy(b):
        rs = pl.ds(b * ab, ab)
        return pltpu.make_async_copy(a_hbm.at[rs, :], a.at[rs, :], a_sem.at[b])

    def send_rows(s, slot, group, target, rs):
        pltpu.make_async_remote_copy(
            src_ref=p.at[s, rs], dst_ref=rx.at[slot, rs], send_sem=send_sem.at[0], recv_sem=recv_sem.at[group],
            device_id={"tp": target}, device_id_type=MESH).start()

    def send_block(s, slot, group, target):
        send_rows(s, slot, group, target, pl.ds(0, rows))

    def wait_bytes(ref, sem):
        pltpu.make_async_copy(ref, ref, sem).wait()

    def local_unit(g, h, i):
        return g * per_group + i * 4 + 2 + lax.rem(h + c, 2)

    def send_relay(r):
        for h in range(2):
            pltpu.make_async_remote_copy(
                src_ref=relay_out.at[r, h], dst_ref=relay_in.at[r, h],
                send_sem=rsend_sem.at[0], recv_sem=rrecv_sem.at[r],
                device_id={"tp": chip(3 - 2 * h, c)}, device_id_type=MESH).start()

    def chunk_rows(r):
        return pl.ds(pl.multiple_of(r * RB, RB), RB)

    barrier = pltpu.get_barrier_semaphore()
    for t in range(1, tp_size):
        pl.semaphore_signal(barrier, inc=1, device_id={"tp": lax.rem(me + t, tp_size)}, device_id_type=MESH)

    w_copy(jnp.int32(0)).start()
    for b in range(A_BLOCKS):
        a_copy(b).start()
    for s in range(1, W_SLOTS):
        w_copy(jnp.int32(s)).start()
    r_copy = pltpu.make_async_copy(r_hbm, res, in_sem.at[0])
    r_copy.start()
    g_copy = pltpu.make_async_copy(g_hbm, gain, in_sem.at[1])
    g_copy.start()

    _, i0, _, e0, h0 = decode(jnp.int32(0))
    w_copy(jnp.int32(0)).wait()
    for b in range(A_BLOCKS):
        a_copy(b).wait()
        rs = pl.ds(b * ab, ab)
        p[0, rs, :] = jnp.dot(a[rs, :], w[0], preferred_element_type=jnp.float32).astype(p.dtype)
        if b == 0:
            pl.semaphore_wait(barrier, tp_size - 1)
        send_rows(0, (h0 * 2 + c) * nu + i0, 0, chip(3 + 2 * h0, e0), rs)
    w_copy(jnp.int32(W_SLOTS)).start()

    @pl.loop(1, total)
    def _(s):
        g, i, eb, e, h = decode(s)
        w_copy(s).wait()
        k = lax.rem(s, W_SLOTS)
        p[s] = jnp.dot(a[...], w[k], preferred_element_type=jnp.float32).astype(p.dtype)

        @pl.when(s + W_SLOTS < total)
        def _():
            w_copy(s + W_SLOTS).start()

        @pl.when(g == 0)
        def _():
            send_block(s, (h * 2 + c) * nu + i, 0, chip(3 + 2 * h, e))

        @pl.when(g == 1)
        def _():
            send_block(s, (4 + h * 2 + c) * nu + i, 1, chip(1 + 2 * h, e))

        @pl.when(jnp.logical_and(g >= 2, eb == 0))
        def _():
            send_block(s, (4 + g * 2 + h) * nu + i, g, x * CORES + 1 - c)

    wait_bytes(rx.at[pl.ds(0, 4 * nu)], recv_sem.at[0])
    wait_bytes(rx.at[pl.ds(10 * nu, 2 * nu)], recv_sem.at[3])

    @pl.loop(0, chunks)
    def _(r):
        rs = chunk_rows(r)
        for h in range(2):
            for i in range(nu):
                acc = p[local_unit(3, h, i), rs, :].astype(jnp.float32)
                acc += rx[(10 + h) * nu + i, rs, :].astype(jnp.float32)
                acc += rx[(h * 2) * nu + i, rs, :].astype(jnp.float32)
                acc += rx[(h * 2 + 1) * nu + i, rs, :].astype(jnp.float32)
                relay_out[r, h, :, i * UNIT:(i + 1) * UNIT] = acc

        @pl.when(r < AHEAD)
        def _():
            send_relay(r)

    r_copy.wait()
    g_copy.wait()
    wait_bytes(rx.at[pl.ds(8 * nu, 2 * nu)], recv_sem.at[2])
    wait_bytes(rx.at[pl.ds(4 * nu, 4 * nu)], recv_sem.at[1])

    eye = (lax.broadcasted_iota(jnp.int32, (RB, 128), 0)
           == lax.broadcasted_iota(jnp.int32, (RB, 128), 1))

    def normalise(r):
        wait_bytes(sq_in.at[r, pl.ds(0, tp_size - 1)], qrecv_sem.at[r])
        tot = sq_in[r, 0]
        for t in range(1, tp_size):
            tot += sq_in[r, t]
        col = jnp.sum(jnp.where(eye, jnp.broadcast_to(tot, (RB, 128)), 0.0), axis=1, keepdims=True)
        scale = lax.rsqrt(col / d_model + EPS)
        nrm[chunk_rows(r), :] = (hbuf[r] * scale * gain[...].reshape(1, d_local)).astype(nrm.dtype)

    @pl.loop(0, chunks)
    def _(r):
        @pl.when(r + AHEAD < chunks)
        def _():
            send_relay(r + AHEAD)

        wait_bytes(relay_in.at[r], rrecv_sem.at[r])
        rs = chunk_rows(r)
        sq = jnp.zeros((RB, UNIT), jnp.float32)
        for h in range(2):
            for i in range(nu):
                cols = slice(h * half + i * UNIT, h * half + (i + 1) * UNIT)
                acc = p[local_unit(2, h, i), rs, :].astype(jnp.float32)
                acc += rx[(8 + h) * nu + i, rs, :].astype(jnp.float32)
                acc += rx[(4 + h * 2) * nu + i, rs, :].astype(jnp.float32)
                acc += rx[(5 + h * 2) * nu + i, rs, :].astype(jnp.float32)
                acc += relay_in[r, h, :, i * UNIT:(i + 1) * UNIT]
                acc += res[rs, cols].astype(jnp.float32)
                hbuf[r, :, cols] = acc
                sq += acc * acc
        sq = jnp.sum(sq, axis=1, keepdims=True)
        packed = jnp.sum(jnp.where(eye, jnp.broadcast_to(sq, (RB, 128)), 0.0), axis=0, keepdims=True)
        sq_out[r] = packed
        sq_in[r, me] = packed
        hid[rs, :] = hbuf[r].astype(hid.dtype)
        for t in range(1, tp_size):
            pltpu.make_async_remote_copy(
                src_ref=sq_out.at[r], dst_ref=sq_in.at[r, me],
                send_sem=qsend_sem.at[0], recv_sem=qrecv_sem.at[r],
                device_id={"tp": lax.rem(me + t, tp_size)}, device_id_type=MESH).start()

        @pl.when(r >= LAG)
        def _():
            normalise(r - LAG)

    wait_bytes(rx, send_sem.at[0])
    wait_bytes(relay_out, rsend_sem.at[0])

    @pl.loop(chunks - LAG, chunks)
    def _(r):
        normalise(r)

    wait_bytes(sq_in.at[:, pl.ds(0, tp_size - 1)], qsend_sem.at[0])


def _write(hid, nrm, hid_hbm, nrm_hbm, sem):
    blocks = 4
    rows = hid.shape[0] // blocks
    copies = []
    for k, (src, dst) in enumerate(((hid, hid_hbm), (nrm, nrm_hbm))):
        for b in range(blocks):
            rs = pl.ds(b * rows, rows)
            copies.append(pltpu.make_async_copy(src.at[rs, :], dst.at[rs, :], sem.at[k, b]))
    for copy in copies:
        copy.start()
    for copy in copies:
        copy.wait()


def solution(mesh):
    tp_size = mesh.shape["tp"]

    def local_step(attn_blk, w_blk, resid_blk, gain_blk):
        rows, k_dim = attn_blk.shape
        d_local = resid_blk.shape[1]
        d_model = w_blk.shape[1]
        half = d_local // 2
        nu = half // UNIT
        units = tp_size * 2 * nu
        chunks = rows // RB
        assert tp_size == CORES * CHIPS and half % UNIT == 0 and rows % RB == 0
        hbm_spec = pl.BlockSpec(memory_space=pltpu.HBM)
        vmem_spec = pl.BlockSpec(memory_space=pltpu.VMEM)
        dma = pltpu.SemaphoreType.DMA
        out_shape = [jax.ShapeDtypeStruct((rows, d_local), jnp.bfloat16)] * 2
        hid, nrm = pl.pallas_call(
            functools.partial(_kernel, tp_size, d_model),
            out_shape=[pltpu.VMEM((rows, d_local), jnp.bfloat16)] * 2,
            in_specs=[hbm_spec] * 4,
            out_specs=[vmem_spec] * 2,
            scratch_shapes=[
                pltpu.VMEM((rows, k_dim), jnp.bfloat16),
                pltpu.VMEM((W_SLOTS, k_dim, UNIT), jnp.bfloat16),
                pltpu.VMEM((units, rows, UNIT), jnp.bfloat16),
                pltpu.VMEM((12 * nu, rows, UNIT), jnp.bfloat16),
                pltpu.VMEM((chunks, 2, RB, half), jnp.float32),
                pltpu.VMEM((chunks, 2, RB, half), jnp.float32),
                pltpu.VMEM((rows, d_local), jnp.bfloat16),
                pltpu.VMEM((d_local,), jnp.float32),
                pltpu.VMEM((chunks, RB, d_local), jnp.float32),
                pltpu.VMEM((chunks, 1, 128), jnp.float32),
                pltpu.VMEM((chunks, tp_size, 1, 128), jnp.float32),
                dma((A_BLOCKS,)),
                dma((2,)),
                dma((W_SLOTS,)),
                dma((1,)),
                dma((4,)),
                dma((1,)),
                dma((chunks,)),
                dma((1,)),
                dma((chunks,)),
            ],
            compiler_params=pltpu.CompilerParams(
                collective_id=0, has_side_effects=True, vmem_limit_bytes=62 * 1000 * 1000
            ),
            name="proj_scatter_norm",
        )(attn_blk, w_blk, resid_blk, gain_blk)
        return pl.pallas_call(
            _write,
            out_shape=out_shape,
            in_specs=[vmem_spec] * 2,
            out_specs=[hbm_spec] * 2,
            scratch_shapes=[dma((2, 4))],
            compiler_params=pltpu.CompilerParams(vmem_limit_bytes=8 * 1024 * 1024),
            name="write_out",
        )(hid, nrm)

    return jax.shard_map(
        local_step,
        mesh=mesh,
        in_specs=(P("data", "tp"), P("tp", None), P("data", "tp"), P("tp")),
        out_specs=(P("data", "tp"), P("data", "tp")),
        check_vma=False,
    )
```

```python
import functools

import jax
import jax.numpy as jnp
from jax import lax
from jax.experimental import pallas as pl
from jax.experimental.pallas import tpu as pltpu
from jax.sharding import PartitionSpec as P

EPS = 1e-5
MESH = pl.DeviceIdType.MESH
CORES = 2
CHIPS = 4
UNIT = 256
W_SLOTS = 4
RB = 64
AHEAD = 3
A_BLOCKS = 4


def _kernel(
    tp_size, d_model,
    a_hbm, w_hbm, r_hbm, g_hbm, hid, nrm,
    a, w, p, rx, relay_out, relay_in, res, gain, hbuf, sq_out, sq_in,
    a_sem, in_sem, w_sem, send_sem, recv_sem, rsend_sem, rrecv_sem, qsend_sem, qrecv_sem,
):
    rows, d_local = r_hbm.shape
    half = d_local // 2
    nu = half // UNIT
    per_group = CORES * 2 * nu
    total = CHIPS * per_group
    chunks = rows // RB
    ab = rows // A_BLOCKS

    me = lax.axis_index("tp")
    x, c = lax.div(me, CORES), lax.rem(me, CORES)

    def chip(offset, core):
        return lax.rem(x + offset, CHIPS) * CORES + core

    def decode(s):
        g, j = lax.div(s, per_group), lax.rem(s, per_group)
        i, eb, hh = lax.div(j, 4), lax.rem(lax.div(j, 2), 2), lax.rem(j, 2)
        return g, i, eb, lax.rem(eb + 1 + c, 2), lax.rem(hh + c, 2)

    def w_copy(s):
        g, i, _, e, h = decode(s)
        o = lax.rem(6 - g + 2 * h * lax.rem(g, 2), CHIPS)
        col = pl.multiple_of(chip(o, e) * d_local + h * half + i * UNIT, UNIT)
        k = lax.rem(s, W_SLOTS)
        return pltpu.make_async_copy(w_hbm.at[:, pl.ds(col, UNIT)], w.at[k], w_sem.at[k])

    def a_copy(b):
        rs = pl.ds(b * ab, ab)
        return pltpu.make_async_copy(a_hbm.at[rs, :], a.at[rs, :], a_sem.at[b])

    def send_rows(s, slot, group, target, rs):
        pltpu.make_async_remote_copy(
            src_ref=p.at[s, rs], dst_ref=rx.at[slot, rs], send_sem=send_sem.at[0], recv_sem=recv_sem.at[group],
            device_id={"tp": target}, device_id_type=MESH).start()

    def send_block(s, slot, group, target):
        send_rows(s, slot, group, target, pl.ds(0, rows))

    def wait_bytes(ref, sem):
        pltpu.make_async_copy(ref, ref, sem).wait()

    def local_unit(g, h, i):
        return g * per_group + i * 4 + 2 + lax.rem(h + c, 2)

    def send_relay(r):
        for h in range(2):
            pltpu.make_async_remote_copy(
                src_ref=relay_out.at[r, h], dst_ref=relay_in.at[r, h],
                send_sem=rsend_sem.at[0], recv_sem=rrecv_sem.at[r],
                device_id={"tp": chip(3 - 2 * h, c)}, device_id_type=MESH).start()

    def chunk_rows(r):
        return pl.ds(pl.multiple_of(r * RB, RB), RB)

    w_copy(jnp.int32(0)).start()
    a_copy(0).start()

    peers = [x * CORES + 1 - c] + [chip(o, core) for o in (1, CHIPS - 1) for core in range(CORES)]
    barrier = pltpu.get_barrier_semaphore()
    for peer in peers:
        pl.semaphore_signal(barrier, inc=1, device_id={"tp": peer}, device_id_type=MESH)

    for b in range(1, A_BLOCKS):
        a_copy(b).start()
    r_copy = pltpu.make_async_copy(r_hbm, res, in_sem.at[0])
    g_copy = pltpu.make_async_copy(g_hbm, gain, in_sem.at[1])

    _, i0, _, e0, h0 = decode(jnp.int32(0))
    w_copy(jnp.int32(0)).wait()
    for b in range(A_BLOCKS):
        a_copy(b).wait()
        if b == 0:
            for s in range(1, W_SLOTS):
                w_copy(jnp.int32(s)).start()
        rs = pl.ds(b * ab, ab)
        p[0, rs, :] = jnp.dot(a[rs, :], w[0], preferred_element_type=jnp.float32).astype(p.dtype)
        if b == 0:
            pl.semaphore_wait(barrier, len(peers))
        send_rows(0, (h0 * 2 + c) * nu + i0, 0, chip(3 + 2 * h0, e0), rs)
    w_copy(jnp.int32(W_SLOTS)).start()
    r_copy.start()
    g_copy.start()

    @pl.loop(1, total)
    def _(s):
        g, i, eb, e, h = decode(s)
        w_copy(s).wait()
        k = lax.rem(s, W_SLOTS)
        p[s] = jnp.dot(a[...], w[k], preferred_element_type=jnp.float32).astype(p.dtype)

        @pl.when(s + W_SLOTS < total)
        def _():
            w_copy(s + W_SLOTS).start()

        @pl.when(g == 0)
        def _():
            send_block(s, (h * 2 + c) * nu + i, 0, chip(3 + 2 * h, e))

        @pl.when(g == 1)
        def _():
            send_block(s, (4 + h * 2 + c) * nu + i, 1, chip(1 + 2 * h, e))

        @pl.when(jnp.logical_and(g >= 2, eb == 0))
        def _():
            send_block(s, (4 + g * 2 + h) * nu + i, g, x * CORES + 1 - c)

    wait_bytes(rx.at[pl.ds(0, 4 * nu)], recv_sem.at[0])
    wait_bytes(rx.at[pl.ds(10 * nu, 2 * nu)], recv_sem.at[3])

    @pl.loop(0, chunks)
    def _(r):
        rs = chunk_rows(r)
        for h in range(2):
            for i in range(nu):
                acc = p[local_unit(3, h, i), rs, :].astype(jnp.float32)
                acc += rx[(10 + h) * nu + i, rs, :].astype(jnp.float32)
                acc += rx[(h * 2) * nu + i, rs, :].astype(jnp.float32)
                acc += rx[(h * 2 + 1) * nu + i, rs, :].astype(jnp.float32)
                relay_out[r, h, :, i * UNIT:(i + 1) * UNIT] = acc

        @pl.when(r < AHEAD)
        def _():
            send_relay(r)

    r_copy.wait()
    g_copy.wait()
    wait_bytes(rx.at[pl.ds(8 * nu, 2 * nu)], recv_sem.at[2])
    wait_bytes(rx.at[pl.ds(4 * nu, 4 * nu)], recv_sem.at[1])

    eye = (lax.broadcasted_iota(jnp.int32, (RB, 128), 0)
           == lax.broadcasted_iota(jnp.int32, (RB, 128), 1))

    def columns():
        for h in range(2):
            for i in range(nu):
                yield h, i, slice(h * half + i * UNIT, h * half + (i + 1) * UNIT)

    def add_early(r):
        rs = chunk_rows(r)
        for h, i, cols in columns():
            acc = p[local_unit(2, h, i), rs, :].astype(jnp.float32)
            acc += rx[(8 + h) * nu + i, rs, :].astype(jnp.float32)
            acc += rx[(4 + h * 2) * nu + i, rs, :].astype(jnp.float32)
            acc += rx[(5 + h * 2) * nu + i, rs, :].astype(jnp.float32)
            hbuf[r, :, cols] = acc + res[rs, cols].astype(jnp.float32)

    def finish(r):
        sq = jnp.zeros((RB, UNIT), jnp.float32)
        for h, i, cols in columns():
            acc = hbuf[r, :, cols] + relay_in[r, h, :, i * UNIT:(i + 1) * UNIT]
            hbuf[r, :, cols] = acc
            sq += acc * acc
        sq = jnp.sum(sq, axis=1, keepdims=True)
        packed = jnp.sum(jnp.where(eye, jnp.broadcast_to(sq, (RB, 128)), 0.0), axis=0, keepdims=True)
        sq_out[r] = packed
        sq_in[me, r] = packed

    def send_sums(lo, n, k):
        for t in range(1, tp_size):
            pltpu.make_async_remote_copy(
                src_ref=sq_out.at[pl.ds(lo, n)], dst_ref=sq_in.at[me, pl.ds(lo, n)],
                send_sem=qsend_sem.at[k], recv_sem=qrecv_sem.at[k],
                device_id={"tp": lax.rem(me + t, tp_size)}, device_id_type=MESH).start()

    def wait_sums(lo, n, sem):
        wait_bytes(sq_in.at[pl.ds(0, tp_size - 1), pl.ds(lo, n)], sem)

    def normalise(r):
        tot = sq_in[0, r]
        for t in range(1, tp_size):
            tot += sq_in[t, r]
        col = jnp.sum(jnp.where(eye, jnp.broadcast_to(tot, (RB, 128)), 0.0), axis=1, keepdims=True)
        scale = lax.rsqrt(col / d_model + EPS)
        nrm[chunk_rows(r), :] = (hbuf[r] * scale * gain[...].reshape(1, d_local)).astype(nrm.dtype)

    def write_hidden(r):
        hid[chunk_rows(r), :] = hbuf[r].astype(hid.dtype)

    last = chunks - 1

    @pl.loop(0, last)
    def _(r):
        @pl.when(r + AHEAD < chunks)
        def _():
            send_relay(r + AHEAD)

        add_early(r)
        wait_bytes(relay_in.at[r], rrecv_sem.at[r])
        finish(r)
        write_hidden(r)

    send_sums(0, last, 0)
    add_early(last)
    wait_bytes(rx, send_sem.at[0])
    wait_sums(0, last, qrecv_sem.at[0])

    @pl.loop(0, last)
    def _(r):
        normalise(r)

    wait_bytes(relay_in.at[last], rrecv_sem.at[last])
    finish(last)
    send_sums(last, 1, 1)
    write_hidden(last)
    wait_bytes(relay_out, rsend_sem.at[0])
    wait_sums(0, last, qsend_sem.at[0])
    wait_sums(last, 1, qrecv_sem.at[1])
    normalise(last)
    wait_sums(last, 1, qsend_sem.at[1])


def _write(hid, nrm, hid_hbm, nrm_hbm, sem):
    blocks = 4
    rows = hid.shape[0] // blocks
    copies = []
    for k, (src, dst) in enumerate(((hid, hid_hbm), (nrm, nrm_hbm))):
        for b in range(blocks):
            rs = pl.ds(b * rows, rows)
            copies.append(pltpu.make_async_copy(src.at[rs, :], dst.at[rs, :], sem.at[k, b]))
    for copy in copies:
        copy.start()
    for copy in copies:
        copy.wait()


def solution(mesh):
    tp_size = mesh.shape["tp"]

    def local_step(attn_blk, w_blk, resid_blk, gain_blk):
        rows, k_dim = attn_blk.shape
        d_local = resid_blk.shape[1]
        d_model = w_blk.shape[1]
        half = d_local // 2
        nu = half // UNIT
        units = tp_size * 2 * nu
        chunks = rows // RB
        assert tp_size == CORES * CHIPS and half % UNIT == 0 and rows % RB == 0
        hbm_spec = pl.BlockSpec(memory_space=pltpu.HBM)
        vmem_spec = pl.BlockSpec(memory_space=pltpu.VMEM)
        dma = pltpu.SemaphoreType.DMA
        out_shape = [jax.ShapeDtypeStruct((rows, d_local), jnp.bfloat16)] * 2
        hid, nrm = pl.pallas_call(
            functools.partial(_kernel, tp_size, d_model),
            out_shape=[pltpu.VMEM((rows, d_local), jnp.bfloat16)] * 2,
            in_specs=[hbm_spec] * 4,
            out_specs=[vmem_spec] * 2,
            scratch_shapes=[
                pltpu.VMEM((rows, k_dim), jnp.bfloat16),
                pltpu.VMEM((W_SLOTS, k_dim, UNIT), jnp.bfloat16),
                pltpu.VMEM((units, rows, UNIT), jnp.bfloat16),
                pltpu.VMEM((12 * nu, rows, UNIT), jnp.bfloat16),
                pltpu.VMEM((chunks, 2, RB, half), jnp.float32),
                pltpu.VMEM((chunks, 2, RB, half), jnp.float32),
                pltpu.VMEM((rows, d_local), jnp.bfloat16),
                pltpu.VMEM((d_local,), jnp.float32),
                pltpu.VMEM((chunks, RB, d_local), jnp.float32),
                pltpu.VMEM((chunks, 1, 128), jnp.float32),
                pltpu.VMEM((tp_size, chunks, 1, 128), jnp.float32),
                dma((A_BLOCKS,)),
                dma((2,)),
                dma((W_SLOTS,)),
                dma((1,)),
                dma((4,)),
                dma((1,)),
                dma((chunks,)),
                dma((2,)),
                dma((2,)),
            ],
            compiler_params=pltpu.CompilerParams(
                collective_id=0, has_side_effects=True, vmem_limit_bytes=62 * 1000 * 1000
            ),
            name="proj_scatter_norm",
        )(attn_blk, w_blk, resid_blk, gain_blk)
        return pl.pallas_call(
            _write,
            out_shape=out_shape,
            in_specs=[vmem_spec] * 2,
            out_specs=[hbm_spec] * 2,
            scratch_shapes=[dma((2, 4))],
            compiler_params=pltpu.CompilerParams(vmem_limit_bytes=8 * 1024 * 1024),
            name="write_out",
        )(hid, nrm)

    return jax.shard_map(
        local_step,
        mesh=mesh,
        in_specs=(P("data", "tp"), P("tp", None), P("data", "tp"), P("tp")),
        out_specs=(P("data", "tp"), P("data", "tp")),
        check_vma=False,
    )
```

```python
import functools

import jax
import jax.numpy as jnp
from jax import lax
from jax.experimental import pallas as pl
from jax.experimental.pallas import tpu as pltpu
from jax.sharding import PartitionSpec as P

EPS = 1e-5
MESH = pl.DeviceIdType.MESH
CORES = 2
CHIPS = 4
UNIT = 256
W_SLOTS = 4
RB = 64
AHEAD = 3
A_BLOCKS = 4


def _kernel(
    tp_size, d_model,
    a_hbm, w_hbm, r_hbm, g_hbm, hid, nrm,
    a, w, p, rx, relay_out, relay_in, res, gain, hbuf, sq_out, sq_in,
    a_sem, in_sem, w_sem, send_sem, recv_sem, rsend_sem, rrecv_sem, qsend_sem, qrecv_sem,
):
    rows, d_local = r_hbm.shape
    half = d_local // 2
    nu = half // UNIT
    per_group = CORES * 2 * nu
    total = CHIPS * per_group
    chunks = rows // RB
    ab = rows // A_BLOCKS

    me = lax.axis_index("tp")
    x, c = lax.div(me, CORES), lax.rem(me, CORES)

    def chip(offset, core):
        return lax.rem(x + offset, CHIPS) * CORES + core

    def decode(s):
        g, j = lax.div(s, per_group), lax.rem(s, per_group)
        i, eb, hh = lax.div(j, 4), lax.rem(lax.div(j, 2), 2), lax.rem(j, 2)
        return g, i, eb, lax.rem(eb + 1 + c, 2), lax.rem(hh + c, 2)

    def w_copy(s):
        g, i, _, e, h = decode(s)
        o = lax.rem(6 - g + 2 * h * lax.rem(g, 2), CHIPS)
        col = pl.multiple_of(chip(o, e) * d_local + h * half + i * UNIT, UNIT)
        k = lax.rem(s, W_SLOTS)
        return pltpu.make_async_copy(w_hbm.at[:, pl.ds(col, UNIT)], w.at[k], w_sem.at[k])

    def a_copy(b):
        rs = pl.ds(b * ab, ab)
        return pltpu.make_async_copy(a_hbm.at[rs, :], a.at[rs, :], a_sem.at[b])

    def send_rows(s, slot, group, target, rs):
        pltpu.make_async_remote_copy(
            src_ref=p.at[s, rs], dst_ref=rx.at[slot, rs], send_sem=send_sem.at[0], recv_sem=recv_sem.at[group],
            device_id={"tp": target}, device_id_type=MESH).start()

    def send_block(s, slot, group, target):
        send_rows(s, slot, group, target, pl.ds(0, rows))

    def wait_bytes(ref, sem):
        pltpu.make_async_copy(ref, ref, sem).wait()

    def local_unit(g, h, i):
        return g * per_group + i * 4 + 2 + lax.rem(h + c, 2)

    def send_relay(r):
        for h in range(2):
            pltpu.make_async_remote_copy(
                src_ref=relay_out.at[r, h], dst_ref=relay_in.at[r, h],
                send_sem=rsend_sem.at[0], recv_sem=rrecv_sem.at[r],
                device_id={"tp": chip(3 - 2 * h, c)}, device_id_type=MESH).start()

    def chunk_rows(r):
        return pl.ds(pl.multiple_of(r * RB, RB), RB)

    w_copy(jnp.int32(0)).start()
    a_copy(0).start()

    peers = [x * CORES + 1 - c] + [chip(o, core) for o in (1, CHIPS - 1) for core in range(CORES)]
    barrier = pltpu.get_barrier_semaphore()
    for peer in peers:
        pl.semaphore_signal(barrier, inc=1, device_id={"tp": peer}, device_id_type=MESH)

    for b in range(1, A_BLOCKS):
        a_copy(b).start()
    r_copy = pltpu.make_async_copy(r_hbm, res, in_sem.at[0])
    g_copy = pltpu.make_async_copy(g_hbm, gain, in_sem.at[1])

    _, i0, _, e0, h0 = decode(jnp.int32(0))
    w_copy(jnp.int32(0)).wait()
    for b in range(A_BLOCKS):
        a_copy(b).wait()
        if b == 0:
            for s in range(1, W_SLOTS):
                w_copy(jnp.int32(s)).start()
        rs = pl.ds(b * ab, ab)
        p[0, rs, :] = jnp.dot(a[rs, :], w[0], preferred_element_type=jnp.float32).astype(p.dtype)
        if b == 0:
            pl.semaphore_wait(barrier, len(peers))
        send_rows(0, (h0 * 2 + c) * nu + i0, 0, chip(3 + 2 * h0, e0), rs)
    w_copy(jnp.int32(W_SLOTS)).start()
    r_copy.start()
    g_copy.start()

    @pl.loop(1, total)
    def _(s):
        g, i, eb, e, h = decode(s)
        w_copy(s).wait()
        k = lax.rem(s, W_SLOTS)
        p[s] = jnp.dot(a[...], w[k], preferred_element_type=jnp.float32).astype(p.dtype)

        @pl.when(s + W_SLOTS < total)
        def _():
            w_copy(s + W_SLOTS).start()

        @pl.when(g == 0)
        def _():
            send_block(s, (h * 2 + c) * nu + i, 0, chip(3 + 2 * h, e))

        @pl.when(g == 1)
        def _():
            send_block(s, (4 + h * 2 + c) * nu + i, 1, chip(1 + 2 * h, e))

        @pl.when(jnp.logical_and(g >= 2, eb == 0))
        def _():
            send_block(s, (4 + g * 2 + h) * nu + i, g, x * CORES + 1 - c)

    wait_bytes(rx.at[pl.ds(0, 4 * nu)], recv_sem.at[0])
    wait_bytes(rx.at[pl.ds(10 * nu, 2 * nu)], recv_sem.at[3])

    @pl.loop(0, chunks)
    def _(r):
        rs = chunk_rows(r)
        for h in range(2):
            for i in range(nu):
                acc = p[local_unit(3, h, i), rs, :].astype(jnp.float32)
                acc += rx[(10 + h) * nu + i, rs, :].astype(jnp.float32)
                acc += rx[(h * 2) * nu + i, rs, :].astype(jnp.float32)
                acc += rx[(h * 2 + 1) * nu + i, rs, :].astype(jnp.float32)
                relay_out[r, h, :, i * UNIT:(i + 1) * UNIT] = acc

        @pl.when(r < AHEAD)
        def _():
            send_relay(r)

    r_copy.wait()
    g_copy.wait()
    wait_bytes(rx.at[pl.ds(8 * nu, 2 * nu)], recv_sem.at[2])
    wait_bytes(rx.at[pl.ds(4 * nu, 4 * nu)], recv_sem.at[1])

    eye = (lax.broadcasted_iota(jnp.int32, (RB, 128), 0)
           == lax.broadcasted_iota(jnp.int32, (RB, 128), 1))

    def columns():
        for h in range(2):
            for i in range(nu):
                yield h, i, slice(h * half + i * UNIT, h * half + (i + 1) * UNIT)

    def add_early(r):
        rs = chunk_rows(r)
        for h, i, cols in columns():
            acc = p[local_unit(2, h, i), rs, :].astype(jnp.float32)
            acc += rx[(8 + h) * nu + i, rs, :].astype(jnp.float32)
            acc += rx[(4 + h * 2) * nu + i, rs, :].astype(jnp.float32)
            acc += rx[(5 + h * 2) * nu + i, rs, :].astype(jnp.float32)
            hbuf[r, :, cols] = acc + res[rs, cols].astype(jnp.float32)

    def finish(r):
        sq = jnp.zeros((RB, UNIT), jnp.float32)
        for h, i, cols in columns():
            acc = hbuf[r, :, cols] + relay_in[r, h, :, i * UNIT:(i + 1) * UNIT]
            hbuf[r, :, cols] = acc
            sq += acc * acc
        sq = jnp.sum(sq, axis=1, keepdims=True)
        packed = jnp.sum(jnp.where(eye, jnp.broadcast_to(sq, (RB, 128)), 0.0), axis=0, keepdims=True)
        sq_out[r] = packed
        sq_in[me, r] = packed

    def send_sums(lo, n, k):
        for t in range(1, tp_size):
            pltpu.make_async_remote_copy(
                src_ref=sq_out.at[pl.ds(lo, n)], dst_ref=sq_in.at[me, pl.ds(lo, n)],
                send_sem=qsend_sem.at[k], recv_sem=qrecv_sem.at[k],
                device_id={"tp": lax.rem(me + t, tp_size)}, device_id_type=MESH).start()

    def wait_sums(lo, n, sem):
        wait_bytes(sq_in.at[pl.ds(0, tp_size - 1), pl.ds(lo, n)], sem)

    def normalise(r):
        tot = sq_in[0, r]
        for t in range(1, tp_size):
            tot += sq_in[t, r]
        col = jnp.sum(jnp.where(eye, jnp.broadcast_to(tot, (RB, 128)), 0.0), axis=1, keepdims=True)
        scale = lax.rsqrt(col / d_model + EPS)
        nrm[chunk_rows(r), :] = (hbuf[r] * scale * gain[...].reshape(1, d_local)).astype(nrm.dtype)

    def write_hidden(r):
        hid[chunk_rows(r), :] = hbuf[r].astype(hid.dtype)

    last = chunks - 1

    @pl.loop(0, last)
    def _(r):
        @pl.when(r + AHEAD < chunks)
        def _():
            send_relay(r + AHEAD)

        add_early(r)
        wait_bytes(relay_in.at[r], rrecv_sem.at[r])
        finish(r)
        write_hidden(r)

    send_sums(0, last, 0)
    add_early(last)
    wait_bytes(rx, send_sem.at[0])
    wait_bytes(relay_in.at[last], rrecv_sem.at[last])
    finish(last)
    send_sums(last, 1, 1)
    write_hidden(last)
    wait_bytes(relay_out, rsend_sem.at[0])
    wait_sums(0, last, qsend_sem.at[0])
    wait_sums(0, last, qrecv_sem.at[0])

    @pl.loop(0, last)
    def _(r):
        normalise(r)

    wait_sums(last, 1, qrecv_sem.at[1])
    normalise(last)
    wait_sums(last, 1, qsend_sem.at[1])


def _write(hid, nrm, hid_hbm, nrm_hbm, sem):
    blocks = 4
    rows = hid.shape[0] // blocks
    copies = []
    for k, (src, dst) in enumerate(((hid, hid_hbm), (nrm, nrm_hbm))):
        for b in range(blocks):
            rs = pl.ds(b * rows, rows)
            copies.append(pltpu.make_async_copy(src.at[rs, :], dst.at[rs, :], sem.at[k, b]))
    for copy in copies:
        copy.start()
    for copy in copies:
        copy.wait()


def solution(mesh):
    tp_size = mesh.shape["tp"]

    def local_step(attn_blk, w_blk, resid_blk, gain_blk):
        rows, k_dim = attn_blk.shape
        d_local = resid_blk.shape[1]
        d_model = w_blk.shape[1]
        half = d_local // 2
        nu = half // UNIT
        units = tp_size * 2 * nu
        chunks = rows // RB
        assert tp_size == CORES * CHIPS and half % UNIT == 0 and rows % RB == 0
        hbm_spec = pl.BlockSpec(memory_space=pltpu.HBM)
        vmem_spec = pl.BlockSpec(memory_space=pltpu.VMEM)
        dma = pltpu.SemaphoreType.DMA
        out_shape = [jax.ShapeDtypeStruct((rows, d_local), jnp.bfloat16)] * 2
        hid, nrm = pl.pallas_call(
            functools.partial(_kernel, tp_size, d_model),
            out_shape=[pltpu.VMEM((rows, d_local), jnp.bfloat16)] * 2,
            in_specs=[hbm_spec] * 4,
            out_specs=[vmem_spec] * 2,
            scratch_shapes=[
                pltpu.VMEM((rows, k_dim), jnp.bfloat16),
                pltpu.VMEM((W_SLOTS, k_dim, UNIT), jnp.bfloat16),
                pltpu.VMEM((units, rows, UNIT), jnp.bfloat16),
                pltpu.VMEM((12 * nu, rows, UNIT), jnp.bfloat16),
                pltpu.VMEM((chunks, 2, RB, half), jnp.float32),
                pltpu.VMEM((chunks, 2, RB, half), jnp.float32),
                pltpu.VMEM((rows, d_local), jnp.bfloat16),
                pltpu.VMEM((d_local,), jnp.float32),
                pltpu.VMEM((chunks, RB, d_local), jnp.float32),
                pltpu.VMEM((chunks, 1, 128), jnp.float32),
                pltpu.VMEM((tp_size, chunks, 1, 128), jnp.float32),
                dma((A_BLOCKS,)),
                dma((2,)),
                dma((W_SLOTS,)),
                dma((1,)),
                dma((4,)),
                dma((1,)),
                dma((chunks,)),
                dma((2,)),
                dma((2,)),
            ],
            compiler_params=pltpu.CompilerParams(
                collective_id=0, has_side_effects=True, vmem_limit_bytes=62 * 1000 * 1000
            ),
            name="proj_scatter_norm",
        )(attn_blk, w_blk, resid_blk, gain_blk)
        return pl.pallas_call(
            _write,
            out_shape=out_shape,
            in_specs=[vmem_spec] * 2,
            out_specs=[hbm_spec] * 2,
            scratch_shapes=[dma((2, 4))],
            compiler_params=pltpu.CompilerParams(vmem_limit_bytes=8 * 1024 * 1024),
            name="write_out",
        )(hid, nrm)

    return jax.shard_map(
        local_step,
        mesh=mesh,
        in_specs=(P("data", "tp"), P("tp", None), P("data", "tp"), P("tp")),
        out_specs=(P("data", "tp"), P("data", "tp")),
        check_vma=False,
    )
```

```python
import functools

import jax
import jax.numpy as jnp
from jax import lax
from jax.experimental import pallas as pl
from jax.experimental.pallas import tpu as pltpu
from jax.sharding import PartitionSpec as P

EPS = 1e-5
MESH = pl.DeviceIdType.MESH
CORES = 2
CHIPS = 4
UNIT = 256
W_SLOTS = 4
RB = 32
AHEAD = 6
A_BLOCKS = 4


def _kernel(
    tp_size, d_model,
    a_hbm, w_hbm, r_hbm, g_hbm, hid, nrm,
    a, w, p, rx, relay_out, relay_in, res, gain, hbuf, sq_out, sq_in,
    a_sem, in_sem, w_sem, send_sem, recv_sem, rsend_sem, rrecv_sem, qsend_sem, qrecv_sem,
):
    rows, d_local = r_hbm.shape
    half = d_local // 2
    nu = half // UNIT
    per_group = CORES * 2 * nu
    total = CHIPS * per_group
    chunks = rows // RB
    ab = rows // A_BLOCKS

    me = lax.axis_index("tp")
    x, c = lax.div(me, CORES), lax.rem(me, CORES)

    def chip(offset, core):
        return lax.rem(x + offset, CHIPS) * CORES + core

    def decode(s):
        g, j = lax.div(s, per_group), lax.rem(s, per_group)
        i, eb, hh = lax.div(j, 4), lax.rem(lax.div(j, 2), 2), lax.rem(j, 2)
        return g, i, eb, lax.rem(eb + 1 + c, 2), lax.rem(hh + c, 2)

    def w_copy(s):
        g, i, _, e, h = decode(s)
        o = lax.rem(6 - g + 2 * h * lax.rem(g, 2), CHIPS)
        col = pl.multiple_of(chip(o, e) * d_local + h * half + i * UNIT, UNIT)
        k = lax.rem(s, W_SLOTS)
        return pltpu.make_async_copy(w_hbm.at[:, pl.ds(col, UNIT)], w.at[k], w_sem.at[k])

    def a_copy(b):
        rs = pl.ds(b * ab, ab)
        return pltpu.make_async_copy(a_hbm.at[rs, :], a.at[rs, :], a_sem.at[b])

    def send_rows(s, slot, group, target, rs):
        pltpu.make_async_remote_copy(
            src_ref=p.at[s, rs], dst_ref=rx.at[slot, rs], send_sem=send_sem.at[0], recv_sem=recv_sem.at[group],
            device_id={"tp": target}, device_id_type=MESH).start()

    def send_block(s, slot, group, target):
        send_rows(s, slot, group, target, pl.ds(0, rows))

    def wait_bytes(ref, sem):
        pltpu.make_async_copy(ref, ref, sem).wait()

    def local_unit(g, h, i):
        return g * per_group + i * 4 + 2 + lax.rem(h + c, 2)

    def send_relay(r):
        for h in range(2):
            pltpu.make_async_remote_copy(
                src_ref=relay_out.at[r, h], dst_ref=relay_in.at[r, h],
                send_sem=rsend_sem.at[0], recv_sem=rrecv_sem.at[r],
                device_id={"tp": chip(3 - 2 * h, c)}, device_id_type=MESH).start()

    def chunk_rows(r):
        return pl.ds(pl.multiple_of(r * RB, RB), RB)

    w_copy(jnp.int32(0)).start()
    a_copy(0).start()

    peers = [x * CORES + 1 - c] + [chip(o, core) for o in (1, CHIPS - 1) for core in range(CORES)]
    barrier = pltpu.get_barrier_semaphore()
    for peer in peers:
        pl.semaphore_signal(barrier, inc=1, device_id={"tp": peer}, device_id_type=MESH)

    for b in range(1, A_BLOCKS):
        a_copy(b).start()
    r_copy = pltpu.make_async_copy(r_hbm, res, in_sem.at[0])
    g_copy = pltpu.make_async_copy(g_hbm, gain, in_sem.at[1])

    _, i0, _, e0, h0 = decode(jnp.int32(0))
    w_copy(jnp.int32(0)).wait()
    for b in range(A_BLOCKS):
        a_copy(b).wait()
        if b == 0:
            for s in range(1, W_SLOTS):
                w_copy(jnp.int32(s)).start()
        rs = pl.ds(b * ab, ab)
        p[0, rs, :] = jnp.dot(a[rs, :], w[0], preferred_element_type=jnp.float32).astype(p.dtype)
        if b == 0:
            pl.semaphore_wait(barrier, len(peers))
        send_rows(0, (h0 * 2 + c) * nu + i0, 0, chip(3 + 2 * h0, e0), rs)
    w_copy(jnp.int32(W_SLOTS)).start()
    r_copy.start()
    g_copy.start()

    @pl.loop(1, total)
    def _(s):
        g, i, eb, e, h = decode(s)
        w_copy(s).wait()
        k = lax.rem(s, W_SLOTS)
        p[s] = jnp.dot(a[...], w[k], preferred_element_type=jnp.float32).astype(p.dtype)

        @pl.when(s + W_SLOTS < total)
        def _():
            w_copy(s + W_SLOTS).start()

        @pl.when(g == 0)
        def _():
            send_block(s, (h * 2 + c) * nu + i, 0, chip(3 + 2 * h, e))

        @pl.when(g == 1)
        def _():
            send_block(s, (4 + h * 2 + c) * nu + i, 1, chip(1 + 2 * h, e))

        @pl.when(jnp.logical_and(g >= 2, eb == 0))
        def _():
            send_block(s, (4 + g * 2 + h) * nu + i, g, x * CORES + 1 - c)

    wait_bytes(rx.at[pl.ds(0, 4 * nu)], recv_sem.at[0])
    wait_bytes(rx.at[pl.ds(10 * nu, 2 * nu)], recv_sem.at[3])

    @pl.loop(0, chunks)
    def _(r):
        rs = chunk_rows(r)
        for h in range(2):
            for i in range(nu):
                acc = p[local_unit(3, h, i), rs, :].astype(jnp.float32)
                acc += rx[(10 + h) * nu + i, rs, :].astype(jnp.float32)
                acc += rx[(h * 2) * nu + i, rs, :].astype(jnp.float32)
                acc += rx[(h * 2 + 1) * nu + i, rs, :].astype(jnp.float32)
                relay_out[r, h, :, i * UNIT:(i + 1) * UNIT] = acc

        @pl.when(r < AHEAD)
        def _():
            send_relay(r)

    r_copy.wait()
    g_copy.wait()
    wait_bytes(rx.at[pl.ds(8 * nu, 2 * nu)], recv_sem.at[2])
    wait_bytes(rx.at[pl.ds(4 * nu, 4 * nu)], recv_sem.at[1])

    eye = (lax.broadcasted_iota(jnp.int32, (RB, 128), 0)
           == lax.broadcasted_iota(jnp.int32, (RB, 128), 1))

    def columns():
        for h in range(2):
            for i in range(nu):
                yield h, i, slice(h * half + i * UNIT, h * half + (i + 1) * UNIT)

    def add_early(r):
        rs = chunk_rows(r)
        for h, i, cols in columns():
            acc = p[local_unit(2, h, i), rs, :].astype(jnp.float32)
            acc += rx[(8 + h) * nu + i, rs, :].astype(jnp.float32)
            acc += rx[(4 + h * 2) * nu + i, rs, :].astype(jnp.float32)
            acc += rx[(5 + h * 2) * nu + i, rs, :].astype(jnp.float32)
            hbuf[r, :, cols] = acc + res[rs, cols].astype(jnp.float32)

    def finish(r):
        sq = jnp.zeros((RB, UNIT), jnp.float32)
        for h, i, cols in columns():
            acc = hbuf[r, :, cols] + relay_in[r, h, :, i * UNIT:(i + 1) * UNIT]
            hbuf[r, :, cols] = acc
            sq += acc * acc
        sq = jnp.sum(sq, axis=1, keepdims=True)
        packed = jnp.sum(jnp.where(eye, jnp.broadcast_to(sq, (RB, 128)), 0.0), axis=0, keepdims=True)
        sq_out[r] = packed
        sq_in[me, r] = packed

    def send_sums(lo, n, k):
        for t in range(1, tp_size):
            pltpu.make_async_remote_copy(
                src_ref=sq_out.at[pl.ds(lo, n)], dst_ref=sq_in.at[me, pl.ds(lo, n)],
                send_sem=qsend_sem.at[k], recv_sem=qrecv_sem.at[k],
                device_id={"tp": lax.rem(me + t, tp_size)}, device_id_type=MESH).start()

    def wait_sums(lo, n, sem):
        wait_bytes(sq_in.at[pl.ds(0, tp_size - 1), pl.ds(lo, n)], sem)

    def normalise(r):
        tot = sq_in[0, r]
        for t in range(1, tp_size):
            tot += sq_in[t, r]
        col = jnp.sum(jnp.where(eye, jnp.broadcast_to(tot, (RB, 128)), 0.0), axis=1, keepdims=True)
        scale = lax.rsqrt(col / d_model + EPS)
        nrm[chunk_rows(r), :] = (hbuf[r] * scale * gain[...].reshape(1, d_local)).astype(nrm.dtype)

    def write_hidden(r):
        hid[chunk_rows(r), :] = hbuf[r].astype(hid.dtype)

    last = chunks - 1

    @pl.loop(0, last)
    def _(r):
        @pl.when(r + AHEAD < chunks)
        def _():
            send_relay(r + AHEAD)

        add_early(r)
        wait_bytes(relay_in.at[r], rrecv_sem.at[r])
        finish(r)
        write_hidden(r)

    send_sums(0, last, 0)
    add_early(last)
    wait_bytes(rx, send_sem.at[0])
    wait_bytes(relay_in.at[last], rrecv_sem.at[last])
    finish(last)
    send_sums(last, 1, 1)
    write_hidden(last)
    wait_bytes(relay_out, rsend_sem.at[0])
    wait_sums(0, last, qsend_sem.at[0])
    wait_sums(0, last, qrecv_sem.at[0])

    @pl.loop(0, last)
    def _(r):
        normalise(r)

    wait_sums(last, 1, qrecv_sem.at[1])
    normalise(last)
    wait_sums(last, 1, qsend_sem.at[1])


def _write(hid, nrm, hid_hbm, nrm_hbm, sem):
    blocks = 4
    rows = hid.shape[0] // blocks
    copies = []
    for k, (src, dst) in enumerate(((hid, hid_hbm), (nrm, nrm_hbm))):
        for b in range(blocks):
            rs = pl.ds(b * rows, rows)
            copies.append(pltpu.make_async_copy(src.at[rs, :], dst.at[rs, :], sem.at[k, b]))
    for copy in copies:
        copy.start()
    for copy in copies:
        copy.wait()


def solution(mesh):
    tp_size = mesh.shape["tp"]

    def local_step(attn_blk, w_blk, resid_blk, gain_blk):
        rows, k_dim = attn_blk.shape
        d_local = resid_blk.shape[1]
        d_model = w_blk.shape[1]
        half = d_local // 2
        nu = half // UNIT
        units = tp_size * 2 * nu
        chunks = rows // RB
        assert tp_size == CORES * CHIPS and half % UNIT == 0 and rows % RB == 0
        hbm_spec = pl.BlockSpec(memory_space=pltpu.HBM)
        vmem_spec = pl.BlockSpec(memory_space=pltpu.VMEM)
        dma = pltpu.SemaphoreType.DMA
        out_shape = [jax.ShapeDtypeStruct((rows, d_local), jnp.bfloat16)] * 2
        hid, nrm = pl.pallas_call(
            functools.partial(_kernel, tp_size, d_model),
            out_shape=[pltpu.VMEM((rows, d_local), jnp.bfloat16)] * 2,
            in_specs=[hbm_spec] * 4,
            out_specs=[vmem_spec] * 2,
            scratch_shapes=[
                pltpu.VMEM((rows, k_dim), jnp.bfloat16),
                pltpu.VMEM((W_SLOTS, k_dim, UNIT), jnp.bfloat16),
                pltpu.VMEM((units, rows, UNIT), jnp.bfloat16),
                pltpu.VMEM((12 * nu, rows, UNIT), jnp.bfloat16),
                pltpu.VMEM((chunks, 2, RB, half), jnp.float32),
                pltpu.VMEM((chunks, 2, RB, half), jnp.float32),
                pltpu.VMEM((rows, d_local), jnp.bfloat16),
                pltpu.VMEM((d_local,), jnp.float32),
                pltpu.VMEM((chunks, RB, d_local), jnp.float32),
                pltpu.VMEM((chunks, 1, 128), jnp.float32),
                pltpu.VMEM((tp_size, chunks, 1, 128), jnp.float32),
                dma((A_BLOCKS,)),
                dma((2,)),
                dma((W_SLOTS,)),
                dma((1,)),
                dma((4,)),
                dma((1,)),
                dma((chunks,)),
                dma((2,)),
                dma((2,)),
            ],
            compiler_params=pltpu.CompilerParams(
                collective_id=0, has_side_effects=True, vmem_limit_bytes=62 * 1000 * 1000
            ),
            name="proj_scatter_norm",
        )(attn_blk, w_blk, resid_blk, gain_blk)
        return pl.pallas_call(
            _write,
            out_shape=out_shape,
            in_specs=[vmem_spec] * 2,
            out_specs=[hbm_spec] * 2,
            scratch_shapes=[dma((2, 4))],
            compiler_params=pltpu.CompilerParams(vmem_limit_bytes=8 * 1024 * 1024),
            name="write_out",
        )(hid, nrm)

    return jax.shard_map(
        local_step,
        mesh=mesh,
        in_specs=(P("data", "tp"), P("tp", None), P("data", "tp"), P("tp")),
        out_specs=(P("data", "tp"), P("data", "tp")),
        check_vma=False,
    )
```

```python
import functools

import jax
import jax.numpy as jnp
from jax import lax
from jax.experimental import pallas as pl
from jax.experimental.pallas import tpu as pltpu
from jax.sharding import PartitionSpec as P

EPS = 1e-5
MESH = pl.DeviceIdType.MESH
CORES = 2
CHIPS = 4
UNIT = 256
W_SLOTS = 4
RB = 64
RELAY_ROWS = (256, 128, 64, 64)
FIRST_ROWS = (128, 384)


def _kernel(
    tp_size, d_model,
    a_hbm, w_hbm, r_hbm, g_hbm, hid, nrm,
    a, w, p, rx, relay_out, relay_in, res, gain, hbuf, sq_out, sq_in,
    a_sem, in_sem, w_sem, send_sem, recv_sem, rsend_sem, rrecv_sem, qsend_sem, qrecv_sem,
):
    rows, d_local = r_hbm.shape
    half = d_local // 2
    nu = half // UNIT
    per_group = CORES * 2 * nu
    total = CHIPS * per_group
    chunks = rows // RB

    me = lax.axis_index("tp")
    x, c = lax.div(me, CORES), lax.rem(me, CORES)

    def chip(offset, core):
        return lax.rem(x + offset, CHIPS) * CORES + core

    def decode(s):
        g, j = lax.div(s, per_group), lax.rem(s, per_group)
        late = lax.div(lax.div(s, 2 * nu) + 7, 8)
        more = lax.div(lax.div(s, 2) + 1, 2)
        b = late * lax.div(j, nu) + (1 - late) * ((1 - more) * s + more * (lax.div(s, 2) - 1))
        i = late * lax.rem(j, nu) + (1 - late) * more * (1 + lax.rem(s, 2))
        return g, i, b, lax.rem(lax.div(b, 2) + 1 + c, 2), lax.rem(b + c, 2)

    def w_copy(s):
        g, i, _, e, h = decode(s)
        o = lax.rem(6 - g + 2 * h * lax.rem(g, 2), CHIPS)
        col = pl.multiple_of(chip(o, e) * d_local + h * half + i * UNIT, UNIT)
        k = lax.rem(s, W_SLOTS)
        return pltpu.make_async_copy(w_hbm.at[:, pl.ds(col, UNIT)], w.at[k], w_sem.at[k])

    first_lo = [sum(FIRST_ROWS[:b]) for b in range(len(FIRST_ROWS))]

    def a_copy(b):
        rs = pl.ds(first_lo[b], FIRST_ROWS[b])
        return pltpu.make_async_copy(a_hbm.at[rs, :], a.at[rs, :], a_sem.at[b])

    def send(src, dst, group, target):
        pltpu.make_async_remote_copy(
            src_ref=src, dst_ref=dst, send_sem=send_sem.at[0], recv_sem=recv_sem.at[group],
            device_id={"tp": target}, device_id_type=MESH).start()

    def send_units(g, b, lo, n, block, group, target):
        send(p.at[pl.ds((g * 4 + b) * nu + lo, n)], rx.at[pl.ds(block * nu + lo, n)], group, target)

    def wait_bytes(ref, sem):
        pltpu.make_async_copy(ref, ref, sem).wait()

    def local_unit(g, h, i):
        return (g * 4 + 2 + lax.rem(h + c, 2)) * nu + i

    relay_lo = [sum(RELAY_ROWS[:m]) for m in range(len(RELAY_ROWS))]

    def relay_rows(m):
        return pl.ds(relay_lo[m], RELAY_ROWS[m])

    def send_relay(m):
        for h in range(2):
            pltpu.make_async_remote_copy(
                src_ref=relay_out.at[h, relay_rows(m)], dst_ref=relay_in.at[h, relay_rows(m)],
                send_sem=rsend_sem.at[0], recv_sem=rrecv_sem.at[m],
                device_id={"tp": chip(3 - 2 * h, c)}, device_id_type=MESH).start()

    def chunk_rows(r):
        return pl.ds(pl.multiple_of(r * RB, RB), RB)

    w_copy(jnp.int32(0)).start()
    a_copy(0).start()

    peers = [x * CORES + 1 - c] + [chip(o, core) for o in (1, CHIPS - 1) for core in range(CORES)]
    barrier = pltpu.get_barrier_semaphore()
    for peer in peers:
        pl.semaphore_signal(barrier, inc=1, device_id={"tp": peer}, device_id_type=MESH)

    for b in range(1, len(FIRST_ROWS)):
        a_copy(b).start()
    r_copy = pltpu.make_async_copy(r_hbm, res, in_sem.at[0])
    g_copy = pltpu.make_async_copy(g_hbm, gain, in_sem.at[1])

    _, _, _, e0, h0 = decode(jnp.int32(0))
    with jax.named_scope("w0"):
        w_copy(jnp.int32(0)).wait()
    for b in range(len(FIRST_ROWS)):
        with jax.named_scope("awt"):
            a_copy(b).wait()
        if b == 0:
            for s in range(1, W_SLOTS):
                w_copy(jnp.int32(s)).start()
        rs = pl.ds(first_lo[b], FIRST_ROWS[b])
        p[0, rs, :] = jnp.dot(a[rs, :], w[0], preferred_element_type=jnp.float32).astype(p.dtype)
        if b == 0:
            with jax.named_scope("bar"):
                pl.semaphore_wait(barrier, len(peers))
        send(p.at[0, rs], rx.at[(h0 * 2 + c) * nu, rs], 0, chip(3 + 2 * h0, e0))
    w_copy(jnp.int32(W_SLOTS)).start()
    r_copy.start()
    g_copy.start()

    @pl.loop(1, total)
    def _(s):
        g, i, b, e, h = decode(s)
        w_copy(s).wait()
        k = lax.rem(s, W_SLOTS)
        p[(g * 4 + b) * nu + i] = jnp.dot(
            a[...], w[k], preferred_element_type=jnp.float32).astype(p.dtype)

        @pl.when(s + W_SLOTS < total)
        def _():
            w_copy(s + W_SLOTS).start()

        def to_relay(lo, n):
            send_units(g, b, lo, n, h * 2 + c, 0, chip(3 + 2 * h, e))

        @pl.when(s == 1)
        def _():
            to_relay(0, 1)

        @pl.when(i == nu - 1)
        def _():
            @pl.when(s < 2 * nu)
            def _():
                to_relay(1, nu - 1)

            @pl.when(jnp.logical_and(g == 0, s >= 2 * nu))
            def _():
                to_relay(0, nu)

            @pl.when(g == 1)
            def _():
                send_units(g, b, 0, nu, 4 + h * 2 + c, 1, chip(1 + 2 * h, e))

            @pl.when(jnp.logical_and(g >= 2, b < 2))
            def _():
                send_units(g, b, 0, nu, 4 + g * 2 + h, g, x * CORES + 1 - c)

    with jax.named_scope("l2r"):
        wait_bytes(rx.at[pl.ds(0, 4 * nu)], recv_sem.at[0])
    wait_bytes(rx.at[pl.ds(10 * nu, 2 * nu)], recv_sem.at[3])

    @pl.loop(0, chunks)
    def _(r):
        rs = chunk_rows(r)
        for h in range(2):
            for i in range(nu):
                acc = p[local_unit(3, h, i), rs, :].astype(jnp.float32)
                acc += rx[(10 + h) * nu + i, rs, :].astype(jnp.float32)
                acc += rx[(h * 2) * nu + i, rs, :].astype(jnp.float32)
                acc += rx[(h * 2 + 1) * nu + i, rs, :].astype(jnp.float32)
                relay_out[h, rs, i * UNIT:(i + 1) * UNIT] = acc

    for m in range(len(RELAY_ROWS)):
        send_relay(m)

    r_copy.wait()
    g_copy.wait()
    wait_bytes(rx.at[pl.ds(8 * nu, 2 * nu)], recv_sem.at[2])
    with jax.named_scope("direct"):
        wait_bytes(rx.at[pl.ds(4 * nu, 4 * nu)], recv_sem.at[1])

    eye = (lax.broadcasted_iota(jnp.int32, (RB, 128), 0)
           == lax.broadcasted_iota(jnp.int32, (RB, 128), 1))

    def columns():
        for h in range(2):
            for i in range(nu):
                yield h, i, slice(h * half + i * UNIT, h * half + (i + 1) * UNIT)

    def add_early(r):
        rs = chunk_rows(r)
        for h, i, cols in columns():
            acc = p[local_unit(2, h, i), rs, :].astype(jnp.float32)
            acc += rx[(8 + h) * nu + i, rs, :].astype(jnp.float32)
            acc += rx[(4 + h * 2) * nu + i, rs, :].astype(jnp.float32)
            acc += rx[(5 + h * 2) * nu + i, rs, :].astype(jnp.float32)
            hbuf[r, :, cols] = acc + res[rs, cols].astype(jnp.float32)

    def finish(r):
        sq = jnp.zeros((RB, UNIT), jnp.float32)
        for h, i, cols in columns():
            acc = hbuf[r, :, cols] + relay_in[h, chunk_rows(r), i * UNIT:(i + 1) * UNIT]
            hbuf[r, :, cols] = acc
            sq += acc * acc
        sq = jnp.sum(sq, axis=1, keepdims=True)
        packed = jnp.sum(jnp.where(eye, jnp.broadcast_to(sq, (RB, 128)), 0.0), axis=0, keepdims=True)
        sq_out[r] = packed
        sq_in[me, r] = packed

    def send_sums(lo, n, k):
        for t in range(1, tp_size):
            pltpu.make_async_remote_copy(
                src_ref=sq_out.at[pl.ds(lo, n)], dst_ref=sq_in.at[me, pl.ds(lo, n)],
                send_sem=qsend_sem.at[k], recv_sem=qrecv_sem.at[k],
                device_id={"tp": lax.rem(me + t, tp_size)}, device_id_type=MESH).start()

    def wait_sums(lo, n, sem):
        wait_bytes(sq_in.at[pl.ds(0, tp_size - 1), pl.ds(lo, n)], sem)

    def normalise(r):
        tot = sq_in[0, r]
        for t in range(1, tp_size):
            tot += sq_in[t, r]
        col = jnp.sum(jnp.where(eye, jnp.broadcast_to(tot, (RB, 128)), 0.0), axis=1, keepdims=True)
        scale = lax.rsqrt(col / d_model + EPS)
        nrm[chunk_rows(r), :] = (hbuf[r] * scale * gain[...].reshape(1, d_local)).astype(nrm.dtype)

    def write_hidden(r):
        hid[chunk_rows(r), :] = hbuf[r].astype(hid.dtype)

    last = chunks - 1

    def wait_relay(m):
        wait_bytes(relay_in.at[:, relay_rows(m)], rrecv_sem.at[m])

    for m in range(len(RELAY_ROWS) - 1):
        lo = relay_lo[m] // RB
        hi = lo + RELAY_ROWS[m] // RB

        @pl.loop(lo, hi)
        def _(r):
            add_early(r)

        with jax.named_scope(f"relay{m}"):
            wait_relay(m)

        @pl.loop(lo, hi)
        def _(r):
            finish(r)
            write_hidden(r)

    send_sums(0, last, 0)
    add_early(last)
    wait_bytes(rx, send_sem.at[0])
    with jax.named_scope("rlast"):
        wait_relay(len(RELAY_ROWS) - 1)
    finish(last)
    send_sums(last, 1, 1)
    write_hidden(last)
    with jax.named_scope("drain"):
        wait_bytes(relay_out, rsend_sem.at[0])
    wait_sums(0, last, qsend_sem.at[0])
    with jax.named_scope("sqA"):
        wait_sums(0, last, qrecv_sem.at[0])

    @pl.loop(0, last)
    def _(r):
        normalise(r)

    with jax.named_scope("sqB"):
        wait_sums(last, 1, qrecv_sem.at[1])
    normalise(last)
    with jax.named_scope("qdrain"):
        wait_sums(last, 1, qsend_sem.at[1])


def _write(hid, nrm, hid_hbm, nrm_hbm, sem):
    blocks = 4
    rows = hid.shape[0] // blocks
    copies = []
    for k, (src, dst) in enumerate(((hid, hid_hbm), (nrm, nrm_hbm))):
        for b in range(blocks):
            rs = pl.ds(b * rows, rows)
            copies.append(pltpu.make_async_copy(src.at[rs, :], dst.at[rs, :], sem.at[k, b]))
    for copy in copies:
        copy.start()
    for copy in copies:
        copy.wait()


def solution(mesh):
    tp_size = mesh.shape["tp"]

    def local_step(attn_blk, w_blk, resid_blk, gain_blk):
        rows, k_dim = attn_blk.shape
        d_local = resid_blk.shape[1]
        d_model = w_blk.shape[1]
        half = d_local // 2
        nu = half // UNIT
        units = tp_size * 2 * nu
        chunks = rows // RB
        assert tp_size == CORES * CHIPS and half % UNIT == 0
        assert sum(FIRST_ROWS) == sum(RELAY_ROWS) == rows and RELAY_ROWS[-1] == RB and nu == 3
        hbm_spec = pl.BlockSpec(memory_space=pltpu.HBM)
        vmem_spec = pl.BlockSpec(memory_space=pltpu.VMEM)
        dma = pltpu.SemaphoreType.DMA
        out_shape = [jax.ShapeDtypeStruct((rows, d_local), jnp.bfloat16)] * 2
        hid, nrm = pl.pallas_call(
            functools.partial(_kernel, tp_size, d_model),
            out_shape=[pltpu.VMEM((rows, d_local), jnp.bfloat16)] * 2,
            in_specs=[hbm_spec] * 4,
            out_specs=[vmem_spec] * 2,
            scratch_shapes=[
                pltpu.VMEM((rows, k_dim), jnp.bfloat16),
                pltpu.VMEM((W_SLOTS, k_dim, UNIT), jnp.bfloat16),
                pltpu.VMEM((units, rows, UNIT), jnp.bfloat16),
                pltpu.VMEM((12 * nu, rows, UNIT), jnp.bfloat16),
                pltpu.VMEM((2, rows, half), jnp.float32),
                pltpu.VMEM((2, rows, half), jnp.float32),
                pltpu.VMEM((rows, d_local), jnp.bfloat16),
                pltpu.VMEM((d_local,), jnp.float32),
                pltpu.VMEM((chunks, RB, d_local), jnp.float32),
                pltpu.VMEM((chunks, 1, 128), jnp.float32),
                pltpu.VMEM((tp_size, chunks, 1, 128), jnp.float32),
                dma((len(FIRST_ROWS),)),
                dma((2,)),
                dma((W_SLOTS,)),
                dma((1,)),
                dma((4,)),
                dma((1,)),
                dma((len(RELAY_ROWS),)),
                dma((2,)),
                dma((2,)),
            ],
            compiler_params=pltpu.CompilerParams(
                collective_id=0, has_side_effects=True, vmem_limit_bytes=62 * 1000 * 1000
            ),
            name="proj_scatter_norm",
        )(attn_blk, w_blk, resid_blk, gain_blk)
        return pl.pallas_call(
            _write,
            out_shape=out_shape,
            in_specs=[vmem_spec] * 2,
            out_specs=[hbm_spec] * 2,
            scratch_shapes=[dma((2, 4))],
            compiler_params=pltpu.CompilerParams(vmem_limit_bytes=8 * 1024 * 1024),
            name="write_out",
        )(hid, nrm)

    return jax.shard_map(
        local_step,
        mesh=mesh,
        in_specs=(P("data", "tp"), P("tp", None), P("data", "tp"), P("tp")),
        out_specs=(P("data", "tp"), P("data", "tp")),
        check_vma=False,
    )
```

```python
import functools

import jax
import jax.numpy as jnp
from jax import lax
from jax.experimental import pallas as pl
from jax.experimental.pallas import tpu as pltpu
from jax.sharding import PartitionSpec as P

EPS = 1e-5
MESH = pl.DeviceIdType.MESH
CORES = 2
CHIPS = 4
UNIT = 256
W_SLOTS = 4
RB = 64
RELAY_ROWS = (256, 128, 64, 64)
FIRST_ROWS = (128, 384)


def _kernel(
    tp_size, d_model,
    a_hbm, w_hbm, r_hbm, g_hbm, hid, nrm,
    a, w, p, rx, relay_out, relay_in, res, gain, hbuf, sq_out, sq_in,
    a_sem, in_sem, w_sem, send_sem, recv_sem, rsend_sem, rrecv_sem, qsend_sem, qrecv_sem,
):
    rows, d_local = r_hbm.shape
    half = d_local // 2
    nu = half // UNIT
    per_group = CORES * 2 * nu
    total = CHIPS * per_group
    chunks = rows // RB

    me = lax.axis_index("tp")
    x, c = lax.div(me, CORES), lax.rem(me, CORES)

    def chip(offset, core):
        return lax.rem(x + offset, CHIPS) * CORES + core

    def decode(s):
        g, j = lax.div(s, per_group), lax.rem(s, per_group)
        late = lax.div(lax.div(s, 2 * nu) + 7, 8)
        more = lax.div(lax.div(s, 2) + 1, 2)
        b = late * lax.div(j, nu) + (1 - late) * ((1 - more) * s + more * (lax.div(s, 2) - 1))
        i = late * lax.rem(j, nu) + (1 - late) * more * (1 + lax.rem(s, 2))
        return g, i, b, lax.rem(lax.div(b, 2) + 1 + c, 2), lax.rem(b + c, 2)

    def w_copy(s):
        g, i, _, e, h = decode(s)
        o = lax.rem(6 - g + 2 * h * lax.rem(g, 2), CHIPS)
        col = pl.multiple_of(chip(o, e) * d_local + h * half + i * UNIT, UNIT)
        k = lax.rem(s, W_SLOTS)
        return pltpu.make_async_copy(w_hbm.at[:, pl.ds(col, UNIT)], w.at[k], w_sem.at[k])

    first_lo = [sum(FIRST_ROWS[:b]) for b in range(len(FIRST_ROWS))]

    def a_copy(b):
        rs = pl.ds(first_lo[b], FIRST_ROWS[b])
        return pltpu.make_async_copy(a_hbm.at[rs, :], a.at[rs, :], a_sem.at[b])

    def send(src, dst, group, target):
        pltpu.make_async_remote_copy(
            src_ref=src, dst_ref=dst, send_sem=send_sem.at[0], recv_sem=recv_sem.at[group],
            device_id={"tp": target}, device_id_type=MESH).start()

    def send_units(g, b, lo, n, block, group, target):
        send(p.at[pl.ds((g * 4 + b) * nu + lo, n)], rx.at[pl.ds(block * nu + lo, n)], group, target)

    def wait_bytes(ref, sem):
        pltpu.make_async_copy(ref, ref, sem).wait()

    def local_unit(g, h, i):
        return (g * 4 + 2 + lax.rem(h + c, 2)) * nu + i

    relay_lo = [sum(RELAY_ROWS[:m]) for m in range(len(RELAY_ROWS))]

    def relay_rows(m):
        return pl.ds(relay_lo[m], RELAY_ROWS[m])

    def send_relay(m):
        for h in range(2):
            pltpu.make_async_remote_copy(
                src_ref=relay_out.at[h, relay_rows(m)], dst_ref=relay_in.at[h, relay_rows(m)],
                send_sem=rsend_sem.at[0], recv_sem=rrecv_sem.at[m, h],
                device_id={"tp": chip(3 - 2 * h, c)}, device_id_type=MESH).start()

    def chunk_rows(r):
        return pl.ds(pl.multiple_of(r * RB, RB), RB)

    w_copy(jnp.int32(0)).start()
    a_copy(0).start()

    peers = [x * CORES + 1 - c] + [chip(o, core) for o in (1, CHIPS - 1) for core in range(CORES)]
    barrier = pltpu.get_barrier_semaphore()
    for peer in peers:
        pl.semaphore_signal(barrier, inc=1, device_id={"tp": peer}, device_id_type=MESH)

    for b in range(1, len(FIRST_ROWS)):
        a_copy(b).start()
    r_copy = pltpu.make_async_copy(r_hbm, res, in_sem.at[0])
    g_copy = pltpu.make_async_copy(g_hbm, gain, in_sem.at[1])

    _, _, _, e0, h0 = decode(jnp.int32(0))
    with jax.named_scope("w0"):
        w_copy(jnp.int32(0)).wait()
    for b in range(len(FIRST_ROWS)):
        with jax.named_scope("awt"):
            a_copy(b).wait()
        if b == 0:
            for s in range(1, W_SLOTS):
                w_copy(jnp.int32(s)).start()
        rs = pl.ds(first_lo[b], FIRST_ROWS[b])
        p[0, rs, :] = jnp.dot(a[rs, :], w[0], preferred_element_type=jnp.float32).astype(p.dtype)
        if b == 0:
            with jax.named_scope("bar"):
                pl.semaphore_wait(barrier, len(peers))
        send(p.at[0, rs], rx.at[(h0 * 2 + c) * nu, rs], 0, chip(3 + 2 * h0, e0))
    w_copy(jnp.int32(W_SLOTS)).start()
    r_copy.start()
    g_copy.start()

    @pl.loop(1, total)
    def _(s):
        g, i, b, e, h = decode(s)
        w_copy(s).wait()
        k = lax.rem(s, W_SLOTS)
        p[(g * 4 + b) * nu + i] = jnp.dot(
            a[...], w[k], preferred_element_type=jnp.float32).astype(p.dtype)

        @pl.when(s + W_SLOTS < total)
        def _():
            w_copy(s + W_SLOTS).start()

        def to_relay(lo, n):
            send_units(g, b, lo, n, h * 2 + c, 0, chip(3 + 2 * h, e))

        @pl.when(s == 1)
        def _():
            to_relay(0, 1)

        @pl.when(i == nu - 1)
        def _():
            @pl.when(s < 2 * nu)
            def _():
                to_relay(1, nu - 1)

            @pl.when(jnp.logical_and(g == 0, s >= 2 * nu))
            def _():
                to_relay(0, nu)

            @pl.when(g == 1)
            def _():
                send_units(g, b, 0, nu, 4 + h * 2 + c, 1, chip(1 + 2 * h, e))

            @pl.when(jnp.logical_and(g >= 2, b < 2))
            def _():
                send_units(g, b, 0, nu, 4 + g * 2 + h, g, x * CORES + 1 - c)

    with jax.named_scope("l2r"):
        wait_bytes(rx.at[pl.ds(0, 4 * nu)], recv_sem.at[0])
    wait_bytes(rx.at[pl.ds(10 * nu, 2 * nu)], recv_sem.at[3])

    @pl.loop(0, chunks)
    def _(r):
        rs = chunk_rows(r)
        for h in range(2):
            for i in range(nu):
                acc = p[local_unit(3, h, i), rs, :].astype(jnp.float32)
                acc += rx[(10 + h) * nu + i, rs, :].astype(jnp.float32)
                acc += rx[(h * 2) * nu + i, rs, :].astype(jnp.float32)
                acc += rx[(h * 2 + 1) * nu + i, rs, :].astype(jnp.float32)
                relay_out[h, rs, i * UNIT:(i + 1) * UNIT] = acc

    for m in range(len(RELAY_ROWS)):
        send_relay(m)

    r_copy.wait()
    g_copy.wait()
    wait_bytes(rx.at[pl.ds(8 * nu, 2 * nu)], recv_sem.at[2])
    with jax.named_scope("direct"):
        wait_bytes(rx.at[pl.ds(4 * nu, 4 * nu)], recv_sem.at[1])

    eye = (lax.broadcasted_iota(jnp.int32, (RB, 128), 0)
           == lax.broadcasted_iota(jnp.int32, (RB, 128), 1))

    def columns():
        for h in range(2):
            for i in range(nu):
                yield h, i, slice(h * half + i * UNIT, h * half + (i + 1) * UNIT)

    def add_early(r):
        rs = chunk_rows(r)
        for h, i, cols in columns():
            acc = p[local_unit(2, h, i), rs, :].astype(jnp.float32)
            acc += rx[(8 + h) * nu + i, rs, :].astype(jnp.float32)
            acc += rx[(4 + h * 2) * nu + i, rs, :].astype(jnp.float32)
            acc += rx[(5 + h * 2) * nu + i, rs, :].astype(jnp.float32)
            hbuf[r, :, cols] = acc + res[rs, cols].astype(jnp.float32)

    def finish(r):
        sq = jnp.zeros((RB, UNIT), jnp.float32)
        for h, i, cols in columns():
            acc = hbuf[r, :, cols] + relay_in[h, chunk_rows(r), i * UNIT:(i + 1) * UNIT]
            hbuf[r, :, cols] = acc
            sq += acc * acc
        sq = jnp.sum(sq, axis=1, keepdims=True)
        packed = jnp.sum(jnp.where(eye, jnp.broadcast_to(sq, (RB, 128)), 0.0), axis=0, keepdims=True)
        sq_out[r] = packed
        sq_in[me, r] = packed

    def send_sums(lo, n, k):
        for t in range(1, tp_size):
            pltpu.make_async_remote_copy(
                src_ref=sq_out.at[pl.ds(lo, n)], dst_ref=sq_in.at[me, pl.ds(lo, n)],
                send_sem=qsend_sem.at[k], recv_sem=qrecv_sem.at[k],
                device_id={"tp": lax.rem(me + t, tp_size)}, device_id_type=MESH).start()

    def wait_sums(lo, n, sem):
        wait_bytes(sq_in.at[pl.ds(0, tp_size - 1), pl.ds(lo, n)], sem)

    def normalise(r):
        tot = sq_in[0, r]
        for t in range(1, tp_size):
            tot += sq_in[t, r]
        col = jnp.sum(jnp.where(eye, jnp.broadcast_to(tot, (RB, 128)), 0.0), axis=1, keepdims=True)
        scale = lax.rsqrt(col / d_model + EPS)
        nrm[chunk_rows(r), :] = (hbuf[r] * scale * gain[...].reshape(1, d_local)).astype(nrm.dtype)

    def write_hidden(r):
        hid[chunk_rows(r), :] = hbuf[r].astype(hid.dtype)

    last = chunks - 1

    def wait_relay(m):
        for h in (1, 0):
            with jax.named_scope(f"r{m}h{h}"):
                wait_bytes(relay_in.at[h, relay_rows(m)], rrecv_sem.at[m, h])

    for m in range(len(RELAY_ROWS) - 1):
        lo = relay_lo[m] // RB
        hi = lo + RELAY_ROWS[m] // RB

        @pl.loop(lo, hi)
        def _(r):
            add_early(r)

        with jax.named_scope(f"relay{m}"):
            wait_relay(m)

        @pl.loop(lo, hi)
        def _(r):
            finish(r)
            write_hidden(r)

    send_sums(0, last, 0)
    add_early(last)
    wait_bytes(rx, send_sem.at[0])
    with jax.named_scope("rlast"):
        wait_relay(len(RELAY_ROWS) - 1)
    finish(last)
    send_sums(last, 1, 1)
    write_hidden(last)
    with jax.named_scope("drain"):
        wait_bytes(relay_out, rsend_sem.at[0])
    wait_sums(0, last, qsend_sem.at[0])
    with jax.named_scope("sqA"):
        wait_sums(0, last, qrecv_sem.at[0])

    @pl.loop(0, last)
    def _(r):
        normalise(r)

    with jax.named_scope("sqB"):
        wait_sums(last, 1, qrecv_sem.at[1])
    normalise(last)
    with jax.named_scope("qdrain"):
        wait_sums(last, 1, qsend_sem.at[1])


def _write(hid, nrm, hid_hbm, nrm_hbm, sem):
    blocks = 1
    rows = hid.shape[0] // blocks
    copies = []
    for k, (src, dst) in enumerate(((hid, hid_hbm), (nrm, nrm_hbm))):
        for b in range(blocks):
            rs = pl.ds(b * rows, rows)
            copies.append(pltpu.make_async_copy(src.at[rs, :], dst.at[rs, :], sem.at[k, b]))
    for copy in copies:
        copy.start()
    for copy in copies:
        copy.wait()


def solution(mesh):
    tp_size = mesh.shape["tp"]

    def local_step(attn_blk, w_blk, resid_blk, gain_blk):
        rows, k_dim = attn_blk.shape
        d_local = resid_blk.shape[1]
        d_model = w_blk.shape[1]
        half = d_local // 2
        nu = half // UNIT
        units = tp_size * 2 * nu
        chunks = rows // RB
        assert tp_size == CORES * CHIPS and half % UNIT == 0
        assert sum(FIRST_ROWS) == sum(RELAY_ROWS) == rows and RELAY_ROWS[-1] == RB and nu == 3
        hbm_spec = pl.BlockSpec(memory_space=pltpu.HBM)
        vmem_spec = pl.BlockSpec(memory_space=pltpu.VMEM)
        dma = pltpu.SemaphoreType.DMA
        out_shape = [jax.ShapeDtypeStruct((rows, d_local), jnp.bfloat16)] * 2
        hid, nrm = pl.pallas_call(
            functools.partial(_kernel, tp_size, d_model),
            out_shape=[pltpu.VMEM((rows, d_local), jnp.bfloat16)] * 2,
            in_specs=[hbm_spec] * 4,
            out_specs=[vmem_spec] * 2,
            scratch_shapes=[
                pltpu.VMEM((rows, k_dim), jnp.bfloat16),
                pltpu.VMEM((W_SLOTS, k_dim, UNIT), jnp.bfloat16),
                pltpu.VMEM((units, rows, UNIT), jnp.bfloat16),
                pltpu.VMEM((12 * nu, rows, UNIT), jnp.bfloat16),
                pltpu.VMEM((2, rows, half), jnp.float32),
                pltpu.VMEM((2, rows, half), jnp.float32),
                pltpu.VMEM((rows, d_local), jnp.bfloat16),
                pltpu.VMEM((d_local,), jnp.float32),
                pltpu.VMEM((chunks, RB, d_local), jnp.float32),
                pltpu.VMEM((chunks, 1, 128), jnp.float32),
                pltpu.VMEM((tp_size, chunks, 1, 128), jnp.float32),
                dma((len(FIRST_ROWS),)),
                dma((2,)),
                dma((W_SLOTS,)),
                dma((1,)),
                dma((4,)),
                dma((1,)),
                dma((len(RELAY_ROWS), 2)),
                dma((2,)),
                dma((2,)),
            ],
            compiler_params=pltpu.CompilerParams(
                collective_id=0, has_side_effects=True, vmem_limit_bytes=62 * 1000 * 1000
            ),
            name="proj_scatter_norm",
        )(attn_blk, w_blk, resid_blk, gain_blk)
        return pl.pallas_call(
            _write,
            out_shape=out_shape,
            in_specs=[vmem_spec] * 2,
            out_specs=[hbm_spec] * 2,
            scratch_shapes=[dma((2, 4))],
            compiler_params=pltpu.CompilerParams(vmem_limit_bytes=8 * 1024 * 1024),
            name="write_out",
        )(hid, nrm)

    return jax.shard_map(
        local_step,
        mesh=mesh,
        in_specs=(P("data", "tp"), P("tp", None), P("data", "tp"), P("tp")),
        out_specs=(P("data", "tp"), P("data", "tp")),
        check_vma=False,
    )
```

```python
import functools

import jax
import jax.numpy as jnp
from jax import lax
from jax.experimental import pallas as pl
from jax.experimental.pallas import tpu as pltpu
from jax.sharding import PartitionSpec as P

EPS = 1e-5
MESH = pl.DeviceIdType.MESH
CORES = 2
CHIPS = 4
UNIT = 256
W_SLOTS = 4
RB = 64
RELAY_ROWS = (256, 128, 64, 64)
FIRST_ROWS = (128, 384)


def _kernel(
    tp_size, d_model,
    a_hbm, w_hbm, r_hbm, g_hbm, hid, nrm,
    a, w, p, rx, relay_out, relay_in, res, gain, hbuf, sq_out, sq_in,
    a_sem, in_sem, w_sem, send_sem, recv_sem, rsend_sem, rrecv_sem, qsend_sem, qrecv_sem,
):
    rows, d_local = r_hbm.shape
    half = d_local // 2
    nu = half // UNIT
    per_group = CORES * 2 * nu
    total = CHIPS * per_group
    chunks = rows // RB

    me = lax.axis_index("tp")
    x, c = lax.div(me, CORES), lax.rem(me, CORES)

    def chip(offset, core):
        return lax.rem(x + offset, CHIPS) * CORES + core

    def decode(s):
        g, j = lax.div(s, per_group), lax.rem(s, per_group)
        late = lax.div(lax.div(s, 2 * nu) + 7, 8)
        more = lax.div(lax.div(s, 2) + 1, 2)
        b = late * lax.div(j, nu) + (1 - late) * ((1 - more) * s + more * (lax.div(s, 2) - 1))
        i = late * lax.rem(j, nu) + (1 - late) * more * (1 + lax.rem(s, 2))
        return g, i, b, lax.rem(lax.div(b, 2) + 1 + c, 2), lax.rem(b + 1 + c, 2)

    def w_copy(s):
        g, i, _, e, h = decode(s)
        o = lax.rem(6 - g + 2 * h * lax.rem(g, 2), CHIPS)
        col = pl.multiple_of(chip(o, e) * d_local + h * half + i * UNIT, UNIT)
        k = lax.rem(s, W_SLOTS)
        return pltpu.make_async_copy(w_hbm.at[:, pl.ds(col, UNIT)], w.at[k], w_sem.at[k])

    first_lo = [sum(FIRST_ROWS[:b]) for b in range(len(FIRST_ROWS))]

    def a_copy(b):
        rs = pl.ds(first_lo[b], FIRST_ROWS[b])
        return pltpu.make_async_copy(a_hbm.at[rs, :], a.at[rs, :], a_sem.at[b])

    def send(src, dst, group, target):
        pltpu.make_async_remote_copy(
            src_ref=src, dst_ref=dst, send_sem=send_sem.at[0], recv_sem=recv_sem.at[group],
            device_id={"tp": target}, device_id_type=MESH).start()

    def send_units(g, b, lo, n, block, group, target):
        send(p.at[pl.ds((g * 4 + b) * nu + lo, n)], rx.at[pl.ds(block * nu + lo, n)], group, target)

    def wait_bytes(ref, sem):
        pltpu.make_async_copy(ref, ref, sem).wait()

    def local_unit(g, h, i):
        return (g * 4 + 2 + lax.rem(h + 1 + c, 2)) * nu + i

    relay_lo = [sum(RELAY_ROWS[:m]) for m in range(len(RELAY_ROWS))]

    def relay_rows(m):
        return pl.ds(relay_lo[m], RELAY_ROWS[m])

    def send_relay(m):
        for h in range(2):
            pltpu.make_async_remote_copy(
                src_ref=relay_out.at[h, relay_rows(m)], dst_ref=relay_in.at[h, relay_rows(m)],
                send_sem=rsend_sem.at[0], recv_sem=rrecv_sem.at[m, h],
                device_id={"tp": chip(3 - 2 * h, c)}, device_id_type=MESH).start()

    def chunk_rows(r):
        return pl.ds(pl.multiple_of(r * RB, RB), RB)

    w_copy(jnp.int32(0)).start()
    a_copy(0).start()

    peers = [x * CORES + 1 - c] + [chip(o, core) for o in (1, CHIPS - 1) for core in range(CORES)]
    barrier = pltpu.get_barrier_semaphore()
    for peer in peers:
        pl.semaphore_signal(barrier, inc=1, device_id={"tp": peer}, device_id_type=MESH)

    for b in range(1, len(FIRST_ROWS)):
        a_copy(b).start()
    r_copy = pltpu.make_async_copy(r_hbm, res, in_sem.at[0])
    g_copy = pltpu.make_async_copy(g_hbm, gain, in_sem.at[1])

    _, _, _, e0, h0 = decode(jnp.int32(0))
    with jax.named_scope("w0"):
        w_copy(jnp.int32(0)).wait()
    for b in range(len(FIRST_ROWS)):
        with jax.named_scope("awt"):
            a_copy(b).wait()
        if b == 0:
            for s in range(1, W_SLOTS):
                w_copy(jnp.int32(s)).start()
        rs = pl.ds(first_lo[b], FIRST_ROWS[b])
        p[0, rs, :] = jnp.dot(a[rs, :], w[0], preferred_element_type=jnp.float32).astype(p.dtype)
        if b == 0:
            with jax.named_scope("bar"):
                pl.semaphore_wait(barrier, len(peers))
        send(p.at[0, rs], rx.at[(h0 * 2 + c) * nu, rs], h0, chip(3 + 2 * h0, e0))
    w_copy(jnp.int32(W_SLOTS)).start()
    r_copy.start()
    g_copy.start()

    @pl.loop(1, total)
    def _(s):
        g, i, b, e, h = decode(s)
        w_copy(s).wait()
        k = lax.rem(s, W_SLOTS)
        p[(g * 4 + b) * nu + i] = jnp.dot(
            a[...], w[k], preferred_element_type=jnp.float32).astype(p.dtype)

        @pl.when(s + W_SLOTS < total)
        def _():
            w_copy(s + W_SLOTS).start()

        def to_relay(lo, n):
            send_units(g, b, lo, n, h * 2 + c, h, chip(3 + 2 * h, e))

        @pl.when(s == 1)
        def _():
            to_relay(0, 1)

        @pl.when(i == nu - 1)
        def _():
            @pl.when(s < 2 * nu)
            def _():
                to_relay(1, nu - 1)

            @pl.when(jnp.logical_and(g == 0, s >= 2 * nu))
            def _():
                to_relay(0, nu)

            @pl.when(g == 1)
            def _():
                send_units(g, b, 0, nu, 4 + h * 2 + c, 2, chip(1 + 2 * h, e))

            @pl.when(jnp.logical_and(g >= 2, b < 2))
            def _():
                send_units(g, b, 0, nu, 4 + g * 2 + h, g + 1, x * CORES + 1 - c)

    for h in (1, 0):
        with jax.named_scope(f"l2r{h}"):
            wait_bytes(rx.at[pl.ds(2 * h * nu, 2 * nu)], recv_sem.at[h])
    wait_bytes(rx.at[pl.ds(10 * nu, 2 * nu)], recv_sem.at[4])

    @pl.loop(0, chunks)
    def _(r):
        rs = chunk_rows(r)
        for h in range(2):
            for i in range(nu):
                acc = p[local_unit(3, h, i), rs, :].astype(jnp.float32)
                acc += rx[(10 + h) * nu + i, rs, :].astype(jnp.float32)
                acc += rx[(h * 2) * nu + i, rs, :].astype(jnp.float32)
                acc += rx[(h * 2 + 1) * nu + i, rs, :].astype(jnp.float32)
                relay_out[h, rs, i * UNIT:(i + 1) * UNIT] = acc

    for m in range(len(RELAY_ROWS)):
        send_relay(m)

    r_copy.wait()
    g_copy.wait()
    wait_bytes(rx.at[pl.ds(8 * nu, 2 * nu)], recv_sem.at[3])
    with jax.named_scope("direct"):
        wait_bytes(rx.at[pl.ds(4 * nu, 4 * nu)], recv_sem.at[2])

    eye = (lax.broadcasted_iota(jnp.int32, (RB, 128), 0)
           == lax.broadcasted_iota(jnp.int32, (RB, 128), 1))

    def columns():
        for h in range(2):
            for i in range(nu):
                yield h, i, slice(h * half + i * UNIT, h * half + (i + 1) * UNIT)

    def add_early(r):
        rs = chunk_rows(r)
        for h, i, cols in columns():
            acc = p[local_unit(2, h, i), rs, :].astype(jnp.float32)
            acc += rx[(8 + h) * nu + i, rs, :].astype(jnp.float32)
            acc += rx[(4 + h * 2) * nu + i, rs, :].astype(jnp.float32)
            acc += rx[(5 + h * 2) * nu + i, rs, :].astype(jnp.float32)
            hbuf[r, :, cols] = acc + res[rs, cols].astype(jnp.float32)

    def finish(r):
        sq = jnp.zeros((RB, UNIT), jnp.float32)
        for h, i, cols in columns():
            acc = hbuf[r, :, cols] + relay_in[h, chunk_rows(r), i * UNIT:(i + 1) * UNIT]
            hbuf[r, :, cols] = acc
            sq += acc * acc
        sq = jnp.sum(sq, axis=1, keepdims=True)
        packed = jnp.sum(jnp.where(eye, jnp.broadcast_to(sq, (RB, 128)), 0.0), axis=0, keepdims=True)
        sq_out[r] = packed
        sq_in[me, r] = packed

    def send_sums(lo, n, k):
        for t in range(1, tp_size):
            pltpu.make_async_remote_copy(
                src_ref=sq_out.at[pl.ds(lo, n)], dst_ref=sq_in.at[me, pl.ds(lo, n)],
                send_sem=qsend_sem.at[k], recv_sem=qrecv_sem.at[k],
                device_id={"tp": lax.rem(me + t, tp_size)}, device_id_type=MESH).start()

    def wait_sums(lo, n, sem):
        wait_bytes(sq_in.at[pl.ds(0, tp_size - 1), pl.ds(lo, n)], sem)

    def normalise(r):
        tot = sq_in[0, r]
        for t in range(1, tp_size):
            tot += sq_in[t, r]
        col = jnp.sum(jnp.where(eye, jnp.broadcast_to(tot, (RB, 128)), 0.0), axis=1, keepdims=True)
        scale = lax.rsqrt(col / d_model + EPS)
        nrm[chunk_rows(r), :] = (hbuf[r] * scale * gain[...].reshape(1, d_local)).astype(nrm.dtype)

    def write_hidden(r):
        hid[chunk_rows(r), :] = hbuf[r].astype(hid.dtype)

    last = chunks - 1

    def wait_relay(m):
        for h in (1, 0):
            with jax.named_scope(f"r{m}h{h}"):
                wait_bytes(relay_in.at[h, relay_rows(m)], rrecv_sem.at[m, h])

    for m in range(len(RELAY_ROWS) - 1):
        lo = relay_lo[m] // RB
        hi = lo + RELAY_ROWS[m] // RB

        @pl.loop(lo, hi)
        def _(r):
            add_early(r)

        with jax.named_scope(f"relay{m}"):
            wait_relay(m)

        @pl.loop(lo, hi)
        def _(r):
            finish(r)
            write_hidden(r)

    send_sums(0, last, 0)
    add_early(last)
    wait_bytes(rx, send_sem.at[0])
    with jax.named_scope("rlast"):
        wait_relay(len(RELAY_ROWS) - 1)
    finish(last)
    send_sums(last, 1, 1)
    write_hidden(last)
    with jax.named_scope("drain"):
        wait_bytes(relay_out, rsend_sem.at[0])
    wait_sums(0, last, qsend_sem.at[0])
    with jax.named_scope("sqA"):
        wait_sums(0, last, qrecv_sem.at[0])

    @pl.loop(0, last)
    def _(r):
        normalise(r)

    with jax.named_scope("sqB"):
        wait_sums(last, 1, qrecv_sem.at[1])
    normalise(last)
    with jax.named_scope("qdrain"):
        wait_sums(last, 1, qsend_sem.at[1])


def _write(hid, nrm, hid_hbm, nrm_hbm, sem):
    blocks = 4
    rows = hid.shape[0] // blocks
    copies = []
    for k, (src, dst) in enumerate(((hid, hid_hbm), (nrm, nrm_hbm))):
        for b in range(blocks):
            rs = pl.ds(b * rows, rows)
            copies.append(pltpu.make_async_copy(src.at[rs, :], dst.at[rs, :], sem.at[k, b]))
    for copy in copies:
        copy.start()
    for copy in copies:
        copy.wait()


def solution(mesh):
    tp_size = mesh.shape["tp"]

    def local_step(attn_blk, w_blk, resid_blk, gain_blk):
        rows, k_dim = attn_blk.shape
        d_local = resid_blk.shape[1]
        d_model = w_blk.shape[1]
        half = d_local // 2
        nu = half // UNIT
        units = tp_size * 2 * nu
        chunks = rows // RB
        assert tp_size == CORES * CHIPS and half % UNIT == 0
        assert sum(FIRST_ROWS) == sum(RELAY_ROWS) == rows and RELAY_ROWS[-1] == RB and nu == 3
        hbm_spec = pl.BlockSpec(memory_space=pltpu.HBM)
        vmem_spec = pl.BlockSpec(memory_space=pltpu.VMEM)
        dma = pltpu.SemaphoreType.DMA
        out_shape = [jax.ShapeDtypeStruct((rows, d_local), jnp.bfloat16)] * 2
        hid, nrm = pl.pallas_call(
            functools.partial(_kernel, tp_size, d_model),
            out_shape=[pltpu.VMEM((rows, d_local), jnp.bfloat16)] * 2,
            in_specs=[hbm_spec] * 4,
            out_specs=[vmem_spec] * 2,
            scratch_shapes=[
                pltpu.VMEM((rows, k_dim), jnp.bfloat16),
                pltpu.VMEM((W_SLOTS, k_dim, UNIT), jnp.bfloat16),
                pltpu.VMEM((units, rows, UNIT), jnp.bfloat16),
                pltpu.VMEM((12 * nu, rows, UNIT), jnp.bfloat16),
                pltpu.VMEM((2, rows, half), jnp.float32),
                pltpu.VMEM((2, rows, half), jnp.float32),
                pltpu.VMEM((rows, d_local), jnp.bfloat16),
                pltpu.VMEM((d_local,), jnp.float32),
                pltpu.VMEM((chunks, RB, d_local), jnp.float32),
                pltpu.VMEM((chunks, 1, 128), jnp.float32),
                pltpu.VMEM((tp_size, chunks, 1, 128), jnp.float32),
                dma((len(FIRST_ROWS),)),
                dma((2,)),
                dma((W_SLOTS,)),
                dma((1,)),
                dma((5,)),
                dma((1,)),
                dma((len(RELAY_ROWS), 2)),
                dma((2,)),
                dma((2,)),
            ],
            compiler_params=pltpu.CompilerParams(
                collective_id=0, has_side_effects=True, vmem_limit_bytes=62 * 1000 * 1000
            ),
            name="proj_scatter_norm",
        )(attn_blk, w_blk, resid_blk, gain_blk)
        return pl.pallas_call(
            _write,
            out_shape=out_shape,
            in_specs=[vmem_spec] * 2,
            out_specs=[hbm_spec] * 2,
            scratch_shapes=[dma((2, 4))],
            compiler_params=pltpu.CompilerParams(vmem_limit_bytes=8 * 1024 * 1024),
            name="write_out",
        )(hid, nrm)

    return jax.shard_map(
        local_step,
        mesh=mesh,
        in_specs=(P("data", "tp"), P("tp", None), P("data", "tp"), P("tp")),
        out_specs=(P("data", "tp"), P("data", "tp")),
        check_vma=False,
    )
```

```python
import functools

import jax
import jax.numpy as jnp
from jax import lax
from jax.experimental import pallas as pl
from jax.experimental.pallas import tpu as pltpu
from jax.sharding import PartitionSpec as P

EPS = 1e-5
MESH = pl.DeviceIdType.MESH
CORES = 2
CHIPS = 4
UNIT = 256
W_SLOTS = 4
RB = 64
RELAY_ROWS = (256, 128, 96, 32)
LANES = 128
FIRST_ROWS = (128, 384)


def _kernel(
    tp_size, d_model,
    a_hbm, w_hbm, r_hbm, g_hbm, hid, nrm,
    a, w, p, rx, relay_out, relay_in, res, gain, hbuf, sq_out, sq_in,
    a_sem, in_sem, w_sem, send_sem, recv_sem, rsend_sem, rrecv_sem, qsend_sem, qrecv_sem,
):
    rows, d_local = r_hbm.shape
    half = d_local // 2
    nu = half // UNIT
    per_group = CORES * 2 * nu
    total = CHIPS * per_group
    chunks = rows // RB

    me = lax.axis_index("tp")
    x, c = lax.div(me, CORES), lax.rem(me, CORES)

    flip = lax.div(CHIPS - x, CHIPS)

    def chip(offset, core):
        return lax.rem(x + offset, CHIPS) * CORES + core

    def decode(s):
        g, j = lax.div(s, per_group), lax.rem(s, per_group)
        late = lax.div(lax.div(s, 2 * nu) + 7, 8)
        more = lax.div(lax.div(s, 2) + 1, 2)
        b = late * lax.div(j, nu) + (1 - late) * ((1 - more) * s + more * (lax.div(s, 2) - 1))
        i = late * lax.rem(j, nu) + (1 - late) * more * (1 + lax.rem(s, 2))
        return g, i, b, lax.rem(lax.div(b, 2) + 1 + c, 2), lax.rem(b + c + flip, 2)

    def w_copy(s):
        g, i, _, e, h = decode(s)
        o = lax.rem(6 - g + 2 * h * lax.rem(g, 2), CHIPS)
        col = pl.multiple_of(chip(o, e) * d_local + h * half + i * UNIT, UNIT)
        k = lax.rem(s, W_SLOTS)
        return pltpu.make_async_copy(w_hbm.at[:, pl.ds(col, UNIT)], w.at[k], w_sem.at[k])

    first_lo = [sum(FIRST_ROWS[:b]) for b in range(len(FIRST_ROWS))]

    def a_copy(b):
        rs = pl.ds(first_lo[b], FIRST_ROWS[b])
        return pltpu.make_async_copy(a_hbm.at[rs, :], a.at[rs, :], a_sem.at[b])

    def send(src, dst, group, target):
        pltpu.make_async_remote_copy(
            src_ref=src, dst_ref=dst, send_sem=send_sem.at[0], recv_sem=recv_sem.at[group],
            device_id={"tp": target}, device_id_type=MESH).start()

    def send_units(g, b, lo, n, block, group, target):
        send(p.at[pl.ds((g * 4 + b) * nu + lo, n)], rx.at[pl.ds(block * nu + lo, n)], group, target)

    def wait_bytes(ref, sem):
        pltpu.make_async_copy(ref, ref, sem).wait()

    def local_unit(g, h, i):
        return (g * 4 + 2 + lax.rem(h + c + flip, 2)) * nu + i

    relay_lo = [sum(RELAY_ROWS[:m]) for m in range(len(RELAY_ROWS))]

    def relay_rows(m):
        return pl.ds(relay_lo[m], RELAY_ROWS[m])

    def send_relay(m):
        for h in range(2):
            pltpu.make_async_remote_copy(
                src_ref=relay_out.at[h, relay_rows(m)], dst_ref=relay_in.at[h, relay_rows(m)],
                send_sem=rsend_sem.at[0], recv_sem=rrecv_sem.at[m, h],
                device_id={"tp": chip(3 - 2 * h, c)}, device_id_type=MESH).start()

    def chunk_rows(r):
        return pl.ds(pl.multiple_of(r * RB, RB), RB)

    def span(lo, n):
        return pl.ds(pl.multiple_of(lo, n), n)

    w_copy(jnp.int32(0)).start()
    a_copy(0).start()

    peers = [x * CORES + 1 - c] + [chip(o, core) for o in (1, CHIPS - 1) for core in range(CORES)]
    barrier = pltpu.get_barrier_semaphore()
    for peer in peers:
        pl.semaphore_signal(barrier, inc=1, device_id={"tp": peer}, device_id_type=MESH)

    for b in range(1, len(FIRST_ROWS)):
        a_copy(b).start()
    r_copy = pltpu.make_async_copy(r_hbm, res, in_sem.at[0])
    g_copy = pltpu.make_async_copy(g_hbm, gain, in_sem.at[1])

    _, _, _, e0, h0 = decode(jnp.int32(0))
    with jax.named_scope("w0"):
        w_copy(jnp.int32(0)).wait()
    for b in range(len(FIRST_ROWS)):
        with jax.named_scope("awt"):
            a_copy(b).wait()
        if b == 0:
            for s in range(1, W_SLOTS):
                w_copy(jnp.int32(s)).start()
        rs = pl.ds(first_lo[b], FIRST_ROWS[b])
        p[0, rs, :] = jnp.dot(a[rs, :], w[0], preferred_element_type=jnp.float32).astype(p.dtype)
        if b == 0:
            with jax.named_scope("bar"):
                pl.semaphore_wait(barrier, len(peers))
        send(p.at[0, rs], rx.at[(h0 * 2 + c) * nu, rs], h0, chip(3 + 2 * h0, e0))
    w_copy(jnp.int32(W_SLOTS)).start()
    r_copy.start()
    g_copy.start()

    @pl.loop(1, total)
    def _(s):
        g, i, b, e, h = decode(s)
        w_copy(s).wait()
        k = lax.rem(s, W_SLOTS)
        p[(g * 4 + b) * nu + i] = jnp.dot(
            a[...], w[k], preferred_element_type=jnp.float32).astype(p.dtype)

        @pl.when(s + W_SLOTS < total)
        def _():
            w_copy(s + W_SLOTS).start()

        def to_relay(lo, n):
            send_units(g, b, lo, n, h * 2 + c, h, chip(3 + 2 * h, e))

        @pl.when(s == 1)
        def _():
            to_relay(0, 1)

        @pl.when(i == nu - 1)
        def _():
            @pl.when(s < 2 * nu)
            def _():
                to_relay(1, nu - 1)

            @pl.when(jnp.logical_and(g == 0, s >= 2 * nu))
            def _():
                to_relay(0, nu)

            @pl.when(g == 1)
            def _():
                send_units(g, b, 0, nu, 4 + h * 2 + c, 2, chip(1 + 2 * h, e))

            @pl.when(jnp.logical_and(g >= 2, b < 2))
            def _():
                send_units(g, b, 0, nu, 4 + g * 2 + h, g + 1, x * CORES + 1 - c)

    for h in (1, 0):
        with jax.named_scope(f"l2r{h}"):
            wait_bytes(rx.at[pl.ds(2 * h * nu, 2 * nu)], recv_sem.at[h])
    wait_bytes(rx.at[pl.ds(10 * nu, 2 * nu)], recv_sem.at[4])

    @pl.loop(0, chunks)
    def _(r):
        rs = chunk_rows(r)
        for h in range(2):
            for i in range(nu):
                acc = p[local_unit(3, h, i), rs, :].astype(jnp.float32)
                acc += rx[(10 + h) * nu + i, rs, :].astype(jnp.float32)
                acc += rx[(h * 2) * nu + i, rs, :].astype(jnp.float32)
                acc += rx[(h * 2 + 1) * nu + i, rs, :].astype(jnp.float32)
                relay_out[h, rs, i * UNIT:(i + 1) * UNIT] = acc

    for m in range(len(RELAY_ROWS)):
        send_relay(m)

    r_copy.wait()
    g_copy.wait()
    wait_bytes(rx.at[pl.ds(8 * nu, 2 * nu)], recv_sem.at[3])
    with jax.named_scope("direct"):
        wait_bytes(rx.at[pl.ds(4 * nu, 4 * nu)], recv_sem.at[2])

    early_rows = rows - RELAY_ROWS[-1]
    sq_rows = -(-early_rows // LANES)

    def place(lo):
        if isinstance(lo, int) and lo >= early_rows:
            return sq_rows, lo - early_rows
        return lax.div(lo, LANES), lax.rem(lo, LANES)

    def on_lane(lane, n):
        return (lax.broadcasted_iota(jnp.int32, (n, LANES), 0) + lane
                == lax.broadcasted_iota(jnp.int32, (n, LANES), 1))

    def columns():
        for h in range(2):
            for i in range(nu):
                yield h, i, slice(h * half + i * UNIT, h * half + (i + 1) * UNIT)

    def add_early(lo, n):
        rs = span(lo, n)
        for h, i, cols in columns():
            acc = p[local_unit(2, h, i), rs, :].astype(jnp.float32)
            acc += rx[(8 + h) * nu + i, rs, :].astype(jnp.float32)
            acc += rx[(4 + h * 2) * nu + i, rs, :].astype(jnp.float32)
            acc += rx[(5 + h * 2) * nu + i, rs, :].astype(jnp.float32)
            hbuf[rs, cols] = acc + res[rs, cols].astype(jnp.float32)

    def finish(lo, n):
        rs = span(lo, n)
        sq = jnp.zeros((n, UNIT), jnp.float32)
        for h, i, cols in columns():
            acc = hbuf[rs, cols] + relay_in[h, rs, i * UNIT:(i + 1) * UNIT]
            hbuf[rs, cols] = acc
            sq += acc * acc
        sq = jnp.sum(sq, axis=1, keepdims=True)
        q, lane = place(lo)
        sq_out[q] += jnp.sum(
            jnp.where(on_lane(lane, n), jnp.broadcast_to(sq, (n, LANES)), 0.0), axis=0, keepdims=True)

    def send_sums(lo, n, k):
        for offset in (2, 1, 3):
            for core in range(CORES):
                send_sum(lo, n, k, chip(offset, core))
        send_sum(lo, n, k, x * CORES + 1 - c)

    def send_sum(lo, n, k, target):
        pltpu.make_async_remote_copy(
            src_ref=sq_out.at[pl.ds(lo, n)], dst_ref=sq_in.at[me, pl.ds(lo, n)],
            send_sem=qsend_sem.at[k], recv_sem=qrecv_sem.at[k],
            device_id={"tp": target}, device_id_type=MESH).start()

    def wait_sums(lo, n, sem):
        wait_bytes(sq_in.at[pl.ds(0, tp_size - 1), pl.ds(lo, n)], sem)

    def normalise(lo, n):
        q, lane = place(lo)
        tot = sq_in[0, q]
        for t in range(1, tp_size):
            tot += sq_in[t, q]
        col = jnp.sum(jnp.where(on_lane(lane, n), jnp.broadcast_to(tot, (n, LANES)), 0.0), axis=1, keepdims=True)
        scale = lax.rsqrt(col / d_model + EPS)
        rs = span(lo, n)
        nrm[rs, :] = (hbuf[rs, :] * scale * gain[...].reshape(1, d_local)).astype(nrm.dtype)

    def write_hidden(lo, n):
        rs = span(lo, n)
        hid[rs, :] = hbuf[rs, :].astype(hid.dtype)

    def each(lo, hi, *steps):
        whole = (hi - lo) // RB * RB

        if whole:
            @pl.loop(0, whole // RB)
            def _(r):
                for step in steps:
                    step(lo + r * RB, RB)

        if lo + whole < hi:
            for step in steps:
                step(lo + whole, hi - lo - whole)

    def wait_relay(m):
        for h in (1, 0):
            with jax.named_scope(f"r{m}h{h}"):
                wait_bytes(relay_in.at[h, relay_rows(m)], rrecv_sem.at[m, h])

    for q in range(sq_rows + 1):
        sq_out[q] = jnp.zeros((1, LANES), jnp.float32)
    for m in range(len(RELAY_ROWS) - 1):
        lo, hi = relay_lo[m], relay_lo[m] + RELAY_ROWS[m]
        each(lo, hi, add_early)
        wait_relay(m)
        each(lo, hi, finish, write_hidden)

    send_sums(0, sq_rows, 0)
    for q in range(sq_rows):
        sq_in[me, q] = sq_out[q]
    each(early_rows, rows, add_early)
    wait_bytes(rx, send_sem.at[0])
    with jax.named_scope("rlast"):
        wait_relay(len(RELAY_ROWS) - 1)
    each(early_rows, rows, finish)
    send_sums(sq_rows, 1, 1)
    sq_in[me, sq_rows] = sq_out[sq_rows]
    each(early_rows, rows, write_hidden)
    with jax.named_scope("drain"):
        wait_bytes(relay_out, rsend_sem.at[0])
    wait_sums(0, sq_rows, qsend_sem.at[0])
    with jax.named_scope("sqA"):
        wait_sums(0, sq_rows, qrecv_sem.at[0])
    each(0, early_rows, normalise)
    with jax.named_scope("sqB"):
        wait_sums(sq_rows, 1, qrecv_sem.at[1])
    each(early_rows, rows, normalise)
    with jax.named_scope("qdrain"):
        wait_sums(sq_rows, 1, qsend_sem.at[1])


def _write(hid, nrm, hid_hbm, nrm_hbm, sem):
    blocks = 4
    rows = hid.shape[0] // blocks
    copies = []
    for k, (src, dst) in enumerate(((hid, hid_hbm), (nrm, nrm_hbm))):
        for b in range(blocks):
            rs = pl.ds(b * rows, rows)
            copies.append(pltpu.make_async_copy(src.at[rs, :], dst.at[rs, :], sem.at[k, b]))
    for copy in copies:
        copy.start()
    for copy in copies:
        copy.wait()


def solution(mesh):
    tp_size = mesh.shape["tp"]

    def local_step(attn_blk, w_blk, resid_blk, gain_blk):
        rows, k_dim = attn_blk.shape
        d_local = resid_blk.shape[1]
        d_model = w_blk.shape[1]
        half = d_local // 2
        nu = half // UNIT
        units = tp_size * 2 * nu
        sq_rows = -(-(rows - RELAY_ROWS[-1]) // LANES) + 1
        assert tp_size == CORES * CHIPS and half % UNIT == 0
        assert sum(FIRST_ROWS) == sum(RELAY_ROWS) == rows and rows % RB == 0 and nu == 3
        hbm_spec = pl.BlockSpec(memory_space=pltpu.HBM)
        vmem_spec = pl.BlockSpec(memory_space=pltpu.VMEM)
        dma = pltpu.SemaphoreType.DMA
        out_shape = [jax.ShapeDtypeStruct((rows, d_local), jnp.bfloat16)] * 2
        hid, nrm = pl.pallas_call(
            functools.partial(_kernel, tp_size, d_model),
            out_shape=[pltpu.VMEM((rows, d_local), jnp.bfloat16)] * 2,
            in_specs=[hbm_spec] * 4,
            out_specs=[vmem_spec] * 2,
            scratch_shapes=[
                pltpu.VMEM((rows, k_dim), jnp.bfloat16),
                pltpu.VMEM((W_SLOTS, k_dim, UNIT), jnp.bfloat16),
                pltpu.VMEM((units, rows, UNIT), jnp.bfloat16),
                pltpu.VMEM((12 * nu, rows, UNIT), jnp.bfloat16),
                pltpu.VMEM((2, rows, half), jnp.float32),
                pltpu.VMEM((2, rows, half), jnp.float32),
                pltpu.VMEM((rows, d_local), jnp.bfloat16),
                pltpu.VMEM((d_local,), jnp.float32),
                pltpu.VMEM((rows, d_local), jnp.float32),
                pltpu.VMEM((sq_rows, 1, LANES), jnp.float32),
                pltpu.VMEM((tp_size, sq_rows, 1, LANES), jnp.float32),
                dma((len(FIRST_ROWS),)),
                dma((2,)),
                dma((W_SLOTS,)),
                dma((1,)),
                dma((5,)),
                dma((1,)),
                dma((len(RELAY_ROWS), 2)),
                dma((2,)),
                dma((2,)),
            ],
            compiler_params=pltpu.CompilerParams(
                collective_id=0, has_side_effects=True, vmem_limit_bytes=62 * 1000 * 1000
            ),
            name="proj_scatter_norm",
        )(attn_blk, w_blk, resid_blk, gain_blk)
        return pl.pallas_call(
            _write,
            out_shape=out_shape,
            in_specs=[vmem_spec] * 2,
            out_specs=[hbm_spec] * 2,
            scratch_shapes=[dma((2, 4))],
            compiler_params=pltpu.CompilerParams(vmem_limit_bytes=8 * 1024 * 1024),
            name="write_out",
        )(hid, nrm)

    return jax.shard_map(
        local_step,
        mesh=mesh,
        in_specs=(P("data", "tp"), P("tp", None), P("data", "tp"), P("tp")),
        out_specs=(P("data", "tp"), P("data", "tp")),
        check_vma=False,
    )
```

```python
import functools

import jax
import jax.numpy as jnp
from jax import lax
from jax.experimental import pallas as pl
from jax.experimental.pallas import tpu as pltpu
from jax.sharding import PartitionSpec as P

EPS = 1e-5
MESH = pl.DeviceIdType.MESH
CORES = 2
CHIPS = 4
UNIT = 256
W_SLOTS = 4
RB = 64
RELAY_ROWS = (256, 128, 96, 32)
LANES = 128
FIRST_ROWS = (128, 384)


def sum_rows():
    n = [-(-r // LANES) for r in RELAY_ROWS]
    return n, [sum(n[:m]) for m in range(len(n))]


def _kernel(
    tp_size, d_model,
    a_hbm, w_hbm, r_hbm, g_hbm, hid, nrm,
    a, w, p, rx, relay_out, relay_in, res, gain, hbuf, sq_out, sq_in,
    a_sem, in_sem, w_sem, send_sem, recv_sem, rsend_sem, rrecv_sem, qsend_sem, qrecv_sem,
):
    rows, d_local = r_hbm.shape
    half = d_local // 2
    nu = half // UNIT
    per_group = CORES * 2 * nu
    total = CHIPS * per_group
    chunks = rows // RB

    me = lax.axis_index("tp")
    x, c = lax.div(me, CORES), lax.rem(me, CORES)

    flip = lax.div(CHIPS - x, CHIPS)

    def chip(offset, core):
        return lax.rem(x + offset, CHIPS) * CORES + core

    def decode(s):
        g, j = lax.div(s, per_group), lax.rem(s, per_group)
        late = lax.div(lax.div(s, 2 * nu) + 7, 8)
        more = lax.div(lax.div(s, 2) + 1, 2)
        b = late * lax.div(j, nu) + (1 - late) * ((1 - more) * s + more * (lax.div(s, 2) - 1))
        i = late * lax.rem(j, nu) + (1 - late) * more * (1 + lax.rem(s, 2))
        return g, i, b, lax.rem(lax.div(b, 2) + 1 + c, 2), lax.rem(b + c + flip, 2)

    def w_copy(s):
        g, i, _, e, h = decode(s)
        o = lax.rem(6 - g + 2 * h * lax.rem(g, 2), CHIPS)
        col = pl.multiple_of(chip(o, e) * d_local + h * half + i * UNIT, UNIT)
        k = lax.rem(s, W_SLOTS)
        return pltpu.make_async_copy(w_hbm.at[:, pl.ds(col, UNIT)], w.at[k], w_sem.at[k])

    first_lo = [sum(FIRST_ROWS[:b]) for b in range(len(FIRST_ROWS))]

    def a_copy(b):
        rs = pl.ds(first_lo[b], FIRST_ROWS[b])
        return pltpu.make_async_copy(a_hbm.at[rs, :], a.at[rs, :], a_sem.at[b])

    def send(src, dst, group, target):
        pltpu.make_async_remote_copy(
            src_ref=src, dst_ref=dst, send_sem=send_sem.at[0], recv_sem=recv_sem.at[group],
            device_id={"tp": target}, device_id_type=MESH).start()

    def send_units(g, b, lo, n, block, group, target):
        send(p.at[pl.ds((g * 4 + b) * nu + lo, n)], rx.at[pl.ds(block * nu + lo, n)], group, target)

    def wait_bytes(ref, sem):
        pltpu.make_async_copy(ref, ref, sem).wait()

    def local_unit(g, h, i):
        return (g * 4 + 2 + lax.rem(h + c + flip, 2)) * nu + i

    relay_lo = [sum(RELAY_ROWS[:m]) for m in range(len(RELAY_ROWS))]

    def relay_rows(m):
        return pl.ds(relay_lo[m], RELAY_ROWS[m])

    def send_relay(m):
        for h in range(2):
            pltpu.make_async_remote_copy(
                src_ref=relay_out.at[h, relay_rows(m)], dst_ref=relay_in.at[h, relay_rows(m)],
                send_sem=rsend_sem.at[0], recv_sem=rrecv_sem.at[m, h],
                device_id={"tp": chip(3 - 2 * h, c)}, device_id_type=MESH).start()

    def chunk_rows(r):
        return pl.ds(pl.multiple_of(r * RB, RB), RB)

    def span(lo, n):
        return pl.ds(pl.multiple_of(lo, n), n)

    w_copy(jnp.int32(0)).start()
    a_copy(0).start()

    peers = [x * CORES + 1 - c] + [chip(o, core) for o in (1, CHIPS - 1) for core in range(CORES)]
    barrier = pltpu.get_barrier_semaphore()
    for peer in peers:
        pl.semaphore_signal(barrier, inc=1, device_id={"tp": peer}, device_id_type=MESH)

    for b in range(1, len(FIRST_ROWS)):
        a_copy(b).start()
    r_copy = pltpu.make_async_copy(r_hbm, res, in_sem.at[0])
    g_copy = pltpu.make_async_copy(g_hbm, gain, in_sem.at[1])

    _, _, _, e0, h0 = decode(jnp.int32(0))
    with jax.named_scope("w0"):
        w_copy(jnp.int32(0)).wait()
    for b in range(len(FIRST_ROWS)):
        with jax.named_scope("awt"):
            a_copy(b).wait()
        if b == 0:
            for s in range(1, W_SLOTS):
                w_copy(jnp.int32(s)).start()
        rs = pl.ds(first_lo[b], FIRST_ROWS[b])
        p[0, rs, :] = jnp.dot(a[rs, :], w[0], preferred_element_type=jnp.float32).astype(p.dtype)
        if b == 0:
            with jax.named_scope("bar"):
                pl.semaphore_wait(barrier, len(peers))
        send(p.at[0, rs], rx.at[(h0 * 2 + c) * nu, rs], h0, chip(3 + 2 * h0, e0))
    w_copy(jnp.int32(W_SLOTS)).start()
    r_copy.start()
    g_copy.start()

    @pl.loop(1, total)
    def _(s):
        g, i, b, e, h = decode(s)
        w_copy(s).wait()
        k = lax.rem(s, W_SLOTS)
        p[(g * 4 + b) * nu + i] = jnp.dot(
            a[...], w[k], preferred_element_type=jnp.float32).astype(p.dtype)

        @pl.when(s + W_SLOTS < total)
        def _():
            w_copy(s + W_SLOTS).start()

        def to_relay(lo, n):
            send_units(g, b, lo, n, h * 2 + c, h, chip(3 + 2 * h, e))

        @pl.when(s == 1)
        def _():
            to_relay(0, 1)

        @pl.when(i == nu - 1)
        def _():
            @pl.when(s < 2 * nu)
            def _():
                to_relay(1, nu - 1)

            @pl.when(jnp.logical_and(g == 0, s >= 2 * nu))
            def _():
                to_relay(0, nu)

            @pl.when(g == 1)
            def _():
                send_units(g, b, 0, nu, 4 + h * 2 + c, 2, chip(1 + 2 * h, e))

            @pl.when(jnp.logical_and(g >= 2, b < 2))
            def _():
                send_units(g, b, 0, nu, 4 + g * 2 + h, g + 1, x * CORES + 1 - c)

    for h in (1, 0):
        with jax.named_scope(f"l2r{h}"):
            wait_bytes(rx.at[pl.ds(2 * h * nu, 2 * nu)], recv_sem.at[h])
    wait_bytes(rx.at[pl.ds(10 * nu, 2 * nu)], recv_sem.at[4])

    @pl.loop(0, chunks)
    def _(r):
        rs = chunk_rows(r)
        for h in range(2):
            for i in range(nu):
                acc = p[local_unit(3, h, i), rs, :].astype(jnp.float32)
                acc += rx[(10 + h) * nu + i, rs, :].astype(jnp.float32)
                acc += rx[(h * 2) * nu + i, rs, :].astype(jnp.float32)
                acc += rx[(h * 2 + 1) * nu + i, rs, :].astype(jnp.float32)
                relay_out[h, rs, i * UNIT:(i + 1) * UNIT] = acc

    for m in range(len(RELAY_ROWS)):
        send_relay(m)

    r_copy.wait()
    g_copy.wait()
    wait_bytes(rx.at[pl.ds(8 * nu, 2 * nu)], recv_sem.at[3])
    with jax.named_scope("direct"):
        wait_bytes(rx.at[pl.ds(4 * nu, 4 * nu)], recv_sem.at[2])

    sq_n, sq_lo = sum_rows()

    def on_lane(lane, n):
        return (lax.broadcasted_iota(jnp.int32, (n, LANES), 0) + lane
                == lax.broadcasted_iota(jnp.int32, (n, LANES), 1))

    def columns():
        for h in range(2):
            for i in range(nu):
                yield h, i, slice(h * half + i * UNIT, h * half + (i + 1) * UNIT)

    def add_early(lo, n):
        rs = span(lo, n)
        for h, i, cols in columns():
            acc = p[local_unit(2, h, i), rs, :].astype(jnp.float32)
            acc += rx[(8 + h) * nu + i, rs, :].astype(jnp.float32)
            acc += rx[(4 + h * 2) * nu + i, rs, :].astype(jnp.float32)
            acc += rx[(5 + h * 2) * nu + i, rs, :].astype(jnp.float32)
            hbuf[rs, cols] = acc + res[rs, cols].astype(jnp.float32)

    def finish(m, lo, n):
        rs = span(lo, n)
        sq = jnp.zeros((n, UNIT), jnp.float32)
        for h, i, cols in columns():
            acc = hbuf[rs, cols] + relay_in[h, rs, i * UNIT:(i + 1) * UNIT]
            hbuf[rs, cols] = acc
            sq += acc * acc
        sq = jnp.sum(sq, axis=1, keepdims=True)
        q, lane = place(m, lo)
        sq_out[q] += jnp.sum(
            jnp.where(on_lane(lane, n), jnp.broadcast_to(sq, (n, LANES)), 0.0), axis=0, keepdims=True)

    def place(m, lo):
        lo = lo - relay_lo[m]
        return sq_lo[m] + lax.div(lo, LANES), lax.rem(lo, LANES)

    def send_sums(m):
        def send_to(target):
            pltpu.make_async_remote_copy(
                src_ref=sq_out.at[sq_span(m)], dst_ref=sq_in.at[me, sq_span(m)],
                send_sem=qsend_sem.at[m], recv_sem=qrecv_sem.at[m],
                device_id={"tp": target}, device_id_type=MESH).start()

        for offset in (2, 1, 3):
            for core in range(CORES):
                send_to(chip(offset, core))
        send_to(x * CORES + 1 - c)
        for q in range(sq_lo[m], sq_lo[m] + sq_n[m]):
            sq_in[me, q] = sq_out[q]

    def sq_span(m):
        return pl.ds(sq_lo[m], sq_n[m])

    def wait_sums(m, sem):
        wait_bytes(sq_in.at[pl.ds(0, tp_size - 1), sq_span(m)], sem.at[m])

    def normalise(m, lo, n):
        q, lane = place(m, lo)
        tot = sq_in[0, q]
        for t in range(1, tp_size):
            tot += sq_in[t, q]
        col = jnp.sum(jnp.where(on_lane(lane, n), jnp.broadcast_to(tot, (n, LANES)), 0.0), axis=1, keepdims=True)
        scale = lax.rsqrt(col / d_model + EPS)
        rs = span(lo, n)
        nrm[rs, :] = (hbuf[rs, :] * scale * gain[...].reshape(1, d_local)).astype(nrm.dtype)

    def write_hidden(lo, n):
        rs = span(lo, n)
        hid[rs, :] = hbuf[rs, :].astype(hid.dtype)

    def each(m, *steps):
        lo, hi = relay_lo[m], relay_lo[m] + RELAY_ROWS[m]
        whole = (hi - lo) // RB * RB

        if whole:
            @pl.loop(0, whole // RB)
            def _(r):
                for step in steps:
                    step(lo + r * RB, RB)

        if lo + whole < hi:
            for step in steps:
                step(lo + whole, hi - lo - whole)

    def wait_relay(m):
        for h in (1, 0):
            with jax.named_scope(f"r{m}h{h}"):
                wait_bytes(relay_in.at[h, relay_rows(m)], rrecv_sem.at[m, h])

    for q in range(sum(sq_n)):
        sq_out[q] = jnp.zeros((1, LANES), jnp.float32)
    last = len(RELAY_ROWS) - 1
    for m in range(last + 1):
        each(m, add_early)
        if m == last:
            wait_bytes(rx, send_sem.at[0])
        wait_relay(m)
        each(m, functools.partial(finish, m))
        send_sums(m)
        each(m, write_hidden)

    wait_bytes(relay_out, rsend_sem.at[0])
    for m in range(last):
        wait_sums(m, qsend_sem)
    for m in range(last + 1):
        with jax.named_scope(f"sq{m}"):
            wait_sums(m, qrecv_sem)
        each(m, functools.partial(normalise, m))
    with jax.named_scope("qdrain"):
        wait_sums(last, qsend_sem)


def _write(hid, nrm, hid_hbm, nrm_hbm, sem):
    blocks = 4
    rows = hid.shape[0] // blocks
    copies = []
    for k, (src, dst) in enumerate(((hid, hid_hbm), (nrm, nrm_hbm))):
        for b in range(blocks):
            rs = pl.ds(b * rows, rows)
            copies.append(pltpu.make_async_copy(src.at[rs, :], dst.at[rs, :], sem.at[k, b]))
    for copy in copies:
        copy.start()
    for copy in copies:
        copy.wait()


def solution(mesh):
    tp_size = mesh.shape["tp"]

    def local_step(attn_blk, w_blk, resid_blk, gain_blk):
        rows, k_dim = attn_blk.shape
        d_local = resid_blk.shape[1]
        d_model = w_blk.shape[1]
        half = d_local // 2
        nu = half // UNIT
        units = tp_size * 2 * nu
        sq_rows = sum(sum_rows()[0])
        assert tp_size == CORES * CHIPS and half % UNIT == 0
        assert sum(FIRST_ROWS) == sum(RELAY_ROWS) == rows and rows % RB == 0 and nu == 3
        hbm_spec = pl.BlockSpec(memory_space=pltpu.HBM)
        vmem_spec = pl.BlockSpec(memory_space=pltpu.VMEM)
        dma = pltpu.SemaphoreType.DMA
        out_shape = [jax.ShapeDtypeStruct((rows, d_local), jnp.bfloat16)] * 2
        hid, nrm = pl.pallas_call(
            functools.partial(_kernel, tp_size, d_model),
            out_shape=[pltpu.VMEM((rows, d_local), jnp.bfloat16)] * 2,
            in_specs=[hbm_spec] * 4,
            out_specs=[vmem_spec] * 2,
            scratch_shapes=[
                pltpu.VMEM((rows, k_dim), jnp.bfloat16),
                pltpu.VMEM((W_SLOTS, k_dim, UNIT), jnp.bfloat16),
                pltpu.VMEM((units, rows, UNIT), jnp.bfloat16),
                pltpu.VMEM((12 * nu, rows, UNIT), jnp.bfloat16),
                pltpu.VMEM((2, rows, half), jnp.float32),
                pltpu.VMEM((2, rows, half), jnp.float32),
                pltpu.VMEM((rows, d_local), jnp.bfloat16),
                pltpu.VMEM((d_local,), jnp.float32),
                pltpu.VMEM((rows, d_local), jnp.float32),
                pltpu.VMEM((sq_rows, 1, LANES), jnp.float32),
                pltpu.VMEM((tp_size, sq_rows, 1, LANES), jnp.float32),
                dma((len(FIRST_ROWS),)),
                dma((2,)),
                dma((W_SLOTS,)),
                dma((1,)),
                dma((5,)),
                dma((1,)),
                dma((len(RELAY_ROWS), 2)),
                dma((len(RELAY_ROWS),)),
                dma((len(RELAY_ROWS),)),
            ],
            compiler_params=pltpu.CompilerParams(
                collective_id=0, has_side_effects=True, vmem_limit_bytes=62 * 1000 * 1000
            ),
            name="proj_scatter_norm",
        )(attn_blk, w_blk, resid_blk, gain_blk)
        return pl.pallas_call(
            _write,
            out_shape=out_shape,
            in_specs=[vmem_spec] * 2,
            out_specs=[hbm_spec] * 2,
            scratch_shapes=[dma((2, 4))],
            compiler_params=pltpu.CompilerParams(vmem_limit_bytes=8 * 1024 * 1024),
            name="write_out",
        )(hid, nrm)

    return jax.shard_map(
        local_step,
        mesh=mesh,
        in_specs=(P("data", "tp"), P("tp", None), P("data", "tp"), P("tp")),
        out_specs=(P("data", "tp"), P("data", "tp")),
        check_vma=False,
    )
```

```python
import functools

import jax
import jax.numpy as jnp
from jax import lax
from jax.experimental import pallas as pl
from jax.experimental.pallas import tpu as pltpu
from jax.sharding import PartitionSpec as P

EPS = 1e-5
MESH = pl.DeviceIdType.MESH
CORES = 2
CHIPS = 4
UNIT = 256
W_SLOTS = 4
RB = 64
RELAY_ROWS = (256, 192, 64)
LANES = 128
FIRST_ROWS = (128, 384)


def sum_rows():
    return -(-sum(RELAY_ROWS[:-1]) // LANES), -(-RELAY_ROWS[-1] // LANES)


def _kernel(
    tp_size, d_model,
    a_hbm, w_hbm, r_hbm, g_hbm, hid, nrm,
    a, w, p, rx, relay_out, relay_in, res, gain, hbuf, sq_out, sq_in,
    a_sem, in_sem, w_sem, send_sem, recv_sem, rsend_sem, rrecv_sem, qsend_sem, qrecv_sem,
):
    rows, d_local = r_hbm.shape
    half = d_local // 2
    nu = half // UNIT
    per_group = CORES * 2 * nu
    total = CHIPS * per_group
    chunks = rows // RB

    me = lax.axis_index("tp")
    x, c = lax.div(me, CORES), lax.rem(me, CORES)

    flip = lax.div(CHIPS - x, CHIPS)

    def chip(offset, core):
        return lax.rem(x + offset, CHIPS) * CORES + core

    def decode(s):
        g, j = lax.div(s, per_group), lax.rem(s, per_group)
        late = lax.div(lax.div(s, 2 * nu) + 7, 8)
        more = lax.div(lax.div(s, 2) + 1, 2)
        b = late * lax.div(j, nu) + (1 - late) * ((1 - more) * s + more * (lax.div(s, 2) - 1))
        i = late * lax.rem(j, nu) + (1 - late) * more * (1 + lax.rem(s, 2))
        return g, i, b, lax.rem(lax.div(b, 2) + 1 + c, 2), lax.rem(b + c + flip, 2)

    def w_copy(s):
        g, i, _, e, h = decode(s)
        o = lax.rem(6 - g + 2 * h * lax.rem(g, 2), CHIPS)
        col = pl.multiple_of(chip(o, e) * d_local + h * half + i * UNIT, UNIT)
        k = lax.rem(s, W_SLOTS)
        return pltpu.make_async_copy(w_hbm.at[:, pl.ds(col, UNIT)], w.at[k], w_sem.at[k])

    first_lo = [sum(FIRST_ROWS[:b]) for b in range(len(FIRST_ROWS))]

    def a_copy(b):
        rs = pl.ds(first_lo[b], FIRST_ROWS[b])
        return pltpu.make_async_copy(a_hbm.at[rs, :], a.at[rs, :], a_sem.at[b])

    def send(src, dst, group, target):
        pltpu.make_async_remote_copy(
            src_ref=src, dst_ref=dst, send_sem=send_sem.at[0], recv_sem=recv_sem.at[group],
            device_id={"tp": target}, device_id_type=MESH).start()

    def send_units(g, b, lo, n, block, group, target):
        send(p.at[pl.ds((g * 4 + b) * nu + lo, n)], rx.at[pl.ds(block * nu + lo, n)], group, target)

    def wait_bytes(ref, sem):
        pltpu.make_async_copy(ref, ref, sem).wait()

    def local_unit(g, h, i):
        return (g * 4 + 2 + lax.rem(h + c + flip, 2)) * nu + i

    relay_lo = [sum(RELAY_ROWS[:m]) for m in range(len(RELAY_ROWS))]

    def relay_rows(m):
        return pl.ds(relay_lo[m], RELAY_ROWS[m])

    def send_relay(m):
        for h in range(2):
            pltpu.make_async_remote_copy(
                src_ref=relay_out.at[h, relay_rows(m)], dst_ref=relay_in.at[h, relay_rows(m)],
                send_sem=rsend_sem.at[0], recv_sem=rrecv_sem.at[m, h],
                device_id={"tp": chip(3 - 2 * h, c)}, device_id_type=MESH).start()

    def chunk_rows(r):
        return pl.ds(pl.multiple_of(r * RB, RB), RB)

    def span(lo, n):
        return pl.ds(pl.multiple_of(lo, n), n)

    for s in range(2):
        w_copy(jnp.int32(s)).start()
        if s == 0:
            a_copy(0).start()

    peers = [x * CORES + 1 - c] + [chip(o, core) for o in (1, CHIPS - 1) for core in range(CORES)]
    barrier = pltpu.get_barrier_semaphore()
    for peer in peers:
        pl.semaphore_signal(barrier, inc=1, device_id={"tp": peer}, device_id_type=MESH)

    r_copy = pltpu.make_async_copy(r_hbm, res, in_sem.at[0])
    g_copy = pltpu.make_async_copy(g_hbm, gain, in_sem.at[1])

    for b in range(len(FIRST_ROWS)):
        rs = pl.ds(first_lo[b], FIRST_ROWS[b])
        for s in range(2):
            _, _, block, e0, h0 = decode(jnp.int32(s))
            if b == 0:
                with jax.named_scope(f"w{s}"):
                    w_copy(jnp.int32(s)).wait()
            if s == 0:
                with jax.named_scope("awt"):
                    a_copy(b).wait()
            if b == 0 and s == 0:
                for k in range(1, len(FIRST_ROWS)):
                    a_copy(k).start()
                for k in range(2, W_SLOTS):
                    w_copy(jnp.int32(k)).start()
            unit = block * nu
            p[unit, rs, :] = jnp.dot(a[rs, :], w[s], preferred_element_type=jnp.float32).astype(p.dtype)
            if b == 0 and s == 0:
                with jax.named_scope("bar"):
                    pl.semaphore_wait(barrier, len(peers))
            send(p.at[unit, rs], rx.at[(h0 * 2 + c) * nu, rs], h0, chip(3 + 2 * h0, e0))
    for s in range(2):
        w_copy(jnp.int32(s + W_SLOTS)).start()
    r_copy.start()
    g_copy.start()

    @pl.loop(2, total)
    def _(s):
        g, i, b, e, h = decode(s)
        w_copy(s).wait()
        k = lax.rem(s, W_SLOTS)
        p[(g * 4 + b) * nu + i] = jnp.dot(
            a[...], w[k], preferred_element_type=jnp.float32).astype(p.dtype)

        @pl.when(s + W_SLOTS < total)
        def _():
            w_copy(s + W_SLOTS).start()

        def to_relay(lo, n):
            send_units(g, b, lo, n, h * 2 + c, h, chip(3 + 2 * h, e))

        @pl.when(i == nu - 1)
        def _():
            @pl.when(s < 2 * nu)
            def _():
                to_relay(1, nu - 1)

            @pl.when(jnp.logical_and(g == 0, s >= 2 * nu))
            def _():
                to_relay(0, nu)

            @pl.when(g == 1)
            def _():
                send_units(g, b, 0, nu, 4 + h * 2 + c, 2, chip(1 + 2 * h, e))

            @pl.when(jnp.logical_and(g >= 2, b < 2))
            def _():
                send_units(g, b, 0, nu, 4 + g * 2 + h, g + 1, x * CORES + 1 - c)

    for h in (1, 0):
        with jax.named_scope(f"l2r{h}"):
            wait_bytes(rx.at[pl.ds(2 * h * nu, 2 * nu)], recv_sem.at[h])
    wait_bytes(rx.at[pl.ds(10 * nu, 2 * nu)], recv_sem.at[4])

    @pl.loop(0, chunks)
    def _(r):
        rs = chunk_rows(r)
        for h in range(2):
            for i in range(nu):
                acc = p[local_unit(3, h, i), rs, :].astype(jnp.float32)
                acc += rx[(10 + h) * nu + i, rs, :].astype(jnp.float32)
                acc += rx[(h * 2) * nu + i, rs, :].astype(jnp.float32)
                acc += rx[(h * 2 + 1) * nu + i, rs, :].astype(jnp.float32)
                relay_out[h, rs, i * UNIT:(i + 1) * UNIT] = acc

    for m in range(len(RELAY_ROWS)):
        send_relay(m)

    r_copy.wait()
    g_copy.wait()
    wait_bytes(rx.at[pl.ds(8 * nu, 2 * nu)], recv_sem.at[3])
    with jax.named_scope("direct"):
        wait_bytes(rx.at[pl.ds(4 * nu, 4 * nu)], recv_sem.at[2])

    sq_n = sum_rows()
    sq_lo = (0, sq_n[0])

    def on_lane(lane, n):
        return (lax.broadcasted_iota(jnp.int32, (n, LANES), 0) + lane
                == lax.broadcasted_iota(jnp.int32, (n, LANES), 1))

    def columns():
        for h in range(2):
            for i in range(nu):
                yield h, i, slice(h * half + i * UNIT, h * half + (i + 1) * UNIT)

    def add_early(lo, n):
        rs = span(lo, n)
        for h, i, cols in columns():
            acc = p[local_unit(2, h, i), rs, :].astype(jnp.float32)
            acc += rx[(8 + h) * nu + i, rs, :].astype(jnp.float32)
            acc += rx[(4 + h * 2) * nu + i, rs, :].astype(jnp.float32)
            acc += rx[(5 + h * 2) * nu + i, rs, :].astype(jnp.float32)
            hbuf[rs, cols] = acc + res[rs, cols].astype(jnp.float32)

    def finish(m, lo, n):
        rs = span(lo, n)
        sq = jnp.zeros((n, UNIT), jnp.float32)
        for h, i, cols in columns():
            acc = hbuf[rs, cols] + relay_in[h, rs, i * UNIT:(i + 1) * UNIT]
            hbuf[rs, cols] = acc
            sq += acc * acc
        sq = jnp.sum(sq, axis=1, keepdims=True)
        q, lane = place(m, lo)
        sq_out[q] += jnp.sum(
            jnp.where(on_lane(lane, n), jnp.broadcast_to(sq, (n, LANES)), 0.0), axis=0, keepdims=True)

    def place(m, lo):
        if m == len(RELAY_ROWS) - 1:
            lo = lo - relay_lo[m]
            return sq_lo[1] + lax.div(lo, LANES), lax.rem(lo, LANES)
        return lax.div(lo, LANES), lax.rem(lo, LANES)

    def send_sums(k):
        def send_to(target):
            pltpu.make_async_remote_copy(
                src_ref=sq_out.at[sq_span(k)], dst_ref=sq_in.at[me, sq_span(k)],
                send_sem=qsend_sem.at[k], recv_sem=qrecv_sem.at[k],
                device_id={"tp": target}, device_id_type=MESH).start()

        for offset in (2, 1, 3):
            for core in range(CORES):
                send_to(chip(offset, core))
        send_to(x * CORES + 1 - c)
        for q in range(sq_lo[k], sq_lo[k] + sq_n[k]):
            sq_in[me, q] = sq_out[q]

    def sq_span(k):
        return pl.ds(sq_lo[k], sq_n[k])

    def wait_sums(k, sem):
        wait_bytes(sq_in.at[pl.ds(0, tp_size - 1), sq_span(k)], sem.at[k])

    def normalise(m, lo, n):
        q, lane = place(m, lo)
        tot = sq_in[0, q]
        for t in range(1, tp_size):
            tot += sq_in[t, q]
        col = jnp.sum(jnp.where(on_lane(lane, n), jnp.broadcast_to(tot, (n, LANES)), 0.0), axis=1, keepdims=True)
        scale = lax.rsqrt(col / d_model + EPS)
        rs = span(lo, n)
        nrm[rs, :] = (hbuf[rs, :] * scale * gain[...].reshape(1, d_local)).astype(nrm.dtype)

    def write_hidden(lo, n):
        rs = span(lo, n)
        hid[rs, :] = hbuf[rs, :].astype(hid.dtype)

    def each(m, *steps):
        lo, hi = relay_lo[m], relay_lo[m] + RELAY_ROWS[m]
        whole = (hi - lo) // RB * RB

        if whole:
            @pl.loop(0, whole // RB)
            def _(r):
                for step in steps:
                    step(lo + r * RB, RB)

        if lo + whole < hi:
            for step in steps:
                step(lo + whole, hi - lo - whole)

    def wait_relay(m):
        for h in (1, 0):
            with jax.named_scope(f"r{m}h{h}"):
                wait_bytes(relay_in.at[h, relay_rows(m)], rrecv_sem.at[m, h])

    for q in range(sum(sq_n)):
        sq_out[q] = jnp.zeros((1, LANES), jnp.float32)
    last = len(RELAY_ROWS) - 1
    for m in range(last + 1):
        each(m, add_early)
        if m == last:
            wait_bytes(rx, send_sem.at[0])
        wait_relay(m)
        each(m, functools.partial(finish, m))
        if m >= last - 1:
            send_sums(m - last + 1)
        each(m, write_hidden)

    wait_bytes(relay_out, rsend_sem.at[0])
    wait_sums(0, qsend_sem)
    for m in range(last + 1):
        if m in (0, last):
            with jax.named_scope(f"sq{m}"):
                wait_sums(min(m, 1), qrecv_sem)
        each(m, functools.partial(normalise, m))
    with jax.named_scope("qdrain"):
        wait_sums(1, qsend_sem)


def _write(hid, nrm, hid_hbm, nrm_hbm, sem):
    blocks = 4
    rows = hid.shape[0] // blocks
    copies = []
    for k, (src, dst) in enumerate(((hid, hid_hbm), (nrm, nrm_hbm))):
        for b in range(blocks):
            rs = pl.ds(b * rows, rows)
            copies.append(pltpu.make_async_copy(src.at[rs, :], dst.at[rs, :], sem.at[k, b]))
    for copy in copies:
        copy.start()
    for copy in copies:
        copy.wait()


def solution(mesh):
    tp_size = mesh.shape["tp"]

    def local_step(attn_blk, w_blk, resid_blk, gain_blk):
        rows, k_dim = attn_blk.shape
        d_local = resid_blk.shape[1]
        d_model = w_blk.shape[1]
        half = d_local // 2
        nu = half // UNIT
        units = tp_size * 2 * nu
        sq_rows = sum(sum_rows())
        assert tp_size == CORES * CHIPS and half % UNIT == 0
        assert sum(FIRST_ROWS) == sum(RELAY_ROWS) == rows and rows % RB == 0 and nu == 3
        hbm_spec = pl.BlockSpec(memory_space=pltpu.HBM)
        vmem_spec = pl.BlockSpec(memory_space=pltpu.VMEM)
        dma = pltpu.SemaphoreType.DMA
        out_shape = [jax.ShapeDtypeStruct((rows, d_local), jnp.bfloat16)] * 2
        hid, nrm = pl.pallas_call(
            functools.partial(_kernel, tp_size, d_model),
            out_shape=[pltpu.VMEM((rows, d_local), jnp.bfloat16)] * 2,
            in_specs=[hbm_spec] * 4,
            out_specs=[vmem_spec] * 2,
            scratch_shapes=[
                pltpu.VMEM((rows, k_dim), jnp.bfloat16),
                pltpu.VMEM((W_SLOTS, k_dim, UNIT), jnp.bfloat16),
                pltpu.VMEM((units, rows, UNIT), jnp.bfloat16),
                pltpu.VMEM((12 * nu, rows, UNIT), jnp.bfloat16),
                pltpu.VMEM((2, rows, half), jnp.float32),
                pltpu.VMEM((2, rows, half), jnp.float32),
                pltpu.VMEM((rows, d_local), jnp.bfloat16),
                pltpu.VMEM((d_local,), jnp.float32),
                pltpu.VMEM((rows, d_local), jnp.float32),
                pltpu.VMEM((sq_rows, 1, LANES), jnp.float32),
                pltpu.VMEM((tp_size, sq_rows, 1, LANES), jnp.float32),
                dma((len(FIRST_ROWS),)),
                dma((2,)),
                dma((W_SLOTS,)),
                dma((1,)),
                dma((5,)),
                dma((1,)),
                dma((len(RELAY_ROWS), 2)),
                dma((2,)),
                dma((2,)),
            ],
            compiler_params=pltpu.CompilerParams(
                collective_id=0, has_side_effects=True, vmem_limit_bytes=62 * 1000 * 1000
            ),
            name="proj_scatter_norm",
        )(attn_blk, w_blk, resid_blk, gain_blk)
        return pl.pallas_call(
            _write,
            out_shape=out_shape,
            in_specs=[vmem_spec] * 2,
            out_specs=[hbm_spec] * 2,
            scratch_shapes=[dma((2, 4))],
            compiler_params=pltpu.CompilerParams(vmem_limit_bytes=8 * 1024 * 1024),
            name="write_out",
        )(hid, nrm)

    return jax.shard_map(
        local_step,
        mesh=mesh,
        in_specs=(P("data", "tp"), P("tp", None), P("data", "tp"), P("tp")),
        out_specs=(P("data", "tp"), P("data", "tp")),
        check_vma=False,
    )
```

```python
import functools

import jax
import jax.numpy as jnp
from jax import lax
from jax.experimental import pallas as pl
from jax.experimental.pallas import tpu as pltpu
from jax.sharding import PartitionSpec as P

EPS = 1e-5
MESH = pl.DeviceIdType.MESH
CORES = 2
CHIPS = 4
UNIT = 256
W_SLOTS = 4
RB = 64
RELAY_ROWS = (256, 192, 64)
LANES = 128
FIRST_ROWS = (128, 384)


def sum_rows():
    return -(-sum(RELAY_ROWS[:-1]) // LANES), -(-RELAY_ROWS[-1] // LANES)


def _kernel(
    tp_size, d_model,
    a_hbm, w_hbm, r_hbm, g_hbm, hid, nrm,
    a, w, p, rx, relay_out, relay_in, res, gain, hbuf, sq_out, sq_in,
    a_sem, in_sem, w_sem, send_sem, recv_sem, rsend_sem, rrecv_sem, qsend_sem, qrecv_sem,
):
    rows, d_local = r_hbm.shape
    half = d_local // 2
    nu = half // UNIT
    per_group = CORES * 2 * nu
    total = CHIPS * per_group
    chunks = rows // RB

    me = lax.axis_index("tp")
    x, c = lax.div(me, CORES), lax.rem(me, CORES)

    flip = lax.div(CHIPS - x, CHIPS)

    def chip(offset, core):
        return lax.rem(x + offset, CHIPS) * CORES + core

    def decode(s):
        g, j = lax.div(s, per_group), lax.rem(s, per_group)
        late = lax.div(lax.div(s, 2 * nu) + 7, 8)
        more = lax.div(lax.div(s, 2) + 1, 2)
        b = late * lax.div(j, nu) + (1 - late) * ((1 - more) * s + more * (lax.div(s, 2) - 1))
        i = late * lax.rem(j, nu) + (1 - late) * more * (1 + lax.rem(s, 2))
        return g, i, b, lax.rem(lax.div(b, 2) + 1 + c, 2), lax.rem(b + c + flip, 2)

    def w_copy(s):
        g, i, _, e, h = decode(s)
        o = lax.rem(6 - g + 2 * h * lax.rem(g, 2), CHIPS)
        col = pl.multiple_of(chip(o, e) * d_local + h * half + i * UNIT, UNIT)
        k = lax.rem(s, W_SLOTS)
        return pltpu.make_async_copy(w_hbm.at[:, pl.ds(col, UNIT)], w.at[k], w_sem.at[k])

    first_lo = [sum(FIRST_ROWS[:b]) for b in range(len(FIRST_ROWS))]

    def a_copy(b):
        rs = pl.ds(first_lo[b], FIRST_ROWS[b])
        return pltpu.make_async_copy(a_hbm.at[rs, :], a.at[rs, :], a_sem.at[b])

    def send(src, dst, group, target):
        pltpu.make_async_remote_copy(
            src_ref=src, dst_ref=dst, send_sem=send_sem.at[0], recv_sem=recv_sem.at[group],
            device_id={"tp": target}, device_id_type=MESH).start()

    def send_units(g, b, lo, n, block, group, target):
        send(p.at[pl.ds((g * 4 + b) * nu + lo, n)], rx.at[pl.ds(block * nu + lo, n)], group, target)

    def wait_bytes(ref, sem):
        pltpu.make_async_copy(ref, ref, sem).wait()

    def local_unit(g, h, i):
        return (g * 4 + 2 + lax.rem(h + c + flip, 2)) * nu + i

    relay_lo = [sum(RELAY_ROWS[:m]) for m in range(len(RELAY_ROWS))]

    def relay_rows(m):
        return pl.ds(relay_lo[m], RELAY_ROWS[m])

    def send_relay(m):
        for h in range(2):
            pltpu.make_async_remote_copy(
                src_ref=relay_out.at[h, relay_rows(m)], dst_ref=relay_in.at[h, relay_rows(m)],
                send_sem=rsend_sem.at[0], recv_sem=rrecv_sem.at[m, h],
                device_id={"tp": chip(3 - 2 * h, c)}, device_id_type=MESH).start()

    def chunk_rows(r):
        return pl.ds(pl.multiple_of(r * RB, RB), RB)

    def span(lo, n):
        return pl.ds(pl.multiple_of(lo, n), n)

    w_copy(jnp.int32(0)).start()
    a_copy(0).start()
    w_copy(jnp.int32(1)).start()

    peers = [x * CORES + 1 - c] + [chip(o, core) for o in (1, CHIPS - 1) for core in range(CORES)]
    barrier = pltpu.get_barrier_semaphore()
    for peer in peers:
        pl.semaphore_signal(barrier, inc=1, device_id={"tp": peer}, device_id_type=MESH)

    for b in range(1, len(FIRST_ROWS)):
        a_copy(b).start()
    r_copy = pltpu.make_async_copy(r_hbm, res, in_sem.at[0])
    g_copy = pltpu.make_async_copy(g_hbm, gain, in_sem.at[1])

    for b in range(len(FIRST_ROWS)):
        rs = pl.ds(first_lo[b], FIRST_ROWS[b])
        for s in range(2):
            _, _, block, e0, h0 = decode(jnp.int32(s))
            if b == 0:
                with jax.named_scope(f"w{s}"):
                    w_copy(jnp.int32(s)).wait()
            if s == 0:
                with jax.named_scope("awt"):
                    a_copy(b).wait()
            if b == 0 and s == 0:
                for k in range(2, W_SLOTS):
                    w_copy(jnp.int32(k)).start()
            unit = block * nu
            p[unit, rs, :] = jnp.dot(a[rs, :], w[s], preferred_element_type=jnp.float32).astype(p.dtype)
            if b == 0 and s == 0:
                with jax.named_scope("bar"):
                    pl.semaphore_wait(barrier, len(peers))
            send(p.at[unit, rs], rx.at[(h0 * 2 + c) * nu, rs], h0, chip(3 + 2 * h0, e0))
    for s in range(2):
        w_copy(jnp.int32(s + W_SLOTS)).start()
    r_copy.start()
    g_copy.start()

    @pl.loop(2, total)
    def _(s):
        g, i, b, e, h = decode(s)
        w_copy(s).wait()
        k = lax.rem(s, W_SLOTS)
        p[(g * 4 + b) * nu + i] = jnp.dot(
            a[...], w[k], preferred_element_type=jnp.float32).astype(p.dtype)

        @pl.when(s + W_SLOTS < total)
        def _():
            w_copy(s + W_SLOTS).start()

        def to_relay(lo, n):
            send_units(g, b, lo, n, h * 2 + c, h, chip(3 + 2 * h, e))

        @pl.when(i == nu - 1)
        def _():
            @pl.when(s < 2 * nu)
            def _():
                to_relay(1, nu - 1)

            @pl.when(jnp.logical_and(g == 0, s >= 2 * nu))
            def _():
                to_relay(0, nu)

            @pl.when(g == 1)
            def _():
                send_units(g, b, 0, nu, 4 + h * 2 + c, 2, chip(1 + 2 * h, e))

            @pl.when(jnp.logical_and(g >= 2, b < 2))
            def _():
                send_units(g, b, 0, nu, 4 + g * 2 + h, g + 1, x * CORES + 1 - c)

    for h in (1, 0):
        with jax.named_scope(f"l2r{h}"):
            wait_bytes(rx.at[pl.ds(2 * h * nu, 2 * nu)], recv_sem.at[h])
    wait_bytes(rx.at[pl.ds(10 * nu, 2 * nu)], recv_sem.at[4])

    @pl.loop(0, chunks)
    def _(r):
        rs = chunk_rows(r)
        for h in range(2):
            for i in range(nu):
                acc = p[local_unit(3, h, i), rs, :].astype(jnp.float32)
                acc += rx[(10 + h) * nu + i, rs, :].astype(jnp.float32)
                acc += rx[(h * 2) * nu + i, rs, :].astype(jnp.float32)
                acc += rx[(h * 2 + 1) * nu + i, rs, :].astype(jnp.float32)
                relay_out[h, rs, i * UNIT:(i + 1) * UNIT] = acc

    for m in range(len(RELAY_ROWS)):
        send_relay(m)

    r_copy.wait()
    g_copy.wait()
    wait_bytes(rx.at[pl.ds(8 * nu, 2 * nu)], recv_sem.at[3])
    with jax.named_scope("direct"):
        wait_bytes(rx.at[pl.ds(4 * nu, 4 * nu)], recv_sem.at[2])

    sq_n = sum_rows()
    sq_lo = (0, sq_n[0])

    def on_lane(lane, n):
        return (lax.broadcasted_iota(jnp.int32, (n, LANES), 0) + lane
                == lax.broadcasted_iota(jnp.int32, (n, LANES), 1))

    def columns():
        for h in range(2):
            for i in range(nu):
                yield h, i, slice(h * half + i * UNIT, h * half + (i + 1) * UNIT)

    def add_early(lo, n):
        rs = span(lo, n)
        for h, i, cols in columns():
            acc = p[local_unit(2, h, i), rs, :].astype(jnp.float32)
            acc += rx[(8 + h) * nu + i, rs, :].astype(jnp.float32)
            acc += rx[(4 + h * 2) * nu + i, rs, :].astype(jnp.float32)
            acc += rx[(5 + h * 2) * nu + i, rs, :].astype(jnp.float32)
            hbuf[rs, cols] = acc + res[rs, cols].astype(jnp.float32)

    def finish(m, lo, n):
        rs = span(lo, n)
        sq = jnp.zeros((n, UNIT), jnp.float32)
        for h, i, cols in columns():
            acc = hbuf[rs, cols] + relay_in[h, rs, i * UNIT:(i + 1) * UNIT]
            hbuf[rs, cols] = acc
            sq += acc * acc
        sq = jnp.sum(sq, axis=1, keepdims=True)
        q, lane = place(m, lo)
        sq_out[q] += jnp.sum(
            jnp.where(on_lane(lane, n), jnp.broadcast_to(sq, (n, LANES)), 0.0), axis=0, keepdims=True)

    def place(m, lo):
        if m == len(RELAY_ROWS) - 1:
            lo = lo - relay_lo[m]
            return sq_lo[1] + lax.div(lo, LANES), lax.rem(lo, LANES)
        return lax.div(lo, LANES), lax.rem(lo, LANES)

    others = [(o, core) for o in (2, 1, 3) for core in range(CORES)] + [(0, 1 - c)]

    def send_sums(k):
        for n, (o, core) in enumerate(others):
            slot = ((CHIPS - o) % CHIPS) * CORES + c if o else c
            pltpu.make_async_remote_copy(
                src_ref=sq_out.at[sq_span(k)], dst_ref=sq_in.at[me, sq_span(k)],
                send_sem=qsend_sem.at[k], recv_sem=qrecv_sem.at[k, slot],
                device_id={"tp": chip(o, core)}, device_id_type=MESH).start()
        for q in range(sq_lo[k], sq_lo[k] + sq_n[k]):
            sq_in[me, q] = sq_out[q]

    def sq_span(k):
        return pl.ds(sq_lo[k], sq_n[k])

    def wait_sent(k):
        wait_bytes(sq_in.at[pl.ds(0, tp_size - 1), sq_span(k)], qsend_sem.at[k])

    def wait_sums(k):
        for o, core in others[::-1]:
            with jax.named_scope(f"q{k}o{o}c{core if o else 'x'}"):
                wait_bytes(sq_in.at[0, sq_span(k)], qrecv_sem.at[k, o * CORES + core])

    def normalise(m, lo, n):
        q, lane = place(m, lo)
        tot = sq_in[0, q]
        for t in range(1, tp_size):
            tot += sq_in[t, q]
        col = jnp.sum(jnp.where(on_lane(lane, n), jnp.broadcast_to(tot, (n, LANES)), 0.0), axis=1, keepdims=True)
        scale = lax.rsqrt(col / d_model + EPS)
        rs = span(lo, n)
        nrm[rs, :] = (hbuf[rs, :] * scale * gain[...].reshape(1, d_local)).astype(nrm.dtype)

    def write_hidden(lo, n):
        rs = span(lo, n)
        hid[rs, :] = hbuf[rs, :].astype(hid.dtype)

    def each(m, *steps):
        lo, hi = relay_lo[m], relay_lo[m] + RELAY_ROWS[m]
        whole = (hi - lo) // RB * RB

        if whole:
            @pl.loop(0, whole // RB)
            def _(r):
                for step in steps:
                    step(lo + r * RB, RB)

        if lo + whole < hi:
            for step in steps:
                step(lo + whole, hi - lo - whole)

    def wait_relay(m):
        for h in (1, 0):
            with jax.named_scope(f"r{m}h{h}"):
                wait_bytes(relay_in.at[h, relay_rows(m)], rrecv_sem.at[m, h])

    for q in range(sum(sq_n)):
        sq_out[q] = jnp.zeros((1, LANES), jnp.float32)
    last = len(RELAY_ROWS) - 1
    for m in range(last + 1):
        each(m, add_early)
        if m == last:
            wait_bytes(rx, send_sem.at[0])
        wait_relay(m)
        each(m, functools.partial(finish, m))
        if m >= last - 1:
            send_sums(m - last + 1)
        each(m, write_hidden)

    wait_bytes(relay_out, rsend_sem.at[0])
    wait_sent(0)
    for m in range(last + 1):
        if m in (0, last):
            wait_sums(min(m, 1))
        each(m, functools.partial(normalise, m))
    with jax.named_scope("qdrain"):
        wait_sent(1)


def _write(hid, nrm, hid_hbm, nrm_hbm, sem):
    blocks = 4
    rows = hid.shape[0] // blocks
    copies = []
    for k, (src, dst) in enumerate(((hid, hid_hbm), (nrm, nrm_hbm))):
        for b in range(blocks):
            rs = pl.ds(b * rows, rows)
            copies.append(pltpu.make_async_copy(src.at[rs, :], dst.at[rs, :], sem.at[k, b]))
    for copy in copies:
        copy.start()
    for copy in copies:
        copy.wait()


def solution(mesh):
    tp_size = mesh.shape["tp"]

    def local_step(attn_blk, w_blk, resid_blk, gain_blk):
        rows, k_dim = attn_blk.shape
        d_local = resid_blk.shape[1]
        d_model = w_blk.shape[1]
        half = d_local // 2
        nu = half // UNIT
        units = tp_size * 2 * nu
        sq_rows = sum(sum_rows())
        assert tp_size == CORES * CHIPS and half % UNIT == 0
        assert sum(FIRST_ROWS) == sum(RELAY_ROWS) == rows and rows % RB == 0 and nu == 3
        hbm_spec = pl.BlockSpec(memory_space=pltpu.HBM)
        vmem_spec = pl.BlockSpec(memory_space=pltpu.VMEM)
        dma = pltpu.SemaphoreType.DMA
        out_shape = [jax.ShapeDtypeStruct((rows, d_local), jnp.bfloat16)] * 2
        hid, nrm = pl.pallas_call(
            functools.partial(_kernel, tp_size, d_model),
            out_shape=[pltpu.VMEM((rows, d_local), jnp.bfloat16)] * 2,
            in_specs=[hbm_spec] * 4,
            out_specs=[vmem_spec] * 2,
            scratch_shapes=[
                pltpu.VMEM((rows, k_dim), jnp.bfloat16),
                pltpu.VMEM((W_SLOTS, k_dim, UNIT), jnp.bfloat16),
                pltpu.VMEM((units, rows, UNIT), jnp.bfloat16),
                pltpu.VMEM((12 * nu, rows, UNIT), jnp.bfloat16),
                pltpu.VMEM((2, rows, half), jnp.float32),
                pltpu.VMEM((2, rows, half), jnp.float32),
                pltpu.VMEM((rows, d_local), jnp.bfloat16),
                pltpu.VMEM((d_local,), jnp.float32),
                pltpu.VMEM((rows, d_local), jnp.float32),
                pltpu.VMEM((sq_rows, 1, LANES), jnp.float32),
                pltpu.VMEM((tp_size, sq_rows, 1, LANES), jnp.float32),
                dma((len(FIRST_ROWS),)),
                dma((2,)),
                dma((W_SLOTS,)),
                dma((1,)),
                dma((5,)),
                dma((1,)),
                dma((len(RELAY_ROWS), 2)),
                dma((2,)),
                dma((2, tp_size)),
            ],
            compiler_params=pltpu.CompilerParams(
                collective_id=0, has_side_effects=True, vmem_limit_bytes=62 * 1000 * 1000
            ),
            name="proj_scatter_norm",
        )(attn_blk, w_blk, resid_blk, gain_blk)
        return pl.pallas_call(
            _write,
            out_shape=out_shape,
            in_specs=[vmem_spec] * 2,
            out_specs=[hbm_spec] * 2,
            scratch_shapes=[dma((2, 4))],
            compiler_params=pltpu.CompilerParams(vmem_limit_bytes=8 * 1024 * 1024),
            name="write_out",
        )(hid, nrm)

    return jax.shard_map(
        local_step,
        mesh=mesh,
        in_specs=(P("data", "tp"), P("tp", None), P("data", "tp"), P("tp")),
        out_specs=(P("data", "tp"), P("data", "tp")),
        check_vma=False,
    )
```

```python
import functools

import jax
import jax.numpy as jnp
from jax import lax
from jax.experimental import pallas as pl
from jax.experimental.pallas import tpu as pltpu
from jax.sharding import PartitionSpec as P

EPS = 1e-5
MESH = pl.DeviceIdType.MESH
CORES = 2
CHIPS = 4
UNIT = 256
W_SLOTS = 4
RB = 64
RELAY_ROWS = (256, 192, 64)
LANES = 128
FIRST_ROWS = (128, 384)


def sum_rows():
    return -(-sum(RELAY_ROWS[:-1]) // LANES), -(-RELAY_ROWS[-1] // LANES)


def _kernel(
    tp_size, d_model,
    a_hbm, w_hbm, r_hbm, g_hbm, hid, nrm,
    a, w, p, rx, relay_out, relay_in, res, gain, hbuf, sq_out, sq_in,
    a_sem, in_sem, w_sem, send_sem, recv_sem, rsend_sem, rrecv_sem, qsend_sem, qrecv_sem,
):
    rows, d_local = r_hbm.shape
    half = d_local // 2
    nu = half // UNIT
    per_group = CORES * 2 * nu
    total = CHIPS * per_group
    chunks = rows // RB

    me = lax.axis_index("tp")
    x, c = lax.div(me, CORES), lax.rem(me, CORES)

    flip = lax.div(CHIPS - x, CHIPS)

    def chip(offset, core):
        return lax.rem(x + offset, CHIPS) * CORES + core

    def decode(s):
        g, j = lax.div(s, per_group), lax.rem(s, per_group)
        late = lax.div(lax.div(s, 2 * nu) + 7, 8)
        more = lax.div(lax.div(s, 2) + 1, 2)
        b = late * lax.div(j, nu) + (1 - late) * ((1 - more) * s + more * (lax.div(s, 2) - 1))
        i = late * lax.rem(j, nu) + (1 - late) * more * (1 + lax.rem(s, 2))
        return g, i, b, lax.rem(lax.div(b, 2) + 1 + c, 2), lax.rem(b + c + flip, 2)

    def w_copy(s):
        g, i, _, e, h = decode(s)
        o = lax.rem(6 - g + 2 * h * lax.rem(g, 2), CHIPS)
        col = pl.multiple_of(chip(o, e) * d_local + h * half + i * UNIT, UNIT)
        k = lax.rem(s, W_SLOTS)
        return pltpu.make_async_copy(w_hbm.at[:, pl.ds(col, UNIT)], w.at[k], w_sem.at[k])

    first_lo = [sum(FIRST_ROWS[:b]) for b in range(len(FIRST_ROWS))]

    def a_copy(b):
        rs = pl.ds(first_lo[b], FIRST_ROWS[b])
        return pltpu.make_async_copy(a_hbm.at[rs, :], a.at[rs, :], a_sem.at[b])

    def send(src, dst, group, target):
        pltpu.make_async_remote_copy(
            src_ref=src, dst_ref=dst, send_sem=send_sem.at[0], recv_sem=recv_sem.at[group],
            device_id={"tp": target}, device_id_type=MESH).start()

    def send_units(g, b, lo, n, block, group, target):
        send(p.at[pl.ds((g * 4 + b) * nu + lo, n)], rx.at[pl.ds(block * nu + lo, n)], group, target)

    def wait_bytes(ref, sem):
        pltpu.make_async_copy(ref, ref, sem).wait()

    def local_unit(g, h, i):
        return (g * 4 + (2 if g == 2 else 0) + lax.rem(h + c + flip, 2)) * nu + i

    relay_lo = [sum(RELAY_ROWS[:m]) for m in range(len(RELAY_ROWS))]

    def relay_rows(m):
        return pl.ds(relay_lo[m], RELAY_ROWS[m])

    def send_relay(m):
        for h in range(2):
            pltpu.make_async_remote_copy(
                src_ref=relay_out.at[h, relay_rows(m)], dst_ref=relay_in.at[h, relay_rows(m)],
                send_sem=rsend_sem.at[0], recv_sem=rrecv_sem.at[m, h],
                device_id={"tp": chip(3 - 2 * h, 1 - c)}, device_id_type=MESH).start()

    def chunk_rows(r):
        return pl.ds(pl.multiple_of(r * RB, RB), RB)

    def span(lo, n):
        return pl.ds(pl.multiple_of(lo, n), n)

    w_copy(jnp.int32(0)).start()
    a_copy(0).start()
    w_copy(jnp.int32(1)).start()

    peers = [x * CORES + 1 - c] + [chip(o, core) for o in (1, CHIPS - 1) for core in range(CORES)]
    barrier = pltpu.get_barrier_semaphore()
    for peer in peers:
        pl.semaphore_signal(barrier, inc=1, device_id={"tp": peer}, device_id_type=MESH)

    for b in range(1, len(FIRST_ROWS)):
        a_copy(b).start()
    r_copy = pltpu.make_async_copy(r_hbm, res, in_sem.at[0])
    g_copy = pltpu.make_async_copy(g_hbm, gain, in_sem.at[1])

    for b in range(len(FIRST_ROWS)):
        rs = pl.ds(first_lo[b], FIRST_ROWS[b])
        for s in range(2):
            _, _, block, e0, h0 = decode(jnp.int32(s))
            if b == 0:
                with jax.named_scope(f"w{s}"):
                    w_copy(jnp.int32(s)).wait()
            if s == 0:
                with jax.named_scope("awt"):
                    a_copy(b).wait()
            if b == 0 and s == 0:
                for k in range(2, W_SLOTS):
                    w_copy(jnp.int32(k)).start()
            unit = block * nu
            p[unit, rs, :] = jnp.dot(a[rs, :], w[s], preferred_element_type=jnp.float32).astype(p.dtype)
            if b == 0 and s == 0:
                with jax.named_scope("bar"):
                    pl.semaphore_wait(barrier, len(peers))
            send(p.at[unit, rs], rx.at[(h0 * 2 + c) * nu, rs], h0, chip(3 + 2 * h0, 1 - e0))
    for s in range(2):
        w_copy(jnp.int32(s + W_SLOTS)).start()
    r_copy.start()
    g_copy.start()

    @pl.loop(2, total)
    def _(s):
        g, i, b, e, h = decode(s)
        w_copy(s).wait()
        k = lax.rem(s, W_SLOTS)
        p[(g * 4 + b) * nu + i] = jnp.dot(
            a[...], w[k], preferred_element_type=jnp.float32).astype(p.dtype)

        @pl.when(s + W_SLOTS < total)
        def _():
            w_copy(s + W_SLOTS).start()

        def to_relay(lo, n):
            send_units(g, b, lo, n, h * 2 + c, h, chip(3 + 2 * h, 1 - e))

        @pl.when(i == nu - 1)
        def _():
            @pl.when(s < 2 * nu)
            def _():
                to_relay(1, nu - 1)

            @pl.when(jnp.logical_and(g == 0, s >= 2 * nu))
            def _():
                to_relay(0, nu)

            @pl.when(g == 1)
            def _():
                send_units(g, b, 0, nu, 4 + h * 2 + c, 2, chip(1 + 2 * h, e))

            @pl.when(jnp.logical_or(jnp.logical_and(g == 2, b < 2), jnp.logical_and(g == 3, b >= 2)))
            def _():
                send_units(g, b, 0, nu, 4 + g * 2 + h, g + 1, x * CORES + 1 - c)

    for h in (1, 0):
        with jax.named_scope(f"l2r{h}"):
            wait_bytes(rx.at[pl.ds(2 * h * nu, 2 * nu)], recv_sem.at[h])
    wait_bytes(rx.at[pl.ds(10 * nu, 2 * nu)], recv_sem.at[4])

    @pl.loop(0, chunks)
    def _(r):
        rs = chunk_rows(r)
        for h in range(2):
            for i in range(nu):
                acc = p[local_unit(3, h, i), rs, :].astype(jnp.float32)
                acc += rx[(10 + h) * nu + i, rs, :].astype(jnp.float32)
                acc += rx[(h * 2) * nu + i, rs, :].astype(jnp.float32)
                acc += rx[(h * 2 + 1) * nu + i, rs, :].astype(jnp.float32)
                relay_out[h, rs, i * UNIT:(i + 1) * UNIT] = acc

    for m in range(len(RELAY_ROWS)):
        send_relay(m)

    r_copy.wait()
    g_copy.wait()
    wait_bytes(rx.at[pl.ds(8 * nu, 2 * nu)], recv_sem.at[3])
    with jax.named_scope("direct"):
        wait_bytes(rx.at[pl.ds(4 * nu, 4 * nu)], recv_sem.at[2])

    sq_n = sum_rows()
    sq_lo = (0, sq_n[0])

    def on_lane(lane, n):
        return (lax.broadcasted_iota(jnp.int32, (n, LANES), 0) + lane
                == lax.broadcasted_iota(jnp.int32, (n, LANES), 1))

    def columns():
        for h in range(2):
            for i in range(nu):
                yield h, i, slice(h * half + i * UNIT, h * half + (i + 1) * UNIT)

    def add_early(lo, n):
        rs = span(lo, n)
        for h, i, cols in columns():
            acc = p[local_unit(2, h, i), rs, :].astype(jnp.float32)
            acc += rx[(8 + h) * nu + i, rs, :].astype(jnp.float32)
            acc += rx[(4 + h * 2) * nu + i, rs, :].astype(jnp.float32)
            acc += rx[(5 + h * 2) * nu + i, rs, :].astype(jnp.float32)
            hbuf[rs, cols] = acc + res[rs, cols].astype(jnp.float32)

    def finish(m, lo, n):
        rs = span(lo, n)
        sq = jnp.zeros((n, UNIT), jnp.float32)
        for h, i, cols in columns():
            acc = hbuf[rs, cols] + relay_in[h, rs, i * UNIT:(i + 1) * UNIT]
            hbuf[rs, cols] = acc
            sq += acc * acc
        sq = jnp.sum(sq, axis=1, keepdims=True)
        q, lane = place(m, lo)
        sq_out[q] += jnp.sum(
            jnp.where(on_lane(lane, n), jnp.broadcast_to(sq, (n, LANES)), 0.0), axis=0, keepdims=True)

    def place(m, lo):
        if m == len(RELAY_ROWS) - 1:
            lo = lo - relay_lo[m]
            return sq_lo[1] + lax.div(lo, LANES), lax.rem(lo, LANES)
        return lax.div(lo, LANES), lax.rem(lo, LANES)

    others = [chip(o, core) for o in (2, 1, 3) for core in range(CORES)] + [x * CORES + 1 - c]

    def send_sums(k):
        for target in others:
            pltpu.make_async_remote_copy(
                src_ref=sq_out.at[sq_span(k)], dst_ref=sq_in.at[me, sq_span(k)],
                send_sem=qsend_sem.at[k], recv_sem=qrecv_sem.at[k],
                device_id={"tp": target}, device_id_type=MESH).start()
        for q in range(sq_lo[k], sq_lo[k] + sq_n[k]):
            sq_in[me, q] = sq_out[q]

    def sq_span(k):
        return pl.ds(sq_lo[k], sq_n[k])

    def wait_sums(k, sem):
        wait_bytes(sq_in.at[pl.ds(0, tp_size - 1), sq_span(k)], sem.at[k])

    def normalise(m, lo, n):
        q, lane = place(m, lo)
        tot = sq_in[0, q]
        for t in range(1, tp_size):
            tot += sq_in[t, q]
        col = jnp.sum(jnp.where(on_lane(lane, n), jnp.broadcast_to(tot, (n, LANES)), 0.0), axis=1, keepdims=True)
        scale = lax.rsqrt(col / d_model + EPS)
        rs = span(lo, n)
        nrm[rs, :] = (hbuf[rs, :] * scale * gain[...].reshape(1, d_local)).astype(nrm.dtype)

    def write_hidden(lo, n):
        rs = span(lo, n)
        hid[rs, :] = hbuf[rs, :].astype(hid.dtype)

    def each(m, *steps):
        lo, hi = relay_lo[m], relay_lo[m] + RELAY_ROWS[m]
        whole = (hi - lo) // RB * RB

        if whole:
            @pl.loop(0, whole // RB)
            def _(r):
                for step in steps:
                    step(lo + r * RB, RB)

        if lo + whole < hi:
            for step in steps:
                step(lo + whole, hi - lo - whole)

    def wait_relay(m):
        for h in (1, 0):
            with jax.named_scope(f"r{m}h{h}"):
                wait_bytes(relay_in.at[h, relay_rows(m)], rrecv_sem.at[m, h])

    for q in range(sum(sq_n)):
        sq_out[q] = jnp.zeros((1, LANES), jnp.float32)
    last = len(RELAY_ROWS) - 1
    for m in range(last + 1):
        each(m, add_early)
        if m == last:
            wait_bytes(rx, send_sem.at[0])
        wait_relay(m)
        each(m, functools.partial(finish, m))
        if m >= last - 1:
            send_sums(m - last + 1)
        each(m, write_hidden)

    wait_bytes(relay_out, rsend_sem.at[0])
    wait_sums(0, qsend_sem)
    for m in range(last + 1):
        if m in (0, last):
            with jax.named_scope(f"sq{m}"):
                wait_sums(min(m, 1), qrecv_sem)
        each(m, functools.partial(normalise, m))
    with jax.named_scope("qdrain"):
        wait_sums(1, qsend_sem)


def _write(hid, nrm, hid_hbm, nrm_hbm, sem):
    blocks = 4
    rows = hid.shape[0] // blocks
    copies = []
    for k, (src, dst) in enumerate(((hid, hid_hbm), (nrm, nrm_hbm))):
        for b in range(blocks):
            rs = pl.ds(b * rows, rows)
            copies.append(pltpu.make_async_copy(src.at[rs, :], dst.at[rs, :], sem.at[k, b]))
    for copy in copies:
        copy.start()
    for copy in copies:
        copy.wait()


def solution(mesh):
    tp_size = mesh.shape["tp"]

    def local_step(attn_blk, w_blk, resid_blk, gain_blk):
        rows, k_dim = attn_blk.shape
        d_local = resid_blk.shape[1]
        d_model = w_blk.shape[1]
        half = d_local // 2
        nu = half // UNIT
        units = tp_size * 2 * nu
        sq_rows = sum(sum_rows())
        assert tp_size == CORES * CHIPS and half % UNIT == 0
        assert sum(FIRST_ROWS) == sum(RELAY_ROWS) == rows and rows % RB == 0 and nu == 3
        hbm_spec = pl.BlockSpec(memory_space=pltpu.HBM)
        vmem_spec = pl.BlockSpec(memory_space=pltpu.VMEM)
        dma = pltpu.SemaphoreType.DMA
        out_shape = [jax.ShapeDtypeStruct((rows, d_local), jnp.bfloat16)] * 2
        hid, nrm = pl.pallas_call(
            functools.partial(_kernel, tp_size, d_model),
            out_shape=[pltpu.VMEM((rows, d_local), jnp.bfloat16)] * 2,
            in_specs=[hbm_spec] * 4,
            out_specs=[vmem_spec] * 2,
            scratch_shapes=[
                pltpu.VMEM((rows, k_dim), jnp.bfloat16),
                pltpu.VMEM((W_SLOTS, k_dim, UNIT), jnp.bfloat16),
                pltpu.VMEM((units, rows, UNIT), jnp.bfloat16),
                pltpu.VMEM((12 * nu, rows, UNIT), jnp.bfloat16),
                pltpu.VMEM((2, rows, half), jnp.float32),
                pltpu.VMEM((2, rows, half), jnp.float32),
                pltpu.VMEM((rows, d_local), jnp.bfloat16),
                pltpu.VMEM((d_local,), jnp.float32),
                pltpu.VMEM((rows, d_local), jnp.float32),
                pltpu.VMEM((sq_rows, 1, LANES), jnp.float32),
                pltpu.VMEM((tp_size, sq_rows, 1, LANES), jnp.float32),
                dma((len(FIRST_ROWS),)),
                dma((2,)),
                dma((W_SLOTS,)),
                dma((1,)),
                dma((5,)),
                dma((1,)),
                dma((len(RELAY_ROWS), 2)),
                dma((2,)),
                dma((2,)),
            ],
            compiler_params=pltpu.CompilerParams(
                collective_id=0, has_side_effects=True, vmem_limit_bytes=62 * 1000 * 1000
            ),
            name="proj_scatter_norm",
        )(attn_blk, w_blk, resid_blk, gain_blk)
        return pl.pallas_call(
            _write,
            out_shape=out_shape,
            in_specs=[vmem_spec] * 2,
            out_specs=[hbm_spec] * 2,
            scratch_shapes=[dma((2, 4))],
            compiler_params=pltpu.CompilerParams(vmem_limit_bytes=8 * 1024 * 1024),
            name="write_out",
        )(hid, nrm)

    return jax.shard_map(
        local_step,
        mesh=mesh,
        in_specs=(P("data", "tp"), P("tp", None), P("data", "tp"), P("tp")),
        out_specs=(P("data", "tp"), P("data", "tp")),
        check_vma=False,
    )
```

```python
import functools

import jax
import jax.numpy as jnp
from jax import lax
from jax.experimental import pallas as pl
from jax.experimental.pallas import tpu as pltpu
from jax.sharding import PartitionSpec as P

EPS = 1e-5
MESH = pl.DeviceIdType.MESH
CORES = 2
CHIPS = 4
UNIT = 256
W_SLOTS = 4
RB = 64
RELAY_ROWS = (256, 192, 32, 32)
EARLY = 2
LANES = 128
FIRST_ROWS = (128, 384)


def sum_rows():
    return -(-sum(RELAY_ROWS[:EARLY]) // LANES), -(-sum(RELAY_ROWS[EARLY:]) // LANES)


def _kernel(
    tp_size, d_model,
    a_hbm, w_hbm, r_hbm, g_hbm, hid, nrm,
    a, w, p, rx, relay_out, relay_in, res, gain, hbuf, sq_out, sq_in,
    a_sem, in_sem, w_sem, send_sem, recv_sem, rsend_sem, rrecv_sem, qsend_sem, qrecv_sem,
):
    rows, d_local = r_hbm.shape
    half = d_local // 2
    nu = half // UNIT
    per_group = CORES * 2 * nu
    total = CHIPS * per_group
    chunks = rows // RB

    me = lax.axis_index("tp")
    x, c = lax.div(me, CORES), lax.rem(me, CORES)

    flip = lax.div(CHIPS - x, CHIPS)

    def chip(offset, core):
        return lax.rem(x + offset, CHIPS) * CORES + core

    def decode(s):
        g, j = lax.div(s, per_group), lax.rem(s, per_group)
        late = lax.div(lax.div(s, 2 * nu) + 7, 8)
        more = lax.div(lax.div(s, 2) + 1, 2)
        b = late * lax.div(j, nu) + (1 - late) * ((1 - more) * s + more * (lax.div(s, 2) - 1))
        i = late * lax.rem(j, nu) + (1 - late) * more * (1 + lax.rem(s, 2))
        return g, i, b, lax.rem(lax.div(b, 2) + 1 + c, 2), lax.rem(b + c + flip, 2)

    def w_copy(s):
        g, i, _, e, h = decode(s)
        o = lax.rem(6 - g + 2 * h * lax.rem(g, 2), CHIPS)
        col = pl.multiple_of(chip(o, e) * d_local + h * half + i * UNIT, UNIT)
        k = lax.rem(s, W_SLOTS)
        return pltpu.make_async_copy(w_hbm.at[:, pl.ds(col, UNIT)], w.at[k], w_sem.at[k])

    first_lo = [sum(FIRST_ROWS[:b]) for b in range(len(FIRST_ROWS))]

    def a_copy(b):
        rs = pl.ds(first_lo[b], FIRST_ROWS[b])
        return pltpu.make_async_copy(a_hbm.at[rs, :], a.at[rs, :], a_sem.at[b])

    def send(src, dst, group, target):
        pltpu.make_async_remote_copy(
            src_ref=src, dst_ref=dst, send_sem=send_sem.at[0], recv_sem=recv_sem.at[group],
            device_id={"tp": target}, device_id_type=MESH).start()

    def send_units(g, b, lo, n, block, group, target):
        send(p.at[pl.ds((g * 4 + b) * nu + lo, n)], rx.at[pl.ds(block * nu + lo, n)], group, target)

    def wait_bytes(ref, sem):
        pltpu.make_async_copy(ref, ref, sem).wait()

    def local_unit(g, h, i):
        return (g * 4 + (2 if g == 2 else 0) + lax.rem(h + c + flip, 2)) * nu + i

    relay_lo = [sum(RELAY_ROWS[:m]) for m in range(len(RELAY_ROWS))]

    def relay_rows(m):
        return pl.ds(relay_lo[m], RELAY_ROWS[m])

    def send_relay(m):
        for h in range(2):
            pltpu.make_async_remote_copy(
                src_ref=relay_out.at[h, relay_rows(m)], dst_ref=relay_in.at[h, relay_rows(m)],
                send_sem=rsend_sem.at[0], recv_sem=rrecv_sem.at[m, h],
                device_id={"tp": chip(3 - 2 * h, 1 - c)}, device_id_type=MESH).start()

    def chunk_rows(r):
        return pl.ds(pl.multiple_of(r * RB, RB), RB)

    def span(lo, n):
        return pl.ds(pl.multiple_of(lo, n), n)

    peers = [chip(o, core) for o in (1, CHIPS - 1) for core in range(CORES)] + [x * CORES + 1 - c]
    barrier = pltpu.get_barrier_semaphore()
    for n, peer in enumerate(peers):
        pl.semaphore_signal(barrier, inc=1, device_id={"tp": peer}, device_id_type=MESH)
        if n == CORES - 1:
            w_copy(jnp.int32(0)).start()
            a_copy(0).start()

    w_copy(jnp.int32(1)).start()
    for b in range(1, len(FIRST_ROWS)):
        a_copy(b).start()
    r_copy = pltpu.make_async_copy(r_hbm, res, in_sem.at[0])
    g_copy = pltpu.make_async_copy(g_hbm, gain, in_sem.at[1])

    for b in range(len(FIRST_ROWS)):
        rs = pl.ds(first_lo[b], FIRST_ROWS[b])
        for s in range(2):
            _, _, block, e0, h0 = decode(jnp.int32(s))
            if b == 0:
                with jax.named_scope(f"w{s}"):
                    w_copy(jnp.int32(s)).wait()
            if s == 0:
                with jax.named_scope("awt"):
                    a_copy(b).wait()
            if b == 0 and s == 0:
                for k in range(2, W_SLOTS):
                    w_copy(jnp.int32(k)).start()
            unit = block * nu
            p[unit, rs, :] = jnp.dot(a[rs, :], w[s], preferred_element_type=jnp.float32).astype(p.dtype)
            if b == 0 and s == 0:
                with jax.named_scope("bar"):
                    pl.semaphore_wait(barrier, len(peers))
            send(p.at[unit, rs], rx.at[(h0 * 2 + c) * nu, rs], h0, chip(3 + 2 * h0, 1 - e0))
    for s in range(2):
        w_copy(jnp.int32(s + W_SLOTS)).start()
    r_copy.start()
    g_copy.start()

    @pl.loop(2, total)
    def _(s):
        g, i, b, e, h = decode(s)
        w_copy(s).wait()
        k = lax.rem(s, W_SLOTS)
        p[(g * 4 + b) * nu + i] = jnp.dot(
            a[...], w[k], preferred_element_type=jnp.float32).astype(p.dtype)

        @pl.when(s + W_SLOTS < total)
        def _():
            w_copy(s + W_SLOTS).start()

        def to_relay(lo, n):
            send_units(g, b, lo, n, h * 2 + c, h, chip(3 + 2 * h, 1 - e))

        @pl.when(i == nu - 1)
        def _():
            @pl.when(s < 2 * nu)
            def _():
                to_relay(1, nu - 1)

            @pl.when(jnp.logical_and(g == 0, s >= 2 * nu))
            def _():
                to_relay(0, nu)

            @pl.when(g == 1)
            def _():
                send_units(g, b, 0, nu, 4 + h * 2 + c, 2, chip(1 + 2 * h, e))

            @pl.when(jnp.logical_or(jnp.logical_and(g == 2, b < 2), jnp.logical_and(g == 3, b >= 2)))
            def _():
                send_units(g, b, 0, nu, 4 + g * 2 + h, g + 1, x * CORES + 1 - c)

    for h in (1, 0):
        with jax.named_scope(f"l2r{h}"):
            wait_bytes(rx.at[pl.ds(2 * h * nu, 2 * nu)], recv_sem.at[h])
    wait_bytes(rx.at[pl.ds(10 * nu, 2 * nu)], recv_sem.at[4])

    @pl.loop(0, chunks)
    def _(r):
        rs = chunk_rows(r)
        for h in range(2):
            for i in range(nu):
                acc = p[local_unit(3, h, i), rs, :].astype(jnp.float32)
                acc += rx[(10 + h) * nu + i, rs, :].astype(jnp.float32)
                acc += rx[(h * 2) * nu + i, rs, :].astype(jnp.float32)
                acc += rx[(h * 2 + 1) * nu + i, rs, :].astype(jnp.float32)
                relay_out[h, rs, i * UNIT:(i + 1) * UNIT] = acc

    for m in range(len(RELAY_ROWS)):
        send_relay(m)

    r_copy.wait()
    g_copy.wait()
    wait_bytes(rx.at[pl.ds(8 * nu, 2 * nu)], recv_sem.at[3])
    with jax.named_scope("direct"):
        wait_bytes(rx.at[pl.ds(4 * nu, 4 * nu)], recv_sem.at[2])

    sq_n = sum_rows()
    sq_lo = (0, sq_n[0])

    def on_lane(lane, n):
        return (lax.broadcasted_iota(jnp.int32, (n, LANES), 0) + lane
                == lax.broadcasted_iota(jnp.int32, (n, LANES), 1))

    def columns():
        for h in range(2):
            for i in range(nu):
                yield h, i, slice(h * half + i * UNIT, h * half + (i + 1) * UNIT)

    def add_early(lo, n):
        rs = span(lo, n)
        for h, i, cols in columns():
            acc = p[local_unit(2, h, i), rs, :].astype(jnp.float32)
            acc += rx[(8 + h) * nu + i, rs, :].astype(jnp.float32)
            acc += rx[(4 + h * 2) * nu + i, rs, :].astype(jnp.float32)
            acc += rx[(5 + h * 2) * nu + i, rs, :].astype(jnp.float32)
            hbuf[rs, cols] = acc + res[rs, cols].astype(jnp.float32)

    def finish(m, lo, n):
        rs = span(lo, n)
        sq = jnp.zeros((n, UNIT), jnp.float32)
        for h, i, cols in columns():
            acc = hbuf[rs, cols] + relay_in[h, rs, i * UNIT:(i + 1) * UNIT]
            hbuf[rs, cols] = acc
            sq += acc * acc
        sq = jnp.sum(sq, axis=1, keepdims=True)
        q, lane = place(m, lo)
        sq_out[q] += jnp.sum(
            jnp.where(on_lane(lane, n), jnp.broadcast_to(sq, (n, LANES)), 0.0), axis=0, keepdims=True)

    def place(m, lo):
        if m >= EARLY:
            lo = lo - relay_lo[EARLY]
            return sq_lo[1] + lax.div(lo, LANES), lax.rem(lo, LANES)
        return lax.div(lo, LANES), lax.rem(lo, LANES)

    others = [chip(o, core) for o in (1 + 2 * flip, 2, 3 - 2 * flip) for core in range(CORES)] + [x * CORES + 1 - c]

    def send_sums(k):
        for target in others:
            pltpu.make_async_remote_copy(
                src_ref=sq_out.at[sq_span(k)], dst_ref=sq_in.at[me, sq_span(k)],
                send_sem=qsend_sem.at[k], recv_sem=qrecv_sem.at[k],
                device_id={"tp": target}, device_id_type=MESH).start()
        for q in range(sq_lo[k], sq_lo[k] + sq_n[k]):
            sq_in[me, q] = sq_out[q]

    def sq_span(k):
        return pl.ds(sq_lo[k], sq_n[k])

    def wait_sums(k, sem):
        wait_bytes(sq_in.at[pl.ds(0, tp_size - 1), sq_span(k)], sem.at[k])

    def normalise(m, lo, n):
        q, lane = place(m, lo)
        tot = sq_in[0, q]
        for t in range(1, tp_size):
            tot += sq_in[t, q]
        col = jnp.sum(jnp.where(on_lane(lane, n), jnp.broadcast_to(tot, (n, LANES)), 0.0), axis=1, keepdims=True)
        scale = lax.rsqrt(col / d_model + EPS)
        rs = span(lo, n)
        nrm[rs, :] = (hbuf[rs, :] * scale * gain[...].reshape(1, d_local)).astype(nrm.dtype)

    def write_hidden(lo, n):
        rs = span(lo, n)
        hid[rs, :] = hbuf[rs, :].astype(hid.dtype)

    def each(m, *steps):
        lo, hi = relay_lo[m], relay_lo[m] + RELAY_ROWS[m]
        whole = (hi - lo) // RB * RB

        if whole:
            @pl.loop(0, whole // RB)
            def _(r):
                for step in steps:
                    step(lo + r * RB, RB)

        if lo + whole < hi:
            for step in steps:
                step(lo + whole, hi - lo - whole)

    def wait_relay(m):
        for h in (1, 0):
            with jax.named_scope(f"r{m}h{h}"):
                wait_bytes(relay_in.at[h, relay_rows(m)], rrecv_sem.at[m, h])

    for q in range(sum(sq_n)):
        sq_out[q] = jnp.zeros((1, LANES), jnp.float32)
    last = len(RELAY_ROWS) - 1
    for m in range(last + 1):
        each(m, add_early)
        if m == last:
            wait_bytes(rx, send_sem.at[0])
        wait_relay(m)
        each(m, functools.partial(finish, m))
        if m in (EARLY - 1, last):
            send_sums(int(m == last))
        each(m, write_hidden)

    wait_bytes(relay_out, rsend_sem.at[0])
    wait_sums(0, qsend_sem)
    for m in range(last + 1):
        if m in (0, EARLY):
            with jax.named_scope(f"sq{m}"):
                wait_sums(m // EARLY, qrecv_sem)
        each(m, functools.partial(normalise, m))
    with jax.named_scope("qdrain"):
        wait_sums(1, qsend_sem)


def _write(hid, nrm, hid_hbm, nrm_hbm, sem):
    blocks = 4
    rows = hid.shape[0] // blocks
    copies = []
    for k, (src, dst) in enumerate(((hid, hid_hbm), (nrm, nrm_hbm))):
        for b in range(blocks):
            rs = pl.ds(b * rows, rows)
            copies.append(pltpu.make_async_copy(src.at[rs, :], dst.at[rs, :], sem.at[k, b]))
    for copy in copies:
        copy.start()
    for copy in copies:
        copy.wait()


def solution(mesh):
    tp_size = mesh.shape["tp"]

    def local_step(attn_blk, w_blk, resid_blk, gain_blk):
        rows, k_dim = attn_blk.shape
        d_local = resid_blk.shape[1]
        d_model = w_blk.shape[1]
        half = d_local // 2
        nu = half // UNIT
        units = tp_size * 2 * nu
        sq_rows = sum(sum_rows())
        assert tp_size == CORES * CHIPS and half % UNIT == 0
        assert sum(FIRST_ROWS) == sum(RELAY_ROWS) == rows and rows % RB == 0 and nu == 3
        hbm_spec = pl.BlockSpec(memory_space=pltpu.HBM)
        vmem_spec = pl.BlockSpec(memory_space=pltpu.VMEM)
        dma = pltpu.SemaphoreType.DMA
        out_shape = [jax.ShapeDtypeStruct((rows, d_local), jnp.bfloat16)] * 2
        hid, nrm = pl.pallas_call(
            functools.partial(_kernel, tp_size, d_model),
            out_shape=[pltpu.VMEM((rows, d_local), jnp.bfloat16)] * 2,
            in_specs=[hbm_spec] * 4,
            out_specs=[vmem_spec] * 2,
            scratch_shapes=[
                pltpu.VMEM((rows, k_dim), jnp.bfloat16),
                pltpu.VMEM((W_SLOTS, k_dim, UNIT), jnp.bfloat16),
                pltpu.VMEM((units, rows, UNIT), jnp.bfloat16),
                pltpu.VMEM((12 * nu, rows, UNIT), jnp.bfloat16),
                pltpu.VMEM((2, rows, half), jnp.float32),
                pltpu.VMEM((2, rows, half), jnp.float32),
                pltpu.VMEM((rows, d_local), jnp.bfloat16),
                pltpu.VMEM((d_local,), jnp.float32),
                pltpu.VMEM((rows, d_local), jnp.float32),
                pltpu.VMEM((sq_rows, 1, LANES), jnp.float32),
                pltpu.VMEM((tp_size, sq_rows, 1, LANES), jnp.float32),
                dma((len(FIRST_ROWS),)),
                dma((2,)),
                dma((W_SLOTS,)),
                dma((1,)),
                dma((5,)),
                dma((1,)),
                dma((len(RELAY_ROWS), 2)),
                dma((2,)),
                dma((2,)),
            ],
            compiler_params=pltpu.CompilerParams(
                collective_id=0, has_side_effects=True, vmem_limit_bytes=62 * 1000 * 1000
            ),
            name="proj_scatter_norm",
        )(attn_blk, w_blk, resid_blk, gain_blk)
        return pl.pallas_call(
            _write,
            out_shape=out_shape,
            in_specs=[vmem_spec] * 2,
            out_specs=[hbm_spec] * 2,
            scratch_shapes=[dma((2, 4))],
            compiler_params=pltpu.CompilerParams(vmem_limit_bytes=8 * 1024 * 1024),
            name="write_out",
        )(hid, nrm)

    return jax.shard_map(
        local_step,
        mesh=mesh,
        in_specs=(P("data", "tp"), P("tp", None), P("data", "tp"), P("tp")),
        out_specs=(P("data", "tp"), P("data", "tp")),
        check_vma=False,
    )
```

```python
import functools

import jax
import jax.numpy as jnp
from jax import lax
from jax.experimental import pallas as pl
from jax.experimental.pallas import tpu as pltpu
from jax.sharding import PartitionSpec as P

EPS = 1e-5
MESH = pl.DeviceIdType.MESH
CORES = 2
CHIPS = 4
UNIT = 256
W_SLOTS = 4
RB = 64
RELAY_ROWS = (256, 192, 64)
LANES = 128
FIRST_ROWS = (128, 384)


def sum_rows():
    return -(-sum(RELAY_ROWS[:-1]) // LANES), -(-RELAY_ROWS[-1] // LANES)


def _kernel(
    tp_size, d_model,
    a_hbm, w_hbm, r_hbm, g_hbm, hid, nrm,
    a, w, p, rx, relay_out, relay_in, res, gain, hbuf, sq_out, sq_in,
    a_sem, w_sem, send_sem, recv_sem, rrecv_sem, qsend_sem, qrecv_sem,
):
    rows, d_local = r_hbm.shape
    half = d_local // 2
    nu = half // UNIT
    per_group = CORES * 2 * nu
    total = CHIPS * per_group
    chunks = rows // RB

    me = lax.axis_index("tp")
    x, c = lax.div(me, CORES), lax.rem(me, CORES)

    flip = lax.div(CHIPS - x, CHIPS)

    def chip(offset, core):
        return lax.rem(x + offset, CHIPS) * CORES + core

    def decode(s):
        g, j = lax.div(s, per_group), lax.rem(s, per_group)
        late = lax.div(lax.div(s, 2 * nu) + 7, 8)
        more = lax.div(lax.div(s, 2) + 1, 2)
        b = late * lax.div(j, nu) + (1 - late) * ((1 - more) * s + more * (lax.div(s, 2) - 1))
        i = late * lax.rem(j, nu) + (1 - late) * more * (1 + lax.rem(s, 2))
        return g, i, b, lax.rem(lax.div(b, 2) + 1 + c, 2), lax.rem(b + c + flip, 2)

    def w_copy(s):
        g, i, _, e, h = decode(s)
        o = lax.rem(6 - g + 2 * h * lax.rem(g, 2), CHIPS)
        col = pl.multiple_of(chip(o, e) * d_local + h * half + i * UNIT, UNIT)
        k = lax.rem(s, W_SLOTS)
        return pltpu.make_async_copy(w_hbm.at[:, pl.ds(col, UNIT)], w.at[k], w_sem.at[k])

    first_lo = [sum(FIRST_ROWS[:b]) for b in range(len(FIRST_ROWS))]

    def a_copy(b):
        rs = pl.ds(first_lo[b], FIRST_ROWS[b])
        return pltpu.make_async_copy(a_hbm.at[rs, :], a.at[rs, :], a_sem.at[b])

    def send(src, dst, group, target):
        pltpu.make_async_remote_copy(
            src_ref=src, dst_ref=dst, send_sem=send_sem.at[0], recv_sem=recv_sem.at[group],
            device_id={"tp": target}, device_id_type=MESH).start()

    def send_units(g, b, lo, n, block, group, target):
        send(p.at[pl.ds((g * 4 + b) * nu + lo, n)], rx.at[pl.ds(block * nu + lo, n)], group, target)

    def wait_bytes(ref, sem):
        pltpu.make_async_copy(ref, ref, sem).wait()

    def local_unit(g, h, i):
        return (g * 4 + (2 if g == 2 else 0) + lax.rem(h + c + flip, 2)) * nu + i

    relay_lo = [sum(RELAY_ROWS[:m]) for m in range(len(RELAY_ROWS))]

    def relay_rows(m):
        return pl.ds(relay_lo[m], RELAY_ROWS[m])

    def send_relay(m):
        for h in range(2):
            pltpu.make_async_remote_copy(
                src_ref=relay_out.at[h, relay_rows(m)], dst_ref=relay_in.at[h, relay_rows(m)],
                send_sem=send_sem.at[0], recv_sem=rrecv_sem.at[m],
                device_id={"tp": chip(3 - 2 * h, 1 - c)}, device_id_type=MESH).start()

    def chunk_rows(r):
        return pl.ds(pl.multiple_of(r * RB, RB), RB)

    def span(lo, n):
        return pl.ds(pl.multiple_of(lo, n), n)

    w_copy(jnp.int32(0)).start()
    a_copy(0).start()
    w_copy(jnp.int32(1)).start()

    peers = [x * CORES + 1 - c] + [chip(o, core) for o in (1, CHIPS - 1) for core in range(CORES)]
    barrier = pltpu.get_barrier_semaphore()
    for peer in peers:
        pl.semaphore_signal(barrier, inc=1, device_id={"tp": peer}, device_id_type=MESH)

    for b in range(1, len(FIRST_ROWS)):
        a_copy(b).start()
    r_copy = pltpu.make_async_copy(r_hbm, res, a_sem.at[0])
    g_copy = pltpu.make_async_copy(g_hbm, gain, a_sem.at[1])

    for b in range(len(FIRST_ROWS)):
        rs = pl.ds(first_lo[b], FIRST_ROWS[b])
        for s in range(2):
            _, _, block, e0, h0 = decode(jnp.int32(s))
            if b == 0:
                with jax.named_scope(f"w{s}"):
                    w_copy(jnp.int32(s)).wait()
            if s == 0:
                with jax.named_scope("awt"):
                    a_copy(b).wait()
            if b == 0 and s == 0:
                for k in range(2, W_SLOTS):
                    w_copy(jnp.int32(k)).start()
            unit = block * nu
            p[unit, rs, :] = jnp.dot(a[rs, :], w[s], preferred_element_type=jnp.float32).astype(p.dtype)
            if b == 0 and s == 0:
                with jax.named_scope("bar"):
                    pl.semaphore_wait(barrier, len(peers))
            send(p.at[unit, rs], rx.at[(h0 * 2 + c) * nu, rs], 0, chip(3 + 2 * h0, 1 - e0))
    for s in range(2):
        w_copy(jnp.int32(s + W_SLOTS)).start()
    r_copy.start()
    g_copy.start()

    @pl.loop(2, total)
    def _(s):
        g, i, b, e, h = decode(s)
        w_copy(s).wait()
        k = lax.rem(s, W_SLOTS)
        p[(g * 4 + b) * nu + i] = jnp.dot(
            a[...], w[k], preferred_element_type=jnp.float32).astype(p.dtype)

        @pl.when(s + W_SLOTS < total)
        def _():
            w_copy(s + W_SLOTS).start()

        def to_relay(lo, n):
            send_units(g, b, lo, n, h * 2 + c, 0, chip(3 + 2 * h, 1 - e))

        @pl.when(i == nu - 1)
        def _():
            @pl.when(s < 2 * nu)
            def _():
                to_relay(1, nu - 1)

            @pl.when(jnp.logical_and(g == 0, s >= 2 * nu))
            def _():
                to_relay(0, nu)

            @pl.when(g == 1)
            def _():
                send_units(g, b, 0, nu, 4 + h * 2 + c, 1, chip(1 + 2 * h, e))

            @pl.when(jnp.logical_or(jnp.logical_and(g == 2, b < 2), jnp.logical_and(g == 3, b >= 2)))
            def _():
                send_units(g, b, 0, nu, 4 + g * 2 + h, 3 - g, x * CORES + 1 - c)

    with jax.named_scope("l2r"):
        wait_bytes(rx.at[pl.ds(0, 6 * nu)], recv_sem.at[0])

    @pl.loop(0, chunks)
    def _(r):
        rs = chunk_rows(r)
        for h in range(2):
            for i in range(nu):
                acc = p[local_unit(3, h, i), rs, :].astype(jnp.float32)
                acc += rx[(10 + h) * nu + i, rs, :].astype(jnp.float32)
                acc += rx[(h * 2) * nu + i, rs, :].astype(jnp.float32)
                acc += rx[(h * 2 + 1) * nu + i, rs, :].astype(jnp.float32)
                relay_out[h, rs, i * UNIT:(i + 1) * UNIT] = acc

    for m in range(len(RELAY_ROWS)):
        send_relay(m)

    r_copy.wait()
    g_copy.wait()
    with jax.named_scope("direct"):
        wait_bytes(rx.at[pl.ds(0, 6 * nu)], recv_sem.at[1])

    sq_n = sum_rows()
    sq_lo = (0, sq_n[0])

    def on_lane(lane, n):
        return (lax.broadcasted_iota(jnp.int32, (n, LANES), 0) + lane
                == lax.broadcasted_iota(jnp.int32, (n, LANES), 1))

    def columns():
        for h in range(2):
            for i in range(nu):
                yield h, i, slice(h * half + i * UNIT, h * half + (i + 1) * UNIT)

    def add_early(lo, n):
        rs = span(lo, n)
        for h, i, cols in columns():
            acc = p[local_unit(2, h, i), rs, :].astype(jnp.float32)
            acc += rx[(8 + h) * nu + i, rs, :].astype(jnp.float32)
            acc += rx[(4 + h * 2) * nu + i, rs, :].astype(jnp.float32)
            acc += rx[(5 + h * 2) * nu + i, rs, :].astype(jnp.float32)
            hbuf[rs, cols] = acc + res[rs, cols].astype(jnp.float32)

    def finish(m, lo, n):
        rs = span(lo, n)
        sq = jnp.zeros((n, UNIT), jnp.float32)
        for h, i, cols in columns():
            acc = hbuf[rs, cols] + relay_in[h, rs, i * UNIT:(i + 1) * UNIT]
            hbuf[rs, cols] = acc
            sq += acc * acc
        sq = jnp.sum(sq, axis=1, keepdims=True)
        q, lane = place(m, lo)
        sq_out[q] += jnp.sum(
            jnp.where(on_lane(lane, n), jnp.broadcast_to(sq, (n, LANES)), 0.0), axis=0, keepdims=True)

    def place(m, lo):
        if m == len(RELAY_ROWS) - 1:
            lo = lo - relay_lo[m]
            return sq_lo[1] + lax.div(lo, LANES), lax.rem(lo, LANES)
        return lax.div(lo, LANES), lax.rem(lo, LANES)

    closing = flip + lax.div(x, CHIPS - 1)
    first = closing * (1 + 2 * flip) + (1 - closing) * 2
    second = 1 + closing
    others = [chip(o, core) for o in (first, second, 6 - first - second) for core in range(CORES)]
    others.append(x * CORES + 1 - c)

    def send_sums(k):
        for target in others:
            pltpu.make_async_remote_copy(
                src_ref=sq_out.at[sq_span(k)], dst_ref=sq_in.at[me, sq_span(k)],
                send_sem=qsend_sem.at[0], recv_sem=qrecv_sem.at[k],
                device_id={"tp": target}, device_id_type=MESH).start()
        for q in range(sq_lo[k], sq_lo[k] + sq_n[k]):
            sq_in[me, q] = sq_out[q]

    def sq_span(k):
        return pl.ds(sq_lo[k], sq_n[k])

    def wait_sums(k, sem):
        wait_bytes(sq_in.at[pl.ds(0, tp_size - 1), sq_span(k)], sem.at[k])

    def normalise(m, lo, n):
        q, lane = place(m, lo)
        tot = sq_in[0, q]
        for t in range(1, tp_size):
            tot += sq_in[t, q]
        col = jnp.sum(jnp.where(on_lane(lane, n), jnp.broadcast_to(tot, (n, LANES)), 0.0), axis=1, keepdims=True)
        scale = lax.rsqrt(col / d_model + EPS)
        rs = span(lo, n)
        nrm[rs, :] = (hbuf[rs, :] * scale * gain[...].reshape(1, d_local)).astype(nrm.dtype)

    def write_hidden(lo, n):
        rs = span(lo, n)
        hid[rs, :] = hbuf[rs, :].astype(hid.dtype)

    def each(m, *steps):
        lo, hi = relay_lo[m], relay_lo[m] + RELAY_ROWS[m]
        whole = (hi - lo) // RB * RB

        if whole:
            @pl.loop(0, whole // RB)
            def _(r):
                for step in steps:
                    step(lo + r * RB, RB)

        if lo + whole < hi:
            for step in steps:
                step(lo + whole, hi - lo - whole)

    def wait_relay(m):
        with jax.named_scope(f"r{m}"):
            wait_bytes(relay_in.at[:, relay_rows(m)], rrecv_sem.at[m])

    for q in range(sum(sq_n)):
        sq_out[q] = jnp.zeros((1, LANES), jnp.float32)
    last = len(RELAY_ROWS) - 1
    for m in range(last + 1):
        each(m, add_early)
        wait_relay(m)
        each(m, functools.partial(finish, m))
        if m >= last - 1:
            send_sums(m - last + 1)
        each(m, write_hidden)

    wait_bytes(p, send_sem.at[0])
    for m in range(last + 1):
        if m in (0, last):
            with jax.named_scope(f"sq{m}"):
                wait_sums(min(m, 1), qrecv_sem)
        each(m, functools.partial(normalise, m))
    with jax.named_scope("qdrain"):
        wait_bytes(sq_in.at[pl.ds(0, tp_size - 1)], qsend_sem.at[0])


def _write(hid, nrm, hid_hbm, nrm_hbm, sem):
    blocks = 4
    rows = hid.shape[0] // blocks
    pairs = ((hid, hid_hbm), (nrm, nrm_hbm))
    for k, (src, dst) in enumerate(pairs):
        for b in range(blocks):
            rs = pl.ds(b * rows, rows)
            pltpu.make_async_copy(src.at[rs, :], dst.at[rs, :], sem.at[k]).start()
    for k, (src, dst) in enumerate(pairs):
        pltpu.make_async_copy(src, dst, sem.at[k]).wait()


def solution(mesh):
    tp_size = mesh.shape["tp"]

    def local_step(attn_blk, w_blk, resid_blk, gain_blk):
        rows, k_dim = attn_blk.shape
        d_local = resid_blk.shape[1]
        d_model = w_blk.shape[1]
        half = d_local // 2
        nu = half // UNIT
        units = tp_size * 2 * nu
        sq_rows = sum(sum_rows())
        assert tp_size == CORES * CHIPS and half % UNIT == 0
        assert sum(FIRST_ROWS) == sum(RELAY_ROWS) == rows and rows % RB == 0 and nu == 3
        hbm_spec = pl.BlockSpec(memory_space=pltpu.HBM)
        vmem_spec = pl.BlockSpec(memory_space=pltpu.VMEM)
        dma = pltpu.SemaphoreType.DMA
        out_shape = [jax.ShapeDtypeStruct((rows, d_local), jnp.bfloat16)] * 2
        hid, nrm = pl.pallas_call(
            functools.partial(_kernel, tp_size, d_model),
            out_shape=[pltpu.VMEM((rows, d_local), jnp.bfloat16)] * 2,
            in_specs=[hbm_spec] * 4,
            out_specs=[vmem_spec] * 2,
            scratch_shapes=[
                pltpu.VMEM((rows, k_dim), jnp.bfloat16),
                pltpu.VMEM((W_SLOTS, k_dim, UNIT), jnp.bfloat16),
                pltpu.VMEM((units, rows, UNIT), jnp.bfloat16),
                pltpu.VMEM((12 * nu, rows, UNIT), jnp.bfloat16),
                pltpu.VMEM((2, rows, half), jnp.float32),
                pltpu.VMEM((2, rows, half), jnp.float32),
                pltpu.VMEM((rows, d_local), jnp.bfloat16),
                pltpu.VMEM((d_local,), jnp.float32),
                pltpu.VMEM((rows, d_local), jnp.float32),
                pltpu.VMEM((sq_rows, 1, LANES), jnp.float32),
                pltpu.VMEM((tp_size, sq_rows, 1, LANES), jnp.float32),
                dma((len(FIRST_ROWS),)),
                dma((W_SLOTS,)),
                dma((1,)),
                dma((2,)),
                dma((len(RELAY_ROWS),)),
                dma((1,)),
                dma((2,)),
            ],
            compiler_params=pltpu.CompilerParams(
                collective_id=0, has_side_effects=True, vmem_limit_bytes=62 * 1000 * 1000
            ),
            name="proj_scatter_norm",
        )(attn_blk, w_blk, resid_blk, gain_blk)
        return pl.pallas_call(
            _write,
            out_shape=out_shape,
            in_specs=[vmem_spec] * 2,
            out_specs=[hbm_spec] * 2,
            scratch_shapes=[dma((2,))],
            compiler_params=pltpu.CompilerParams(vmem_limit_bytes=8 * 1024 * 1024),
            name="write_out",
        )(hid, nrm)

    return jax.shard_map(
        local_step,
        mesh=mesh,
        in_specs=(P("data", "tp"), P("tp", None), P("data", "tp"), P("tp")),
        out_specs=(P("data", "tp"), P("data", "tp")),
        check_vma=False,
    )
```

```python
import functools

import jax
import jax.numpy as jnp
from jax import lax
from jax.experimental import pallas as pl
from jax.experimental.pallas import tpu as pltpu
from jax.sharding import PartitionSpec as P

EPS = 1e-5
MESH = pl.DeviceIdType.MESH
CORES = 2
CHIPS = 4
UNIT = 256
W_SLOTS = 4
RB = 64
RELAY_ROWS = (256, 192, 64)
LANES = 128
FIRST_ROWS = (128, 384)


def sum_rows():
    return -(-sum(RELAY_ROWS[:-1]) // LANES), -(-RELAY_ROWS[-1] // LANES)


def _kernel(
    tp_size, d_model,
    a_hbm, w_hbm, r_hbm, g_hbm, hid, nrm,
    a, w, p, rx, relay_out, relay_in, res, gain, hbuf, sq_out, sq_in,
    a_sem, w_sem, send_sem, recv_sem, rrecv_sem, qsend_sem, qrecv_sem,
):
    rows, d_local = r_hbm.shape
    half = d_local // 2
    nu = half // UNIT
    per_group = CORES * 2 * nu
    total = CHIPS * per_group
    chunks = rows // RB

    me = lax.axis_index("tp")
    x, c = lax.div(me, CORES), lax.rem(me, CORES)

    flip = lax.div(CHIPS - x, CHIPS)

    def chip(offset, core):
        return lax.rem(x + offset, CHIPS) * CORES + core

    def decode(s):
        g, j = lax.div(s, per_group), lax.rem(s, per_group)
        late = lax.div(lax.div(s, 2 * nu) + 7, 8)
        more = lax.div(lax.div(s, 2) + 1, 2)
        b = late * lax.div(j, nu) + (1 - late) * ((1 - more) * s + more * (lax.div(s, 2) - 1))
        i = late * lax.rem(j, nu) + (1 - late) * more * (1 + lax.rem(s, 2))
        return g, i, b, lax.rem(lax.div(b, 2) + 1 + c, 2), lax.rem(b + c + flip, 2)

    def w_copy(s):
        g, i, _, e, h = decode(s)
        o = lax.rem(6 - g + 2 * h * lax.rem(g, 2), CHIPS)
        col = pl.multiple_of(chip(o, e) * d_local + h * half + i * UNIT, UNIT)
        k = lax.rem(s, W_SLOTS)
        return pltpu.make_async_copy(w_hbm.at[:, pl.ds(col, UNIT)], w.at[k], w_sem.at[k])

    def w_first(part):
        _, _, _, e, h = decode(jnp.int32(0))
        cols = UNIT // 2
        col = pl.multiple_of(chip(2, e) * d_local + h * half + part * cols, cols)
        return pltpu.make_async_copy(
            w_hbm.at[:, pl.ds(col, cols)], w.at[0, :, pl.ds(part * cols, cols)], w_sem.at[part * W_SLOTS])

    first_lo = [sum(FIRST_ROWS[:b]) for b in range(len(FIRST_ROWS))]

    def a_copy(b):
        rs = pl.ds(first_lo[b], FIRST_ROWS[b])
        return pltpu.make_async_copy(a_hbm.at[rs, :], a.at[rs, :], a_sem.at[b])

    def send(src, dst, group, target):
        pltpu.make_async_remote_copy(
            src_ref=src, dst_ref=dst, send_sem=send_sem.at[0], recv_sem=recv_sem.at[group],
            device_id={"tp": target}, device_id_type=MESH).start()

    def send_units(g, b, lo, n, block, group, target):
        send(p.at[pl.ds((g * 4 + b) * nu + lo, n)], rx.at[pl.ds(block * nu + lo, n)], group, target)

    def wait_bytes(ref, sem):
        pltpu.make_async_copy(ref, ref, sem).wait()

    def local_unit(g, h, i):
        return (g * 4 + (2 if g == 2 else 0) + lax.rem(h + c + flip, 2)) * nu + i

    relay_lo = [sum(RELAY_ROWS[:m]) for m in range(len(RELAY_ROWS))]

    def relay_rows(m):
        return pl.ds(relay_lo[m], RELAY_ROWS[m])

    def send_relay(m):
        for h in range(2):
            pltpu.make_async_remote_copy(
                src_ref=relay_out.at[h, relay_rows(m)], dst_ref=relay_in.at[h, relay_rows(m)],
                send_sem=send_sem.at[0], recv_sem=rrecv_sem.at[m],
                device_id={"tp": chip(3 - 2 * h, 1 - c)}, device_id_type=MESH).start()

    def chunk_rows(r):
        return pl.ds(pl.multiple_of(r * RB, RB), RB)

    def span(lo, n):
        return pl.ds(pl.multiple_of(lo, n), n)

    w_first(0).start()
    a_copy(0).start()
    w_first(1).start()
    w_copy(jnp.int32(1)).start()

    peers = [x * CORES + 1 - c] + [chip(o, core) for o in (1, CHIPS - 1) for core in range(CORES)]
    barrier = pltpu.get_barrier_semaphore()
    for peer in peers:
        pl.semaphore_signal(barrier, inc=1, device_id={"tp": peer}, device_id_type=MESH)

    for b in range(1, len(FIRST_ROWS)):
        a_copy(b).start()
    r_copy = pltpu.make_async_copy(r_hbm, res, a_sem.at[0])
    g_copy = pltpu.make_async_copy(g_hbm, gain, a_sem.at[1])

    def piece(s, b, lo, n):
        _, _, block, e0, h0 = decode(jnp.int32(s))
        rs, cols, unit = pl.ds(first_lo[b], FIRST_ROWS[b]), pl.ds(lo, n), block * nu
        p[unit, rs, cols] = jnp.dot(
            a[rs, :], w[s, :, cols], preferred_element_type=jnp.float32).astype(p.dtype)
        if (s, b, lo) == (0, 0, 0):
            with jax.named_scope("bar"):
                pl.semaphore_wait(barrier, len(peers))
        send(p.at[unit, rs, cols], rx.at[(h0 * 2 + c) * nu, rs, cols], 0, chip(3 + 2 * h0, 1 - e0))

    with jax.named_scope("w0"):
        w_first(0).wait()
        a_copy(0).wait()
    for k in range(2, W_SLOTS):
        w_copy(jnp.int32(k)).start()
    piece(0, 0, 0, UNIT // 2)
    with jax.named_scope("w0b"):
        w_first(1).wait()
    piece(0, 0, UNIT // 2, UNIT // 2)
    with jax.named_scope("w1"):
        w_copy(jnp.int32(1)).wait()
    piece(1, 0, 0, UNIT)
    for b in range(1, len(FIRST_ROWS)):
        with jax.named_scope("awt"):
            a_copy(b).wait()
        for s in range(2):
            piece(s, b, 0, UNIT)
    for s in range(2):
        w_copy(jnp.int32(s + W_SLOTS)).start()
    r_copy.start()
    g_copy.start()

    @pl.loop(2, total)
    def _(s):
        g, i, b, e, h = decode(s)
        w_copy(s).wait()
        k = lax.rem(s, W_SLOTS)
        p[(g * 4 + b) * nu + i] = jnp.dot(
            a[...], w[k], preferred_element_type=jnp.float32).astype(p.dtype)

        @pl.when(s + W_SLOTS < total)
        def _():
            w_copy(s + W_SLOTS).start()

        def to_relay(lo, n):
            send_units(g, b, lo, n, h * 2 + c, 0, chip(3 + 2 * h, 1 - e))

        @pl.when(i == nu - 1)
        def _():
            @pl.when(s < 2 * nu)
            def _():
                to_relay(1, nu - 1)

            @pl.when(jnp.logical_and(g == 0, s >= 2 * nu))
            def _():
                to_relay(0, nu)

            @pl.when(g == 1)
            def _():
                send_units(g, b, 0, nu, 4 + h * 2 + c, 1, chip(1 + 2 * h, e))

            @pl.when(jnp.logical_or(jnp.logical_and(g == 2, b < 2), jnp.logical_and(g == 3, b >= 2)))
            def _():
                send_units(g, b, 0, nu, 4 + g * 2 + h, 3 - g, x * CORES + 1 - c)

    with jax.named_scope("l2r"):
        wait_bytes(rx.at[pl.ds(0, 6 * nu)], recv_sem.at[0])

    @pl.loop(0, chunks)
    def _(r):
        rs = chunk_rows(r)
        for h in range(2):
            for i in range(nu):
                acc = p[local_unit(3, h, i), rs, :].astype(jnp.float32)
                acc += rx[(10 + h) * nu + i, rs, :].astype(jnp.float32)
                acc += rx[(h * 2) * nu + i, rs, :].astype(jnp.float32)
                acc += rx[(h * 2 + 1) * nu + i, rs, :].astype(jnp.float32)
                relay_out[h, rs, i * UNIT:(i + 1) * UNIT] = acc

    for m in range(len(RELAY_ROWS)):
        send_relay(m)

    r_copy.wait()
    g_copy.wait()
    with jax.named_scope("direct"):
        wait_bytes(rx.at[pl.ds(0, 6 * nu)], recv_sem.at[1])

    sq_n = sum_rows()
    sq_lo = (0, sq_n[0])

    def on_lane(lane, n):
        return (lax.broadcasted_iota(jnp.int32, (n, LANES), 0) + lane
                == lax.broadcasted_iota(jnp.int32, (n, LANES), 1))

    def columns():
        for h in range(2):
            for i in range(nu):
                yield h, i, slice(h * half + i * UNIT, h * half + (i + 1) * UNIT)

    def add_early(lo, n):
        rs = span(lo, n)
        for h, i, cols in columns():
            acc = p[local_unit(2, h, i), rs, :].astype(jnp.float32)
            acc += rx[(8 + h) * nu + i, rs, :].astype(jnp.float32)
            acc += rx[(4 + h * 2) * nu + i, rs, :].astype(jnp.float32)
            acc += rx[(5 + h * 2) * nu + i, rs, :].astype(jnp.float32)
            hbuf[rs, cols] = acc + res[rs, cols].astype(jnp.float32)

    def finish(m, lo, n):
        rs = span(lo, n)
        sq = jnp.zeros((n, UNIT), jnp.float32)
        for h, i, cols in columns():
            acc = hbuf[rs, cols] + relay_in[h, rs, i * UNIT:(i + 1) * UNIT]
            hbuf[rs, cols] = acc
            sq += acc * acc
        sq = jnp.sum(sq, axis=1, keepdims=True)
        q, lane = place(m, lo)
        sq_out[q] += jnp.sum(
            jnp.where(on_lane(lane, n), jnp.broadcast_to(sq, (n, LANES)), 0.0), axis=0, keepdims=True)

    def place(m, lo):
        if m == len(RELAY_ROWS) - 1:
            lo = lo - relay_lo[m]
            return sq_lo[1] + lax.div(lo, LANES), lax.rem(lo, LANES)
        return lax.div(lo, LANES), lax.rem(lo, LANES)

    closing = flip + lax.div(x, CHIPS - 1)
    first = closing * (1 + 2 * flip) + (1 - closing) * 2
    second = 1 + closing
    others = [chip(o, core) for o in (first, second, 6 - first - second) for core in range(CORES)]
    others.append(x * CORES + 1 - c)

    def send_sums(k):
        for target in others:
            pltpu.make_async_remote_copy(
                src_ref=sq_out.at[sq_span(k)], dst_ref=sq_in.at[me, sq_span(k)],
                send_sem=qsend_sem.at[0], recv_sem=qrecv_sem.at[k],
                device_id={"tp": target}, device_id_type=MESH).start()
        for q in range(sq_lo[k], sq_lo[k] + sq_n[k]):
            sq_in[me, q] = sq_out[q]

    def sq_span(k):
        return pl.ds(sq_lo[k], sq_n[k])

    def wait_sums(k, sem):
        wait_bytes(sq_in.at[pl.ds(0, tp_size - 1), sq_span(k)], sem.at[k])

    def normalise(m, lo, n):
        q, lane = place(m, lo)
        tot = sq_in[0, q]
        for t in range(1, tp_size):
            tot += sq_in[t, q]
        col = jnp.sum(jnp.where(on_lane(lane, n), jnp.broadcast_to(tot, (n, LANES)), 0.0), axis=1, keepdims=True)
        scale = lax.rsqrt(col / d_model + EPS)
        rs = span(lo, n)
        nrm[rs, :] = (hbuf[rs, :] * scale * gain[...].reshape(1, d_local)).astype(nrm.dtype)

    def write_hidden(lo, n):
        rs = span(lo, n)
        hid[rs, :] = hbuf[rs, :].astype(hid.dtype)

    def each(m, *steps):
        lo, hi = relay_lo[m], relay_lo[m] + RELAY_ROWS[m]
        whole = (hi - lo) // RB * RB

        if whole:
            @pl.loop(0, whole // RB)
            def _(r):
                for step in steps:
                    step(lo + r * RB, RB)

        if lo + whole < hi:
            for step in steps:
                step(lo + whole, hi - lo - whole)

    def wait_relay(m):
        with jax.named_scope(f"r{m}"):
            wait_bytes(relay_in.at[:, relay_rows(m)], rrecv_sem.at[m])

    for q in range(sum(sq_n)):
        sq_out[q] = jnp.zeros((1, LANES), jnp.float32)
    last = len(RELAY_ROWS) - 1
    for m in range(last + 1):
        each(m, add_early)
        wait_relay(m)
        each(m, functools.partial(finish, m))
        if m >= last - 1:
            send_sums(m - last + 1)
        each(m, write_hidden)

    wait_bytes(p, send_sem.at[0])
    for m in range(last + 1):
        if m in (0, last):
            with jax.named_scope(f"sq{m}"):
                wait_sums(min(m, 1), qrecv_sem)
        each(m, functools.partial(normalise, m))
    with jax.named_scope("qdrain"):
        wait_bytes(sq_in.at[pl.ds(0, tp_size - 1)], qsend_sem.at[0])


def _write(hid, nrm, hid_hbm, nrm_hbm, sem):
    blocks = 4
    rows = hid.shape[0] // blocks
    pairs = ((hid, hid_hbm), (nrm, nrm_hbm))
    for k, (src, dst) in enumerate(pairs):
        for b in range(blocks):
            rs = pl.ds(b * rows, rows)
            pltpu.make_async_copy(src.at[rs, :], dst.at[rs, :], sem.at[k]).start()
    for k, (src, dst) in enumerate(pairs):
        pltpu.make_async_copy(src, dst, sem.at[k]).wait()


def solution(mesh):
    tp_size = mesh.shape["tp"]

    def local_step(attn_blk, w_blk, resid_blk, gain_blk):
        rows, k_dim = attn_blk.shape
        d_local = resid_blk.shape[1]
        d_model = w_blk.shape[1]
        half = d_local // 2
        nu = half // UNIT
        units = tp_size * 2 * nu
        sq_rows = sum(sum_rows())
        assert tp_size == CORES * CHIPS and half % UNIT == 0
        assert sum(FIRST_ROWS) == sum(RELAY_ROWS) == rows and rows % RB == 0 and nu == 3
        hbm_spec = pl.BlockSpec(memory_space=pltpu.HBM)
        vmem_spec = pl.BlockSpec(memory_space=pltpu.VMEM)
        dma = pltpu.SemaphoreType.DMA
        out_shape = [jax.ShapeDtypeStruct((rows, d_local), jnp.bfloat16)] * 2
        hid, nrm = pl.pallas_call(
            functools.partial(_kernel, tp_size, d_model),
            out_shape=[pltpu.VMEM((rows, d_local), jnp.bfloat16)] * 2,
            in_specs=[hbm_spec] * 4,
            out_specs=[vmem_spec] * 2,
            scratch_shapes=[
                pltpu.VMEM((rows, k_dim), jnp.bfloat16),
                pltpu.VMEM((W_SLOTS, k_dim, UNIT), jnp.bfloat16),
                pltpu.VMEM((units, rows, UNIT), jnp.bfloat16),
                pltpu.VMEM((12 * nu, rows, UNIT), jnp.bfloat16),
                pltpu.VMEM((2, rows, half), jnp.float32),
                pltpu.VMEM((2, rows, half), jnp.float32),
                pltpu.VMEM((rows, d_local), jnp.bfloat16),
                pltpu.VMEM((d_local,), jnp.float32),
                pltpu.VMEM((rows, d_local), jnp.float32),
                pltpu.VMEM((sq_rows, 1, LANES), jnp.float32),
                pltpu.VMEM((tp_size, sq_rows, 1, LANES), jnp.float32),
                dma((len(FIRST_ROWS),)),
                dma((W_SLOTS + 1,)),
                dma((1,)),
                dma((2,)),
                dma((len(RELAY_ROWS),)),
                dma((1,)),
                dma((2,)),
            ],
            compiler_params=pltpu.CompilerParams(
                collective_id=0, has_side_effects=True, vmem_limit_bytes=62 * 1000 * 1000
            ),
            name="proj_scatter_norm",
        )(attn_blk, w_blk, resid_blk, gain_blk)
        return pl.pallas_call(
            _write,
            out_shape=out_shape,
            in_specs=[vmem_spec] * 2,
            out_specs=[hbm_spec] * 2,
            scratch_shapes=[dma((2,))],
            compiler_params=pltpu.CompilerParams(vmem_limit_bytes=8 * 1024 * 1024),
            name="write_out",
        )(hid, nrm)

    return jax.shard_map(
        local_step,
        mesh=mesh,
        in_specs=(P("data", "tp"), P("tp", None), P("data", "tp"), P("tp")),
        out_specs=(P("data", "tp"), P("data", "tp")),
        check_vma=False,
    )
```

```python
import functools

import jax
import jax.numpy as jnp
from jax import lax
from jax.experimental import pallas as pl
from jax.experimental.pallas import tpu as pltpu
from jax.sharding import PartitionSpec as P

EPS = 1e-5
MESH = pl.DeviceIdType.MESH
CORES = 2
CHIPS = 4
UNIT = 256
W_SLOTS = 4
RB = 64
RELAY_ROWS = (256, 192, 64)
LANES = 128
FIRST_ROWS = (128, 384)


def sum_rows():
    return -(-sum(RELAY_ROWS[:-1]) // LANES), -(-RELAY_ROWS[-1] // LANES)


def _kernel(
    tp_size, d_model,
    a_hbm, w_hbm, r_hbm, g_hbm, hid, nrm,
    a, w, p, rx, relay_out, relay_in, res, gain, hbuf, sq_out, sq_in,
    a_sem, w_sem, send_sem, recv_sem, rrecv_sem, qsend_sem, qrecv_sem,
):
    rows, d_local = r_hbm.shape
    half = d_local // 2
    nu = half // UNIT
    per_group = CORES * 2 * nu
    total = CHIPS * per_group
    chunks = rows // RB

    me = lax.axis_index("tp")
    x, c = lax.div(me, CORES), lax.rem(me, CORES)

    at_first, at_last = lax.div(CHIPS - x, CHIPS), lax.div(x, CHIPS - 1)
    flip = at_first + at_last

    def chip(offset, core):
        return lax.rem(x + offset, CHIPS) * CORES + core

    def decode(s):
        g, j = lax.div(s, per_group), lax.rem(s, per_group)
        late = lax.div(lax.div(s, 2 * nu) + 7, 8)
        more = lax.div(lax.div(s, 2) + 1, 2)
        b = late * lax.div(j, nu) + (1 - late) * ((1 - more) * s + more * (lax.div(s, 2) - 1))
        i = late * lax.rem(j, nu) + (1 - late) * more * (1 + lax.rem(s, 2))
        return g, i, b, lax.rem(lax.div(b, 2) + 1 + c, 2), lax.rem(b + c + flip, 2)

    def w_copy(s):
        g, i, _, e, h = decode(s)
        o = lax.rem(6 - g + 2 * h * lax.rem(g, 2), CHIPS)
        col = pl.multiple_of(chip(o, e) * d_local + h * half + i * UNIT, UNIT)
        k = lax.rem(s, W_SLOTS)
        return pltpu.make_async_copy(w_hbm.at[:, pl.ds(col, UNIT)], w.at[k], w_sem.at[k])

    first_lo = [sum(FIRST_ROWS[:b]) for b in range(len(FIRST_ROWS))]

    def a_copy(b):
        rs = pl.ds(first_lo[b], FIRST_ROWS[b])
        return pltpu.make_async_copy(a_hbm.at[rs, :], a.at[rs, :], a_sem.at[b])

    def send(src, dst, group, target):
        pltpu.make_async_remote_copy(
            src_ref=src, dst_ref=dst, send_sem=send_sem.at[0], recv_sem=recv_sem.at[group],
            device_id={"tp": target}, device_id_type=MESH).start()

    def send_units(g, b, lo, n, block, group, target):
        send(p.at[pl.ds((g * 4 + b) * nu + lo, n)], rx.at[pl.ds(block * nu + lo, n)], group, target)

    def wait_bytes(ref, sem):
        pltpu.make_async_copy(ref, ref, sem).wait()

    def local_unit(g, h, i):
        return (g * 4 + (2 if g == 2 else 0) + lax.rem(h + c + flip, 2)) * nu + i

    relay_lo = [sum(RELAY_ROWS[:m]) for m in range(len(RELAY_ROWS))]

    def relay_rows(m):
        return pl.ds(relay_lo[m], RELAY_ROWS[m])

    def send_relay(m):
        for h in range(2):
            pltpu.make_async_remote_copy(
                src_ref=relay_out.at[h, relay_rows(m)], dst_ref=relay_in.at[h, relay_rows(m)],
                send_sem=send_sem.at[0], recv_sem=rrecv_sem.at[m],
                device_id={"tp": chip(3 - 2 * h, 1 - c)}, device_id_type=MESH).start()

    def chunk_rows(r):
        return pl.ds(pl.multiple_of(r * RB, RB), RB)

    def span(lo, n):
        return pl.ds(pl.multiple_of(lo, n), n)

    w_copy(jnp.int32(0)).start()
    a_copy(0).start()
    w_copy(jnp.int32(1)).start()

    peers = [x * CORES + 1 - c] + [chip(o, core) for o in (1, CHIPS - 1) for core in range(CORES)]
    barrier = pltpu.get_barrier_semaphore()
    for peer in peers:
        pl.semaphore_signal(barrier, inc=1, device_id={"tp": peer}, device_id_type=MESH)

    for b in range(1, len(FIRST_ROWS)):
        a_copy(b).start()
    r_copy = pltpu.make_async_copy(r_hbm, res, a_sem.at[0])
    g_copy = pltpu.make_async_copy(g_hbm, gain, a_sem.at[1])

    for b in range(len(FIRST_ROWS)):
        rs = pl.ds(first_lo[b], FIRST_ROWS[b])
        for s in range(2):
            _, _, block, e0, h0 = decode(jnp.int32(s))
            if b == 0:
                with jax.named_scope(f"w{s}"):
                    w_copy(jnp.int32(s)).wait()
            if s == 0:
                with jax.named_scope("awt"):
                    a_copy(b).wait()
            if b == 0 and s == 0:
                for k in range(2, W_SLOTS):
                    w_copy(jnp.int32(k)).start()
            unit = block * nu
            p[unit, rs, :] = jnp.dot(a[rs, :], w[s], preferred_element_type=jnp.float32).astype(p.dtype)
            if b == 0 and s == 0:
                with jax.named_scope("bar"):
                    pl.semaphore_wait(barrier, len(peers))
            send(p.at[unit, rs], rx.at[(h0 * 2 + c) * nu, rs], 0, chip(3 + 2 * h0, 1 - e0))
    for s in range(2):
        w_copy(jnp.int32(s + W_SLOTS)).start()
    r_copy.start()
    g_copy.start()

    @pl.loop(2, total)
    def _(s):
        g, i, b, e, h = decode(s)
        w_copy(s).wait()
        k = lax.rem(s, W_SLOTS)
        p[(g * 4 + b) * nu + i] = jnp.dot(
            a[...], w[k], preferred_element_type=jnp.float32).astype(p.dtype)

        @pl.when(s + W_SLOTS < total)
        def _():
            w_copy(s + W_SLOTS).start()

        def to_relay(lo, n):
            send_units(g, b, lo, n, h * 2 + c, 0, chip(3 + 2 * h, 1 - e))

        @pl.when(i == nu - 1)
        def _():
            @pl.when(s < 2 * nu)
            def _():
                to_relay(1, nu - 1)

            @pl.when(jnp.logical_and(g == 0, s >= 2 * nu))
            def _():
                to_relay(0, nu)

            @pl.when(g == 1)
            def _():
                send_units(g, b, 0, nu, 4 + h * 2 + c, 1, chip(1 + 2 * h, e))

            @pl.when(jnp.logical_or(jnp.logical_and(g == 2, b < 2), jnp.logical_and(g == 3, b >= 2)))
            def _():
                send_units(g, b, 0, nu, 4 + g * 2 + h, 3 - g, x * CORES + 1 - c)

    with jax.named_scope("l2r"):
        wait_bytes(rx.at[pl.ds(0, 6 * nu)], recv_sem.at[0])

    @pl.loop(0, chunks)
    def _(r):
        rs = chunk_rows(r)
        for h in range(2):
            for i in range(nu):
                acc = p[local_unit(3, h, i), rs, :].astype(jnp.float32)
                acc += rx[(10 + h) * nu + i, rs, :].astype(jnp.float32)
                acc += rx[(h * 2) * nu + i, rs, :].astype(jnp.float32)
                acc += rx[(h * 2 + 1) * nu + i, rs, :].astype(jnp.float32)
                relay_out[h, rs, i * UNIT:(i + 1) * UNIT] = acc

    for m in range(len(RELAY_ROWS)):
        send_relay(m)

    r_copy.wait()
    g_copy.wait()
    with jax.named_scope("direct"):
        wait_bytes(rx.at[pl.ds(0, 6 * nu)], recv_sem.at[1])

    sq_n = sum_rows()
    sq_lo = (0, sq_n[0])

    def on_lane(lane, n):
        return (lax.broadcasted_iota(jnp.int32, (n, LANES), 0) + lane
                == lax.broadcasted_iota(jnp.int32, (n, LANES), 1))

    def columns():
        for h in range(2):
            for i in range(nu):
                yield h, i, slice(h * half + i * UNIT, h * half + (i + 1) * UNIT)

    def add_early(lo, n):
        rs = span(lo, n)
        for h, i, cols in columns():
            acc = p[local_unit(2, h, i), rs, :].astype(jnp.float32)
            acc += rx[(8 + h) * nu + i, rs, :].astype(jnp.float32)
            acc += rx[(4 + h * 2) * nu + i, rs, :].astype(jnp.float32)
            acc += rx[(5 + h * 2) * nu + i, rs, :].astype(jnp.float32)
            hbuf[rs, cols] = acc + res[rs, cols].astype(jnp.float32)

    def finish(m, lo, n):
        rs = span(lo, n)
        sq = jnp.zeros((n, UNIT), jnp.float32)
        for h, i, cols in columns():
            acc = hbuf[rs, cols] + relay_in[h, rs, i * UNIT:(i + 1) * UNIT]
            hbuf[rs, cols] = acc
            sq += acc * acc
        sq = jnp.sum(sq, axis=1, keepdims=True)
        q, lane = place(m, lo)
        sq_out[q] += jnp.sum(
            jnp.where(on_lane(lane, n), jnp.broadcast_to(sq, (n, LANES)), 0.0), axis=0, keepdims=True)

    def place(m, lo):
        if m == len(RELAY_ROWS) - 1:
            lo = lo - relay_lo[m]
            return sq_lo[1] + lax.div(lo, LANES), lax.rem(lo, LANES)
        return lax.div(lo, LANES), lax.rem(lo, LANES)

    first = 3 * at_first + at_last + 2 * (1 - flip)
    second = 1 + flip
    others = [chip(o, core) for o in (first, second, 6 - first - second) for core in range(CORES)]
    others.append(x * CORES + 1 - c)

    def send_sums(k):
        for target in others:
            pltpu.make_async_remote_copy(
                src_ref=sq_out.at[sq_span(k)], dst_ref=sq_in.at[me, sq_span(k)],
                send_sem=qsend_sem.at[0], recv_sem=qrecv_sem.at[k],
                device_id={"tp": target}, device_id_type=MESH).start()
        for q in range(sq_lo[k], sq_lo[k] + sq_n[k]):
            sq_in[me, q] = sq_out[q]

    def sq_span(k):
        return pl.ds(sq_lo[k], sq_n[k])

    def wait_sums(k, sem):
        wait_bytes(sq_in.at[pl.ds(0, tp_size - 1), sq_span(k)], sem.at[k])

    def normalise(m, lo, n):
        q, lane = place(m, lo)
        tot = sq_in[0, q]
        for t in range(1, tp_size):
            tot += sq_in[t, q]
        col = jnp.sum(jnp.where(on_lane(lane, n), jnp.broadcast_to(tot, (n, LANES)), 0.0), axis=1, keepdims=True)
        scale = lax.rsqrt(col / d_model + EPS)
        rs = span(lo, n)
        nrm[rs, :] = (hbuf[rs, :] * scale * gain[...].reshape(1, d_local)).astype(nrm.dtype)

    def write_hidden(lo, n):
        rs = span(lo, n)
        hid[rs, :] = hbuf[rs, :].astype(hid.dtype)

    def each(m, *steps):
        lo, hi = relay_lo[m], relay_lo[m] + RELAY_ROWS[m]
        whole = (hi - lo) // RB * RB

        if whole:
            @pl.loop(0, whole // RB)
            def _(r):
                for step in steps:
                    step(lo + r * RB, RB)

        if lo + whole < hi:
            for step in steps:
                step(lo + whole, hi - lo - whole)

    def wait_relay(m):
        with jax.named_scope(f"r{m}"):
            wait_bytes(relay_in.at[:, relay_rows(m)], rrecv_sem.at[m])

    for q in range(sum(sq_n)):
        sq_out[q] = jnp.zeros((1, LANES), jnp.float32)
    last = len(RELAY_ROWS) - 1
    for m in range(last + 1):
        each(m, add_early)
        wait_relay(m)
        each(m, functools.partial(finish, m))
        if m >= last - 1:
            send_sums(m - last + 1)
        each(m, write_hidden)

    wait_bytes(p, send_sem.at[0])
    for m in range(last + 1):
        if m in (0, last):
            with jax.named_scope(f"sq{m}"):
                wait_sums(min(m, 1), qrecv_sem)
        each(m, functools.partial(normalise, m))
    with jax.named_scope("qdrain"):
        wait_bytes(sq_in.at[pl.ds(0, tp_size - 1)], qsend_sem.at[0])


def _write(hid, nrm, hid_hbm, nrm_hbm, sem):
    blocks = 4
    rows = hid.shape[0] // blocks
    pairs = ((hid, hid_hbm), (nrm, nrm_hbm))
    for k, (src, dst) in enumerate(pairs):
        for b in range(blocks):
            rs = pl.ds(b * rows, rows)
            pltpu.make_async_copy(src.at[rs, :], dst.at[rs, :], sem.at[k]).start()
    for k, (src, dst) in enumerate(pairs):
        pltpu.make_async_copy(src, dst, sem.at[k]).wait()


def solution(mesh):
    tp_size = mesh.shape["tp"]

    def local_step(attn_blk, w_blk, resid_blk, gain_blk):
        rows, k_dim = attn_blk.shape
        d_local = resid_blk.shape[1]
        d_model = w_blk.shape[1]
        half = d_local // 2
        nu = half // UNIT
        units = tp_size * 2 * nu
        sq_rows = sum(sum_rows())
        assert tp_size == CORES * CHIPS and half % UNIT == 0
        assert sum(FIRST_ROWS) == sum(RELAY_ROWS) == rows and rows % RB == 0 and nu == 3
        hbm_spec = pl.BlockSpec(memory_space=pltpu.HBM)
        vmem_spec = pl.BlockSpec(memory_space=pltpu.VMEM)
        dma = pltpu.SemaphoreType.DMA
        out_shape = [jax.ShapeDtypeStruct((rows, d_local), jnp.bfloat16)] * 2
        hid, nrm = pl.pallas_call(
            functools.partial(_kernel, tp_size, d_model),
            out_shape=[pltpu.VMEM((rows, d_local), jnp.bfloat16)] * 2,
            in_specs=[hbm_spec] * 4,
            out_specs=[vmem_spec] * 2,
            scratch_shapes=[
                pltpu.VMEM((rows, k_dim), jnp.bfloat16),
                pltpu.VMEM((W_SLOTS, k_dim, UNIT), jnp.bfloat16),
                pltpu.VMEM((units, rows, UNIT), jnp.bfloat16),
                pltpu.VMEM((12 * nu, rows, UNIT), jnp.bfloat16),
                pltpu.VMEM((2, rows, half), jnp.float32),
                pltpu.VMEM((2, rows, half), jnp.float32),
                pltpu.VMEM((rows, d_local), jnp.bfloat16),
                pltpu.VMEM((d_local,), jnp.float32),
                pltpu.VMEM((rows, d_local), jnp.float32),
                pltpu.VMEM((sq_rows, 1, LANES), jnp.float32),
                pltpu.VMEM((tp_size, sq_rows, 1, LANES), jnp.float32),
                dma((len(FIRST_ROWS),)),
                dma((W_SLOTS,)),
                dma((1,)),
                dma((2,)),
                dma((len(RELAY_ROWS),)),
                dma((1,)),
                dma((2,)),
            ],
            compiler_params=pltpu.CompilerParams(
                collective_id=0, has_side_effects=True, vmem_limit_bytes=62 * 1000 * 1000
            ),
            name="proj_scatter_norm",
        )(attn_blk, w_blk, resid_blk, gain_blk)
        return pl.pallas_call(
            _write,
            out_shape=out_shape,
            in_specs=[vmem_spec] * 2,
            out_specs=[hbm_spec] * 2,
            scratch_shapes=[dma((2,))],
            compiler_params=pltpu.CompilerParams(vmem_limit_bytes=8 * 1024 * 1024),
            name="write_out",
        )(hid, nrm)

    return jax.shard_map(
        local_step,
        mesh=mesh,
        in_specs=(P("data", "tp"), P("tp", None), P("data", "tp"), P("tp")),
        out_specs=(P("data", "tp"), P("data", "tp")),
        check_vma=False,
    )
```

```python
import functools

import jax
import jax.numpy as jnp
from jax import lax
from jax.experimental import pallas as pl
from jax.experimental.pallas import tpu as pltpu
from jax.sharding import PartitionSpec as P

EPS = 1e-5
MESH = pl.DeviceIdType.MESH
CORES = 2
CHIPS = 4
UNIT = 256
W_SLOTS = 4
RB = 64
RELAY_ROWS = (256, 192, 32, 32)
EARLY = 2
LANES = 128
FIRST_ROWS = (128, 384)


def sum_rows():
    return -(-sum(RELAY_ROWS[:EARLY]) // LANES), -(-sum(RELAY_ROWS[EARLY:]) // LANES)


def _kernel(
    tp_size, d_model,
    a_hbm, w_hbm, r_hbm, g_hbm, hid, nrm,
    a, w, p, rx, relay_out, relay_in, res, gain, hbuf, sq_out, sq_in,
    a_sem, w_sem, send_sem, recv_sem, rrecv_sem, qsend_sem, qrecv_sem,
):
    rows, d_local = r_hbm.shape
    half = d_local // 2
    nu = half // UNIT
    per_group = CORES * 2 * nu
    total = CHIPS * per_group
    chunks = rows // RB

    me = lax.axis_index("tp")
    x, c = lax.div(me, CORES), lax.rem(me, CORES)

    at_first, at_last = lax.div(CHIPS - x, CHIPS), lax.div(x, CHIPS - 1)
    flip = at_first + at_last

    def chip(offset, core):
        return lax.rem(x + offset, CHIPS) * CORES + core

    def decode(s):
        g, j = lax.div(s, per_group), lax.rem(s, per_group)
        late = lax.div(lax.div(s, 2 * nu) + 7, 8)
        more = lax.div(lax.div(s, 2) + 1, 2)
        b = late * lax.div(j, nu) + (1 - late) * ((1 - more) * s + more * (lax.div(s, 2) - 1))
        i = late * lax.rem(j, nu) + (1 - late) * more * (1 + lax.rem(s, 2))
        return g, i, b, lax.rem(lax.div(b, 2) + 1 + c, 2), lax.rem(b + c + flip, 2)

    def w_copy(s):
        g, i, _, e, h = decode(s)
        o = lax.rem(6 - g + 2 * h * lax.rem(g, 2), CHIPS)
        col = pl.multiple_of(chip(o, e) * d_local + h * half + i * UNIT, UNIT)
        k = lax.rem(s, W_SLOTS)
        return pltpu.make_async_copy(w_hbm.at[:, pl.ds(col, UNIT)], w.at[k], w_sem.at[k])

    first_lo = [sum(FIRST_ROWS[:b]) for b in range(len(FIRST_ROWS))]

    def a_copy(b):
        rs = pl.ds(first_lo[b], FIRST_ROWS[b])
        return pltpu.make_async_copy(a_hbm.at[rs, :], a.at[rs, :], a_sem.at[b])

    def send(src, dst, group, target):
        pltpu.make_async_remote_copy(
            src_ref=src, dst_ref=dst, send_sem=send_sem.at[0], recv_sem=recv_sem.at[group],
            device_id={"tp": target}, device_id_type=MESH).start()

    def send_units(g, b, lo, n, block, group, target):
        send(p.at[pl.ds((g * 4 + b) * nu + lo, n)], rx.at[pl.ds(block * nu + lo, n)], group, target)

    def wait_bytes(ref, sem):
        pltpu.make_async_copy(ref, ref, sem).wait()

    def local_unit(g, h, i):
        return (g * 4 + (2 if g == 2 else 0) + lax.rem(h + c + flip, 2)) * nu + i

    relay_lo = [sum(RELAY_ROWS[:m]) for m in range(len(RELAY_ROWS))]

    def relay_rows(m):
        return pl.ds(relay_lo[m], RELAY_ROWS[m])

    def send_relay(m):
        for h in range(2):
            pltpu.make_async_remote_copy(
                src_ref=relay_out.at[h, relay_rows(m)], dst_ref=relay_in.at[h, relay_rows(m)],
                send_sem=send_sem.at[0], recv_sem=rrecv_sem.at[m],
                device_id={"tp": chip(3 - 2 * h, 1 - c)}, device_id_type=MESH).start()

    def chunk_rows(r):
        return pl.ds(pl.multiple_of(r * RB, RB), RB)

    def span(lo, n):
        return pl.ds(pl.multiple_of(lo, n), n)

    w_copy(jnp.int32(0)).start()
    a_copy(0).start()
    w_copy(jnp.int32(1)).start()

    peers = [x * CORES + 1 - c] + [chip(o, core) for o in (1, CHIPS - 1) for core in range(CORES)]
    barrier = pltpu.get_barrier_semaphore()
    for peer in peers:
        pl.semaphore_signal(barrier, inc=1, device_id={"tp": peer}, device_id_type=MESH)

    for b in range(1, len(FIRST_ROWS)):
        a_copy(b).start()
    r_copy = pltpu.make_async_copy(r_hbm, res, a_sem.at[0])
    g_copy = pltpu.make_async_copy(g_hbm, gain, a_sem.at[1])

    for b in range(len(FIRST_ROWS)):
        rs = pl.ds(first_lo[b], FIRST_ROWS[b])
        for s in range(2):
            _, _, block, e0, h0 = decode(jnp.int32(s))
            if b == 0:
                with jax.named_scope(f"w{s}"):
                    w_copy(jnp.int32(s)).wait()
            if s == 0:
                with jax.named_scope("awt"):
                    a_copy(b).wait()
            if b == 0 and s == 0:
                for k in range(2, W_SLOTS):
                    w_copy(jnp.int32(k)).start()
            unit = block * nu
            p[unit, rs, :] = jnp.dot(a[rs, :], w[s], preferred_element_type=jnp.float32).astype(p.dtype)
            if b == 0 and s == 0:
                with jax.named_scope("bar"):
                    pl.semaphore_wait(barrier, len(peers))
            send(p.at[unit, rs], rx.at[(h0 * 2 + c) * nu, rs], 0, chip(3 + 2 * h0, 1 - e0))
    for s in range(2):
        w_copy(jnp.int32(s + W_SLOTS)).start()
    r_copy.start()
    g_copy.start()

    @pl.loop(2, total)
    def _(s):
        g, i, b, e, h = decode(s)
        w_copy(s).wait()
        k = lax.rem(s, W_SLOTS)
        p[(g * 4 + b) * nu + i] = jnp.dot(
            a[...], w[k], preferred_element_type=jnp.float32).astype(p.dtype)

        @pl.when(s + W_SLOTS < total)
        def _():
            w_copy(s + W_SLOTS).start()

        def to_relay(lo, n):
            send_units(g, b, lo, n, h * 2 + c, 0, chip(3 + 2 * h, 1 - e))

        @pl.when(i == nu - 1)
        def _():
            @pl.when(s < 2 * nu)
            def _():
                to_relay(1, nu - 1)

            @pl.when(jnp.logical_and(g == 0, s >= 2 * nu))
            def _():
                to_relay(0, nu)

            @pl.when(g == 1)
            def _():
                send_units(g, b, 0, nu, 4 + h * 2 + c, 1, chip(1 + 2 * h, e))

            @pl.when(jnp.logical_or(jnp.logical_and(g == 2, b < 2), jnp.logical_and(g == 3, b >= 2)))
            def _():
                send_units(g, b, 0, nu, 4 + g * 2 + h, 3 - g, x * CORES + 1 - c)

    with jax.named_scope("l2r"):
        wait_bytes(rx.at[pl.ds(0, 6 * nu)], recv_sem.at[0])

    @pl.loop(0, chunks)
    def _(r):
        rs = chunk_rows(r)
        for h in range(2):
            for i in range(nu):
                acc = p[local_unit(3, h, i), rs, :].astype(jnp.float32)
                acc += rx[(10 + h) * nu + i, rs, :].astype(jnp.float32)
                acc += rx[(h * 2) * nu + i, rs, :].astype(jnp.float32)
                acc += rx[(h * 2 + 1) * nu + i, rs, :].astype(jnp.float32)
                relay_out[h, rs, i * UNIT:(i + 1) * UNIT] = acc

    for m in range(len(RELAY_ROWS)):
        send_relay(m)

    r_copy.wait()
    g_copy.wait()
    with jax.named_scope("direct"):
        wait_bytes(rx.at[pl.ds(0, 6 * nu)], recv_sem.at[1])

    sq_n = sum_rows()
    sq_lo = (0, sq_n[0])

    def on_lane(lane, n):
        return (lax.broadcasted_iota(jnp.int32, (n, LANES), 0) + lane
                == lax.broadcasted_iota(jnp.int32, (n, LANES), 1))

    def columns():
        for h in range(2):
            for i in range(nu):
                yield h, i, slice(h * half + i * UNIT, h * half + (i + 1) * UNIT)

    def add_early(lo, n):
        rs = span(lo, n)
        for h, i, cols in columns():
            acc = p[local_unit(2, h, i), rs, :].astype(jnp.float32)
            acc += rx[(8 + h) * nu + i, rs, :].astype(jnp.float32)
            acc += rx[(4 + h * 2) * nu + i, rs, :].astype(jnp.float32)
            acc += rx[(5 + h * 2) * nu + i, rs, :].astype(jnp.float32)
            hbuf[rs, cols] = acc + res[rs, cols].astype(jnp.float32)

    def finish(m, lo, n):
        rs = span(lo, n)
        sq = jnp.zeros((n, UNIT), jnp.float32)
        for h, i, cols in columns():
            acc = hbuf[rs, cols] + relay_in[h, rs, i * UNIT:(i + 1) * UNIT]
            hbuf[rs, cols] = acc
            sq += acc * acc
        sq = jnp.sum(sq, axis=1, keepdims=True)
        q, lane = place(m, lo)
        sq_out[q] += jnp.sum(
            jnp.where(on_lane(lane, n), jnp.broadcast_to(sq, (n, LANES)), 0.0), axis=0, keepdims=True)

    def place(m, lo):
        if m >= EARLY:
            lo = lo - relay_lo[EARLY]
            return sq_lo[1] + lax.div(lo, LANES), lax.rem(lo, LANES)
        return lax.div(lo, LANES), lax.rem(lo, LANES)

    first = 3 * at_first + at_last + 2 * (1 - flip)
    second = 1 + flip
    others = [chip(o, core) for o in (first, second, 6 - first - second) for core in range(CORES)]
    others.append(x * CORES + 1 - c)

    def send_sums(k):
        for target in others:
            pltpu.make_async_remote_copy(
                src_ref=sq_out.at[sq_span(k)], dst_ref=sq_in.at[me, sq_span(k)],
                send_sem=qsend_sem.at[0], recv_sem=qrecv_sem.at[k],
                device_id={"tp": target}, device_id_type=MESH).start()
        for q in range(sq_lo[k], sq_lo[k] + sq_n[k]):
            sq_in[me, q] = sq_out[q]

    def sq_span(k):
        return pl.ds(sq_lo[k], sq_n[k])

    def wait_sums(k, sem):
        wait_bytes(sq_in.at[pl.ds(0, tp_size - 1), sq_span(k)], sem.at[k])

    def normalise(m, lo, n):
        q, lane = place(m, lo)
        tot = sq_in[0, q]
        for t in range(1, tp_size):
            tot += sq_in[t, q]
        col = jnp.sum(jnp.where(on_lane(lane, n), jnp.broadcast_to(tot, (n, LANES)), 0.0), axis=1, keepdims=True)
        scale = lax.rsqrt(col / d_model + EPS)
        rs = span(lo, n)
        nrm[rs, :] = (hbuf[rs, :] * scale * gain[...].reshape(1, d_local)).astype(nrm.dtype)

    def write_hidden(lo, n):
        rs = span(lo, n)
        hid[rs, :] = hbuf[rs, :].astype(hid.dtype)

    def each(m, *steps):
        lo, hi = relay_lo[m], relay_lo[m] + RELAY_ROWS[m]
        whole = (hi - lo) // RB * RB

        if whole:
            @pl.loop(0, whole // RB)
            def _(r):
                for step in steps:
                    step(lo + r * RB, RB)

        if lo + whole < hi:
            for step in steps:
                step(lo + whole, hi - lo - whole)

    def wait_relay(m):
        with jax.named_scope(f"r{m}"):
            wait_bytes(relay_in.at[:, relay_rows(m)], rrecv_sem.at[m])

    for q in range(sum(sq_n)):
        sq_out[q] = jnp.zeros((1, LANES), jnp.float32)
    last = len(RELAY_ROWS) - 1
    for m in range(last + 1):
        each(m, add_early)
        wait_relay(m)
        each(m, functools.partial(finish, m))
        if m in (EARLY - 1, last):
            send_sums(int(m == last))
        each(m, write_hidden)

    wait_bytes(p, send_sem.at[0])
    for m in range(last + 1):
        if m in (0, EARLY):
            with jax.named_scope(f"sq{m}"):
                wait_sums(m // EARLY, qrecv_sem)
        each(m, functools.partial(normalise, m))
    with jax.named_scope("qdrain"):
        wait_bytes(sq_in.at[pl.ds(0, tp_size - 1)], qsend_sem.at[0])


def _write(hid, nrm, hid_hbm, nrm_hbm, sem):
    blocks = 4
    rows = hid.shape[0] // blocks
    pairs = ((hid, hid_hbm), (nrm, nrm_hbm))
    for k, (src, dst) in enumerate(pairs):
        for b in range(blocks):
            rs = pl.ds(b * rows, rows)
            pltpu.make_async_copy(src.at[rs, :], dst.at[rs, :], sem.at[k]).start()
    for k, (src, dst) in enumerate(pairs):
        pltpu.make_async_copy(src, dst, sem.at[k]).wait()


def solution(mesh):
    tp_size = mesh.shape["tp"]

    def local_step(attn_blk, w_blk, resid_blk, gain_blk):
        rows, k_dim = attn_blk.shape
        d_local = resid_blk.shape[1]
        d_model = w_blk.shape[1]
        half = d_local // 2
        nu = half // UNIT
        units = tp_size * 2 * nu
        sq_rows = sum(sum_rows())
        assert tp_size == CORES * CHIPS and half % UNIT == 0
        assert sum(FIRST_ROWS) == sum(RELAY_ROWS) == rows and rows % RB == 0 and nu == 3
        hbm_spec = pl.BlockSpec(memory_space=pltpu.HBM)
        vmem_spec = pl.BlockSpec(memory_space=pltpu.VMEM)
        dma = pltpu.SemaphoreType.DMA
        out_shape = [jax.ShapeDtypeStruct((rows, d_local), jnp.bfloat16)] * 2
        hid, nrm = pl.pallas_call(
            functools.partial(_kernel, tp_size, d_model),
            out_shape=[pltpu.VMEM((rows, d_local), jnp.bfloat16)] * 2,
            in_specs=[hbm_spec] * 4,
            out_specs=[vmem_spec] * 2,
            scratch_shapes=[
                pltpu.VMEM((rows, k_dim), jnp.bfloat16),
                pltpu.VMEM((W_SLOTS, k_dim, UNIT), jnp.bfloat16),
                pltpu.VMEM((units, rows, UNIT), jnp.bfloat16),
                pltpu.VMEM((12 * nu, rows, UNIT), jnp.bfloat16),
                pltpu.VMEM((2, rows, half), jnp.float32),
                pltpu.VMEM((2, rows, half), jnp.float32),
                pltpu.VMEM((rows, d_local), jnp.bfloat16),
                pltpu.VMEM((d_local,), jnp.float32),
                pltpu.VMEM((rows, d_local), jnp.float32),
                pltpu.VMEM((sq_rows, 1, LANES), jnp.float32),
                pltpu.VMEM((tp_size, sq_rows, 1, LANES), jnp.float32),
                dma((len(FIRST_ROWS),)),
                dma((W_SLOTS,)),
                dma((1,)),
                dma((2,)),
                dma((len(RELAY_ROWS),)),
                dma((1,)),
                dma((2,)),
            ],
            compiler_params=pltpu.CompilerParams(
                collective_id=0, has_side_effects=True, vmem_limit_bytes=62 * 1000 * 1000
            ),
            name="proj_scatter_norm",
        )(attn_blk, w_blk, resid_blk, gain_blk)
        return pl.pallas_call(
            _write,
            out_shape=out_shape,
            in_specs=[vmem_spec] * 2,
            out_specs=[hbm_spec] * 2,
            scratch_shapes=[dma((2,))],
            compiler_params=pltpu.CompilerParams(vmem_limit_bytes=8 * 1024 * 1024),
            name="write_out",
        )(hid, nrm)

    return jax.shard_map(
        local_step,
        mesh=mesh,
        in_specs=(P("data", "tp"), P("tp", None), P("data", "tp"), P("tp")),
        out_specs=(P("data", "tp"), P("data", "tp")),
        check_vma=False,
    )
```

```python
import functools

import jax
import jax.numpy as jnp
from jax import lax
from jax.experimental import pallas as pl
from jax.experimental.pallas import tpu as pltpu
from jax.sharding import PartitionSpec as P

EPS = 1e-5
MESH = pl.DeviceIdType.MESH
CORES = 2
CHIPS = 4
UNIT = 256
W_SLOTS = 4
RB = 64
RELAY_ROWS = (256, 192, 32, 32)
EARLY = 2
LANES = 128
FIRST_ROWS = (64, 448)


def sum_rows():
    return -(-sum(RELAY_ROWS[:EARLY]) // LANES), -(-sum(RELAY_ROWS[EARLY:]) // LANES)


def _kernel(
    tp_size, d_model,
    a_hbm, w_hbm, r_hbm, g_hbm, hid, nrm,
    a, w, p, rx, relay_out, relay_in, res, gain, hbuf, sq_out, sq_in,
    a_sem, w_sem, send_sem, recv_sem, rrecv_sem, qsend_sem, qrecv_sem,
):
    rows, d_local = r_hbm.shape
    half = d_local // 2
    nu = half // UNIT
    per_group = CORES * 2 * nu
    total = CHIPS * per_group
    chunks = rows // RB

    me = lax.axis_index("tp")
    x, c = lax.div(me, CORES), lax.rem(me, CORES)

    at_first, at_last = lax.div(CHIPS - x, CHIPS), lax.div(x, CHIPS - 1)
    flip = at_first + at_last

    def chip(offset, core):
        return lax.rem(x + offset, CHIPS) * CORES + core

    def decode(s):
        g, j = lax.div(s, per_group), lax.rem(s, per_group)
        late = lax.div(lax.div(s, 2 * nu) + 7, 8)
        more = lax.div(lax.div(s, 2) + 1, 2)
        b = late * lax.div(j, nu) + (1 - late) * ((1 - more) * s + more * (lax.div(s, 2) - 1))
        i = late * lax.rem(j, nu) + (1 - late) * more * (1 + lax.rem(s, 2))
        return g, i, b, lax.rem(lax.div(b, 2) + 1 + c, 2), lax.rem(b + c + flip, 2)

    def w_copy(s):
        g, i, _, e, h = decode(s)
        o = lax.rem(6 - g + 2 * h * lax.rem(g, 2), CHIPS)
        col = pl.multiple_of(chip(o, e) * d_local + h * half + i * UNIT, UNIT)
        k = lax.rem(s, W_SLOTS)
        return pltpu.make_async_copy(w_hbm.at[:, pl.ds(col, UNIT)], w.at[k], w_sem.at[k])

    first_lo = [sum(FIRST_ROWS[:b]) for b in range(len(FIRST_ROWS))]

    def a_copy(b):
        rs = pl.ds(first_lo[b], FIRST_ROWS[b])
        return pltpu.make_async_copy(a_hbm.at[rs, :], a.at[rs, :], a_sem.at[b])

    def send(src, dst, group, target):
        pltpu.make_async_remote_copy(
            src_ref=src, dst_ref=dst, send_sem=send_sem.at[0], recv_sem=recv_sem.at[group],
            device_id={"tp": target}, device_id_type=MESH).start()

    def send_units(g, b, lo, n, block, group, target):
        send(p.at[pl.ds((g * 4 + b) * nu + lo, n)], rx.at[pl.ds(block * nu + lo, n)], group, target)

    def wait_bytes(ref, sem):
        pltpu.make_async_copy(ref, ref, sem).wait()

    def local_unit(g, h, i):
        return (g * 4 + (2 if g == 2 else 0) + lax.rem(h + c + flip, 2)) * nu + i

    relay_lo = [sum(RELAY_ROWS[:m]) for m in range(len(RELAY_ROWS))]

    def relay_rows(m):
        return pl.ds(relay_lo[m], RELAY_ROWS[m])

    def send_relay(m):
        for h in range(2):
            pltpu.make_async_remote_copy(
                src_ref=relay_out.at[h, relay_rows(m)], dst_ref=relay_in.at[h, relay_rows(m)],
                send_sem=send_sem.at[0], recv_sem=rrecv_sem.at[m],
                device_id={"tp": chip(3 - 2 * h, 1 - c)}, device_id_type=MESH).start()

    def chunk_rows(r):
        return pl.ds(pl.multiple_of(r * RB, RB), RB)

    def span(lo, n):
        return pl.ds(pl.multiple_of(lo, n), n)

    w_copy(jnp.int32(0)).start()
    a_copy(0).start()
    w_copy(jnp.int32(1)).start()

    peers = [x * CORES + 1 - c] + [chip(o, core) for o in (1, CHIPS - 1) for core in range(CORES)]
    barrier = pltpu.get_barrier_semaphore()
    for peer in peers:
        pl.semaphore_signal(barrier, inc=1, device_id={"tp": peer}, device_id_type=MESH)

    for b in range(1, len(FIRST_ROWS)):
        a_copy(b).start()
    r_copy = pltpu.make_async_copy(r_hbm, res, a_sem.at[0])
    g_copy = pltpu.make_async_copy(g_hbm, gain, a_sem.at[1])

    for b in range(len(FIRST_ROWS)):
        rs = pl.ds(first_lo[b], FIRST_ROWS[b])
        for s in range(2):
            _, _, block, e0, h0 = decode(jnp.int32(s))
            if b == 0:
                with jax.named_scope(f"w{s}"):
                    w_copy(jnp.int32(s)).wait()
            if s == 0:
                with jax.named_scope("awt"):
                    a_copy(b).wait()
            if b == 0 and s == 0:
                for k in range(2, W_SLOTS):
                    w_copy(jnp.int32(k)).start()
            unit = block * nu
            p[unit, rs, :] = jnp.dot(a[rs, :], w[s], preferred_element_type=jnp.float32).astype(p.dtype)
            if b == 0 and s == 0:
                with jax.named_scope("bar"):
                    pl.semaphore_wait(barrier, len(peers))
            send(p.at[unit, rs], rx.at[(h0 * 2 + c) * nu, rs], 0, chip(3 + 2 * h0, 1 - e0))
    for s in range(2):
        w_copy(jnp.int32(s + W_SLOTS)).start()
    r_copy.start()
    g_copy.start()

    @pl.loop(2, total)
    def _(s):
        g, i, b, e, h = decode(s)
        w_copy(s).wait()
        k = lax.rem(s, W_SLOTS)
        p[(g * 4 + b) * nu + i] = jnp.dot(
            a[...], w[k], preferred_element_type=jnp.float32).astype(p.dtype)

        @pl.when(s + W_SLOTS < total)
        def _():
            w_copy(s + W_SLOTS).start()

        def to_relay(lo, n):
            send_units(g, b, lo, n, h * 2 + c, 0, chip(3 + 2 * h, 1 - e))

        @pl.when(i == nu - 1)
        def _():
            @pl.when(s < 2 * nu)
            def _():
                to_relay(1, nu - 1)

            @pl.when(jnp.logical_and(g == 0, s >= 2 * nu))
            def _():
                to_relay(0, nu)

            @pl.when(g == 1)
            def _():
                send_units(g, b, 0, nu, 4 + h * 2 + c, 1, chip(1 + 2 * h, e))

            @pl.when(jnp.logical_or(jnp.logical_and(g == 2, b < 2), jnp.logical_and(g == 3, b >= 2)))
            def _():
                send_units(g, b, 0, nu, 4 + g * 2 + h, 3 - g, x * CORES + 1 - c)

    with jax.named_scope("l2r"):
        wait_bytes(rx.at[pl.ds(0, 6 * nu)], recv_sem.at[0])

    @pl.loop(0, chunks)
    def _(r):
        rs = chunk_rows(r)
        for h in range(2):
            for i in range(nu):
                acc = p[local_unit(3, h, i), rs, :].astype(jnp.float32)
                acc += rx[(10 + h) * nu + i, rs, :].astype(jnp.float32)
                acc += rx[(h * 2) * nu + i, rs, :].astype(jnp.float32)
                acc += rx[(h * 2 + 1) * nu + i, rs, :].astype(jnp.float32)
                relay_out[h, rs, i * UNIT:(i + 1) * UNIT] = acc

    for m in range(len(RELAY_ROWS)):
        send_relay(m)

    r_copy.wait()
    g_copy.wait()
    with jax.named_scope("direct"):
        wait_bytes(rx.at[pl.ds(0, 6 * nu)], recv_sem.at[1])

    sq_n = sum_rows()
    sq_lo = (0, sq_n[0])

    def on_lane(lane, n):
        return (lax.broadcasted_iota(jnp.int32, (n, LANES), 0) + lane
                == lax.broadcasted_iota(jnp.int32, (n, LANES), 1))

    def columns():
        for h in range(2):
            for i in range(nu):
                yield h, i, slice(h * half + i * UNIT, h * half + (i + 1) * UNIT)

    def add_early(lo, n):
        rs = span(lo, n)
        for h, i, cols in columns():
            acc = p[local_unit(2, h, i), rs, :].astype(jnp.float32)
            acc += rx[(8 + h) * nu + i, rs, :].astype(jnp.float32)
            acc += rx[(4 + h * 2) * nu + i, rs, :].astype(jnp.float32)
            acc += rx[(5 + h * 2) * nu + i, rs, :].astype(jnp.float32)
            hbuf[rs, cols] = acc + res[rs, cols].astype(jnp.float32)

    def finish(m, lo, n):
        rs = span(lo, n)
        sq = jnp.zeros((n, UNIT), jnp.float32)
        for h, i, cols in columns():
            acc = hbuf[rs, cols] + relay_in[h, rs, i * UNIT:(i + 1) * UNIT]
            hbuf[rs, cols] = acc
            sq += acc * acc
        sq = jnp.sum(sq, axis=1, keepdims=True)
        q, lane = place(m, lo)
        sq_out[q] += jnp.sum(
            jnp.where(on_lane(lane, n), jnp.broadcast_to(sq, (n, LANES)), 0.0), axis=0, keepdims=True)

    def place(m, lo):
        if m >= EARLY:
            lo = lo - relay_lo[EARLY]
            return sq_lo[1] + lax.div(lo, LANES), lax.rem(lo, LANES)
        return lax.div(lo, LANES), lax.rem(lo, LANES)

    first = 3 * at_first + at_last + 2 * (1 - flip)
    second = 1 + flip
    others = [chip(o, core) for o in (first, second, 6 - first - second) for core in range(CORES)]
    others.append(x * CORES + 1 - c)

    def send_sums(k):
        for target in others:
            pltpu.make_async_remote_copy(
                src_ref=sq_out.at[sq_span(k)], dst_ref=sq_in.at[me, sq_span(k)],
                send_sem=qsend_sem.at[0], recv_sem=qrecv_sem.at[k],
                device_id={"tp": target}, device_id_type=MESH).start()
        for q in range(sq_lo[k], sq_lo[k] + sq_n[k]):
            sq_in[me, q] = sq_out[q]

    def sq_span(k):
        return pl.ds(sq_lo[k], sq_n[k])

    def wait_sums(k, sem):
        wait_bytes(sq_in.at[pl.ds(0, tp_size - 1), sq_span(k)], sem.at[k])

    def normalise(m, lo, n):
        q, lane = place(m, lo)
        tot = sq_in[0, q]
        for t in range(1, tp_size):
            tot += sq_in[t, q]
        col = jnp.sum(jnp.where(on_lane(lane, n), jnp.broadcast_to(tot, (n, LANES)), 0.0), axis=1, keepdims=True)
        scale = lax.rsqrt(col / d_model + EPS)
        rs = span(lo, n)
        nrm[rs, :] = (hbuf[rs, :] * scale * gain[...].reshape(1, d_local)).astype(nrm.dtype)

    def write_hidden(lo, n):
        rs = span(lo, n)
        hid[rs, :] = hbuf[rs, :].astype(hid.dtype)

    def each(m, *steps):
        lo, hi = relay_lo[m], relay_lo[m] + RELAY_ROWS[m]
        whole = (hi - lo) // RB * RB

        if whole:
            @pl.loop(0, whole // RB)
            def _(r):
                for step in steps:
                    step(lo + r * RB, RB)

        if lo + whole < hi:
            for step in steps:
                step(lo + whole, hi - lo - whole)

    def wait_relay(m):
        with jax.named_scope(f"r{m}"):
            wait_bytes(relay_in.at[:, relay_rows(m)], rrecv_sem.at[m])

    for q in range(sum(sq_n)):
        sq_out[q] = jnp.zeros((1, LANES), jnp.float32)
    last = len(RELAY_ROWS) - 1
    for m in range(last + 1):
        each(m, add_early)
        wait_relay(m)
        each(m, functools.partial(finish, m))
        if m in (EARLY - 1, last):
            send_sums(int(m == last))
        each(m, write_hidden)

    wait_bytes(p, send_sem.at[0])
    for m in range(last + 1):
        if m in (0, EARLY):
            with jax.named_scope(f"sq{m}"):
                wait_sums(m // EARLY, qrecv_sem)
        each(m, functools.partial(normalise, m))
    with jax.named_scope("qdrain"):
        wait_bytes(sq_in.at[pl.ds(0, tp_size - 1)], qsend_sem.at[0])


def _write(hid, nrm, hid_hbm, nrm_hbm, sem):
    blocks = 4
    rows = hid.shape[0] // blocks
    pairs = ((hid, hid_hbm), (nrm, nrm_hbm))
    for k, (src, dst) in enumerate(pairs):
        for b in range(blocks):
            rs = pl.ds(b * rows, rows)
            pltpu.make_async_copy(src.at[rs, :], dst.at[rs, :], sem.at[k]).start()
    for k, (src, dst) in enumerate(pairs):
        pltpu.make_async_copy(src, dst, sem.at[k]).wait()


def solution(mesh):
    tp_size = mesh.shape["tp"]

    def local_step(attn_blk, w_blk, resid_blk, gain_blk):
        rows, k_dim = attn_blk.shape
        d_local = resid_blk.shape[1]
        d_model = w_blk.shape[1]
        half = d_local // 2
        nu = half // UNIT
        units = tp_size * 2 * nu
        sq_rows = sum(sum_rows())
        assert tp_size == CORES * CHIPS and half % UNIT == 0
        assert sum(FIRST_ROWS) == sum(RELAY_ROWS) == rows and rows % RB == 0 and nu == 3
        hbm_spec = pl.BlockSpec(memory_space=pltpu.HBM)
        vmem_spec = pl.BlockSpec(memory_space=pltpu.VMEM)
        dma = pltpu.SemaphoreType.DMA
        out_shape = [jax.ShapeDtypeStruct((rows, d_local), jnp.bfloat16)] * 2
        hid, nrm = pl.pallas_call(
            functools.partial(_kernel, tp_size, d_model),
            out_shape=[pltpu.VMEM((rows, d_local), jnp.bfloat16)] * 2,
            in_specs=[hbm_spec] * 4,
            out_specs=[vmem_spec] * 2,
            scratch_shapes=[
                pltpu.VMEM((rows, k_dim), jnp.bfloat16),
                pltpu.VMEM((W_SLOTS, k_dim, UNIT), jnp.bfloat16),
                pltpu.VMEM((units, rows, UNIT), jnp.bfloat16),
                pltpu.VMEM((12 * nu, rows, UNIT), jnp.bfloat16),
                pltpu.VMEM((2, rows, half), jnp.float32),
                pltpu.VMEM((2, rows, half), jnp.float32),
                pltpu.VMEM((rows, d_local), jnp.bfloat16),
                pltpu.VMEM((d_local,), jnp.float32),
                pltpu.VMEM((rows, d_local), jnp.float32),
                pltpu.VMEM((sq_rows, 1, LANES), jnp.float32),
                pltpu.VMEM((tp_size, sq_rows, 1, LANES), jnp.float32),
                dma((len(FIRST_ROWS),)),
                dma((W_SLOTS,)),
                dma((1,)),
                dma((2,)),
                dma((len(RELAY_ROWS),)),
                dma((1,)),
                dma((2,)),
            ],
            compiler_params=pltpu.CompilerParams(
                collective_id=0, has_side_effects=True, vmem_limit_bytes=62 * 1000 * 1000
            ),
            name="proj_scatter_norm",
        )(attn_blk, w_blk, resid_blk, gain_blk)
        return pl.pallas_call(
            _write,
            out_shape=out_shape,
            in_specs=[vmem_spec] * 2,
            out_specs=[hbm_spec] * 2,
            scratch_shapes=[dma((2,))],
            compiler_params=pltpu.CompilerParams(vmem_limit_bytes=8 * 1024 * 1024),
            name="write_out",
        )(hid, nrm)

    return jax.shard_map(
        local_step,
        mesh=mesh,
        in_specs=(P("data", "tp"), P("tp", None), P("data", "tp"), P("tp")),
        out_specs=(P("data", "tp"), P("data", "tp")),
        check_vma=False,
    )
```

```python
import functools

import jax
import jax.numpy as jnp
from jax import lax
from jax.experimental import pallas as pl
from jax.experimental.pallas import tpu as pltpu
from jax.sharding import PartitionSpec as P

EPS = 1e-5
MESH = pl.DeviceIdType.MESH
CORES = 2
CHIPS = 4
UNIT = 256
W_SLOTS = 4
RB = 64
RELAY_ROWS = (256, 192, 32, 32)
EARLY = 2
LANES = 128
FIRST_ROWS = (192, 320)


def sum_rows():
    return -(-sum(RELAY_ROWS[:EARLY]) // LANES), -(-sum(RELAY_ROWS[EARLY:]) // LANES)


def _kernel(
    tp_size, d_model,
    a_hbm, w_hbm, r_hbm, g_hbm, hid, nrm,
    a, w, p, rx, relay_out, relay_in, res, gain, hbuf, sq_out, sq_in,
    a_sem, w_sem, send_sem, recv_sem, rrecv_sem, qsend_sem, qrecv_sem,
):
    rows, d_local = r_hbm.shape
    half = d_local // 2
    nu = half // UNIT
    per_group = CORES * 2 * nu
    total = CHIPS * per_group
    chunks = rows // RB

    me = lax.axis_index("tp")
    x, c = lax.div(me, CORES), lax.rem(me, CORES)

    at_first, at_last = lax.div(CHIPS - x, CHIPS), lax.div(x, CHIPS - 1)
    flip = at_first + at_last

    def chip(offset, core):
        return lax.rem(x + offset, CHIPS) * CORES + core

    def decode(s):
        g, j = lax.div(s, per_group), lax.rem(s, per_group)
        late = lax.div(lax.div(s, 2 * nu) + 7, 8)
        more = lax.div(lax.div(s, 2) + 1, 2)
        b = late * lax.div(j, nu) + (1 - late) * ((1 - more) * s + more * (lax.div(s, 2) - 1))
        i = late * lax.rem(j, nu) + (1 - late) * more * (1 + lax.rem(s, 2))
        return g, i, b, lax.rem(lax.div(b, 2) + 1 + c, 2), lax.rem(b + c + flip, 2)

    def w_copy(s):
        g, i, _, e, h = decode(s)
        o = lax.rem(6 - g + 2 * h * lax.rem(g, 2), CHIPS)
        col = pl.multiple_of(chip(o, e) * d_local + h * half + i * UNIT, UNIT)
        k = lax.rem(s, W_SLOTS)
        return pltpu.make_async_copy(w_hbm.at[:, pl.ds(col, UNIT)], w.at[k], w_sem.at[k])

    first_lo = [sum(FIRST_ROWS[:b]) for b in range(len(FIRST_ROWS))]

    def a_copy(b):
        rs = pl.ds(first_lo[b], FIRST_ROWS[b])
        return pltpu.make_async_copy(a_hbm.at[rs, :], a.at[rs, :], a_sem.at[b])

    def send(src, dst, group, target):
        pltpu.make_async_remote_copy(
            src_ref=src, dst_ref=dst, send_sem=send_sem.at[0], recv_sem=recv_sem.at[group],
            device_id={"tp": target}, device_id_type=MESH).start()

    def send_units(g, b, lo, n, block, group, target):
        send(p.at[pl.ds((g * 4 + b) * nu + lo, n)], rx.at[pl.ds(block * nu + lo, n)], group, target)

    def wait_bytes(ref, sem):
        pltpu.make_async_copy(ref, ref, sem).wait()

    def local_unit(g, h, i):
        return (g * 4 + (2 if g == 2 else 0) + lax.rem(h + c + flip, 2)) * nu + i

    relay_lo = [sum(RELAY_ROWS[:m]) for m in range(len(RELAY_ROWS))]

    def relay_rows(m):
        return pl.ds(relay_lo[m], RELAY_ROWS[m])

    def send_relay(m):
        for h in range(2):
            pltpu.make_async_remote_copy(
                src_ref=relay_out.at[h, relay_rows(m)], dst_ref=relay_in.at[h, relay_rows(m)],
                send_sem=send_sem.at[0], recv_sem=rrecv_sem.at[m],
                device_id={"tp": chip(3 - 2 * h, 1 - c)}, device_id_type=MESH).start()

    def chunk_rows(r):
        return pl.ds(pl.multiple_of(r * RB, RB), RB)

    def span(lo, n):
        return pl.ds(pl.multiple_of(lo, n), n)

    w_copy(jnp.int32(0)).start()
    a_copy(0).start()
    w_copy(jnp.int32(1)).start()

    peers = [x * CORES + 1 - c] + [chip(o, core) for o in (1, CHIPS - 1) for core in range(CORES)]
    barrier = pltpu.get_barrier_semaphore()
    for peer in peers:
        pl.semaphore_signal(barrier, inc=1, device_id={"tp": peer}, device_id_type=MESH)

    for b in range(1, len(FIRST_ROWS)):
        a_copy(b).start()
    r_copy = pltpu.make_async_copy(r_hbm, res, a_sem.at[0])
    g_copy = pltpu.make_async_copy(g_hbm, gain, a_sem.at[1])

    for b in range(len(FIRST_ROWS)):
        rs = pl.ds(first_lo[b], FIRST_ROWS[b])
        for s in range(2):
            _, _, block, e0, h0 = decode(jnp.int32(s))
            if b == 0:
                with jax.named_scope(f"w{s}"):
                    w_copy(jnp.int32(s)).wait()
            if s == 0:
                with jax.named_scope("awt"):
                    a_copy(b).wait()
            if b == 0 and s == 0:
                for k in range(2, W_SLOTS):
                    w_copy(jnp.int32(k)).start()
            unit = block * nu
            p[unit, rs, :] = jnp.dot(a[rs, :], w[s], preferred_element_type=jnp.float32).astype(p.dtype)
            if b == 0 and s == 0:
                with jax.named_scope("bar"):
                    pl.semaphore_wait(barrier, len(peers))
            send(p.at[unit, rs], rx.at[(h0 * 2 + c) * nu, rs], 0, chip(3 + 2 * h0, 1 - e0))
    for s in range(2):
        w_copy(jnp.int32(s + W_SLOTS)).start()
    r_copy.start()
    g_copy.start()

    @pl.loop(2, total)
    def _(s):
        g, i, b, e, h = decode(s)
        w_copy(s).wait()
        k = lax.rem(s, W_SLOTS)
        p[(g * 4 + b) * nu + i] = jnp.dot(
            a[...], w[k], preferred_element_type=jnp.float32).astype(p.dtype)

        @pl.when(s + W_SLOTS < total)
        def _():
            w_copy(s + W_SLOTS).start()

        def to_relay(lo, n):
            send_units(g, b, lo, n, h * 2 + c, 0, chip(3 + 2 * h, 1 - e))

        @pl.when(i == nu - 1)
        def _():
            @pl.when(s < 2 * nu)
            def _():
                to_relay(1, nu - 1)

            @pl.when(jnp.logical_and(g == 0, s >= 2 * nu))
            def _():
                to_relay(0, nu)

            @pl.when(g == 1)
            def _():
                send_units(g, b, 0, nu, 4 + h * 2 + c, 1, chip(1 + 2 * h, e))

            @pl.when(jnp.logical_or(jnp.logical_and(g == 2, b < 2), jnp.logical_and(g == 3, b >= 2)))
            def _():
                send_units(g, b, 0, nu, 4 + g * 2 + h, 3 - g, x * CORES + 1 - c)

    with jax.named_scope("l2r"):
        wait_bytes(rx.at[pl.ds(0, 6 * nu)], recv_sem.at[0])

    @pl.loop(0, chunks)
    def _(r):
        rs = chunk_rows(r)
        for h in range(2):
            for i in range(nu):
                acc = p[local_unit(3, h, i), rs, :].astype(jnp.float32)
                acc += rx[(10 + h) * nu + i, rs, :].astype(jnp.float32)
                acc += rx[(h * 2) * nu + i, rs, :].astype(jnp.float32)
                acc += rx[(h * 2 + 1) * nu + i, rs, :].astype(jnp.float32)
                relay_out[h, rs, i * UNIT:(i + 1) * UNIT] = acc

    for m in range(len(RELAY_ROWS)):
        send_relay(m)

    r_copy.wait()
    g_copy.wait()
    with jax.named_scope("direct"):
        wait_bytes(rx.at[pl.ds(0, 6 * nu)], recv_sem.at[1])

    sq_n = sum_rows()
    sq_lo = (0, sq_n[0])

    def on_lane(lane, n):
        return (lax.broadcasted_iota(jnp.int32, (n, LANES), 0) + lane
                == lax.broadcasted_iota(jnp.int32, (n, LANES), 1))

    def columns():
        for h in range(2):
            for i in range(nu):
                yield h, i, slice(h * half + i * UNIT, h * half + (i + 1) * UNIT)

    def add_early(lo, n):
        rs = span(lo, n)
        for h, i, cols in columns():
            acc = p[local_unit(2, h, i), rs, :].astype(jnp.float32)
            acc += rx[(8 + h) * nu + i, rs, :].astype(jnp.float32)
            acc += rx[(4 + h * 2) * nu + i, rs, :].astype(jnp.float32)
            acc += rx[(5 + h * 2) * nu + i, rs, :].astype(jnp.float32)
            hbuf[rs, cols] = acc + res[rs, cols].astype(jnp.float32)

    def finish(m, lo, n):
        rs = span(lo, n)
        sq = jnp.zeros((n, UNIT), jnp.float32)
        for h, i, cols in columns():
            acc = hbuf[rs, cols] + relay_in[h, rs, i * UNIT:(i + 1) * UNIT]
            hbuf[rs, cols] = acc
            sq += acc * acc
        sq = jnp.sum(sq, axis=1, keepdims=True)
        q, lane = place(m, lo)
        sq_out[q] += jnp.sum(
            jnp.where(on_lane(lane, n), jnp.broadcast_to(sq, (n, LANES)), 0.0), axis=0, keepdims=True)

    def place(m, lo):
        if m >= EARLY:
            lo = lo - relay_lo[EARLY]
            return sq_lo[1] + lax.div(lo, LANES), lax.rem(lo, LANES)
        return lax.div(lo, LANES), lax.rem(lo, LANES)

    first = 3 * at_first + at_last + 2 * (1 - flip)
    second = 1 + flip
    others = [chip(o, core) for o in (first, second, 6 - first - second) for core in range(CORES)]
    others.append(x * CORES + 1 - c)

    def send_sums(k):
        for target in others:
            pltpu.make_async_remote_copy(
                src_ref=sq_out.at[sq_span(k)], dst_ref=sq_in.at[me, sq_span(k)],
                send_sem=qsend_sem.at[0], recv_sem=qrecv_sem.at[k],
                device_id={"tp": target}, device_id_type=MESH).start()
        for q in range(sq_lo[k], sq_lo[k] + sq_n[k]):
            sq_in[me, q] = sq_out[q]

    def sq_span(k):
        return pl.ds(sq_lo[k], sq_n[k])

    def wait_sums(k, sem):
        wait_bytes(sq_in.at[pl.ds(0, tp_size - 1), sq_span(k)], sem.at[k])

    def normalise(m, lo, n):
        q, lane = place(m, lo)
        tot = sq_in[0, q]
        for t in range(1, tp_size):
            tot += sq_in[t, q]
        col = jnp.sum(jnp.where(on_lane(lane, n), jnp.broadcast_to(tot, (n, LANES)), 0.0), axis=1, keepdims=True)
        scale = lax.rsqrt(col / d_model + EPS)
        rs = span(lo, n)
        nrm[rs, :] = (hbuf[rs, :] * scale * gain[...].reshape(1, d_local)).astype(nrm.dtype)

    def write_hidden(lo, n):
        rs = span(lo, n)
        hid[rs, :] = hbuf[rs, :].astype(hid.dtype)

    def each(m, *steps):
        lo, hi = relay_lo[m], relay_lo[m] + RELAY_ROWS[m]
        whole = (hi - lo) // RB * RB

        if whole:
            @pl.loop(0, whole // RB)
            def _(r):
                for step in steps:
                    step(lo + r * RB, RB)

        if lo + whole < hi:
            for step in steps:
                step(lo + whole, hi - lo - whole)

    def wait_relay(m):
        with jax.named_scope(f"r{m}"):
            wait_bytes(relay_in.at[:, relay_rows(m)], rrecv_sem.at[m])

    for q in range(sum(sq_n)):
        sq_out[q] = jnp.zeros((1, LANES), jnp.float32)
    last = len(RELAY_ROWS) - 1
    for m in range(last + 1):
        each(m, add_early)
        wait_relay(m)
        each(m, functools.partial(finish, m))
        if m in (EARLY - 1, last):
            send_sums(int(m == last))
        each(m, write_hidden)

    wait_bytes(p, send_sem.at[0])
    for m in range(last + 1):
        if m in (0, EARLY):
            with jax.named_scope(f"sq{m}"):
                wait_sums(m // EARLY, qrecv_sem)
        each(m, functools.partial(normalise, m))
    with jax.named_scope("qdrain"):
        wait_bytes(sq_in.at[pl.ds(0, tp_size - 1)], qsend_sem.at[0])


def _write(hid, nrm, hid_hbm, nrm_hbm, sem):
    blocks = 4
    rows = hid.shape[0] // blocks
    pairs = ((hid, hid_hbm), (nrm, nrm_hbm))
    for k, (src, dst) in enumerate(pairs):
        for b in range(blocks):
            rs = pl.ds(b * rows, rows)
            pltpu.make_async_copy(src.at[rs, :], dst.at[rs, :], sem.at[k]).start()
    for k, (src, dst) in enumerate(pairs):
        pltpu.make_async_copy(src, dst, sem.at[k]).wait()


def solution(mesh):
    tp_size = mesh.shape["tp"]

    def local_step(attn_blk, w_blk, resid_blk, gain_blk):
        rows, k_dim = attn_blk.shape
        d_local = resid_blk.shape[1]
        d_model = w_blk.shape[1]
        half = d_local // 2
        nu = half // UNIT
        units = tp_size * 2 * nu
        sq_rows = sum(sum_rows())
        assert tp_size == CORES * CHIPS and half % UNIT == 0
        assert sum(FIRST_ROWS) == sum(RELAY_ROWS) == rows and rows % RB == 0 and nu == 3
        hbm_spec = pl.BlockSpec(memory_space=pltpu.HBM)
        vmem_spec = pl.BlockSpec(memory_space=pltpu.VMEM)
        dma = pltpu.SemaphoreType.DMA
        out_shape = [jax.ShapeDtypeStruct((rows, d_local), jnp.bfloat16)] * 2
        hid, nrm = pl.pallas_call(
            functools.partial(_kernel, tp_size, d_model),
            out_shape=[pltpu.VMEM((rows, d_local), jnp.bfloat16)] * 2,
            in_specs=[hbm_spec] * 4,
            out_specs=[vmem_spec] * 2,
            scratch_shapes=[
                pltpu.VMEM((rows, k_dim), jnp.bfloat16),
                pltpu.VMEM((W_SLOTS, k_dim, UNIT), jnp.bfloat16),
                pltpu.VMEM((units, rows, UNIT), jnp.bfloat16),
                pltpu.VMEM((12 * nu, rows, UNIT), jnp.bfloat16),
                pltpu.VMEM((2, rows, half), jnp.float32),
                pltpu.VMEM((2, rows, half), jnp.float32),
                pltpu.VMEM((rows, d_local), jnp.bfloat16),
                pltpu.VMEM((d_local,), jnp.float32),
                pltpu.VMEM((rows, d_local), jnp.float32),
                pltpu.VMEM((sq_rows, 1, LANES), jnp.float32),
                pltpu.VMEM((tp_size, sq_rows, 1, LANES), jnp.float32),
                dma((len(FIRST_ROWS),)),
                dma((W_SLOTS,)),
                dma((1,)),
                dma((2,)),
                dma((len(RELAY_ROWS),)),
                dma((1,)),
                dma((2,)),
            ],
            compiler_params=pltpu.CompilerParams(
                collective_id=0, has_side_effects=True, vmem_limit_bytes=62 * 1000 * 1000
            ),
            name="proj_scatter_norm",
        )(attn_blk, w_blk, resid_blk, gain_blk)
        return pl.pallas_call(
            _write,
            out_shape=out_shape,
            in_specs=[vmem_spec] * 2,
            out_specs=[hbm_spec] * 2,
            scratch_shapes=[dma((2,))],
            compiler_params=pltpu.CompilerParams(vmem_limit_bytes=8 * 1024 * 1024),
            name="write_out",
        )(hid, nrm)

    return jax.shard_map(
        local_step,
        mesh=mesh,
        in_specs=(P("data", "tp"), P("tp", None), P("data", "tp"), P("tp")),
        out_specs=(P("data", "tp"), P("data", "tp")),
        check_vma=False,
    )
```
